128 devices in a mesh: ocn: 8 (over z, core), grp: 16 (over x, y).
Axes of the slice: x: 4, y: 4, z: 4, core: 2. Of those that a mesh axis runs over, the one named last changes fastest.
Arguments:
- tracers: float32 [2, 32, 512, 2048], P(None, None, 'grp', 'ocn'), may hold values from -6 to 6
- velocity: float32 [2, 32, 512, 2048], P(None, None, 'grp', 'ocn'), may hold values from -3 to 3
- remap_weights: bfloat16 [512, 8, 128, 128], P('grp'), may hold values from -0.25 to 0.25
- remap_blocks: int32 [512, 8], P('grp'), may hold values from 0 to 8191
- remap_count: int32 [512], P('grp'), may hold values from 1 to 8, as said below
- ice_velocity: float32 [2, 65536], P(None, 'grp'), may hold values from -3 to 3
- ice_mass_rate: float32 [65536], P('grp'), may hold values from 0.5 to 4
- ice_strength: float32 [65536], P('grp'), may hold values from 0.5 to 8
- wind_stress: float32 [2, 65536], P(None, 'grp'), may hold values from -6 to 6
Outputs:
- tracers_next: float32 [2, 32, 512, 2048], P(None, None, 'grp', 'ocn')
- surface_flux: float32 [3, 512, 2048], P(None, 'grp', 'ocn')
- ice_final: float32 [2, 65536], P(None, 'grp')
The draws below stay inside these ranges and needn't reach their ends.
Inputs may be any that keep to these rules, and one draw needn't show every extreme that they name: `remap_count`: every ice block has at least one live entry. The ice blocks of the first and of the last index of grp have 7 or 8 live entries; all others have 1 or 2.
All inputs are finite; a program needn't handle non-finite values.
Results may differ from the reference program's by a relative error of at most 0.0006.
The reference program's roundings to bfloat16 on the way (of `surface` and `ice_flux`) count: a program that leaves them out, or rounds other values in their place, can miss the bound.
Values may be sent and summed in bfloat16 or wider, within the bound.
A program may use at most 128 MiB of HBM per device.

```python
import math
import jax
import jax.numpy as jnp
from jax import lax

L = 32
CY = 32
CX = 256
BS = 128
K = 8
IBD = 32
ITERS = 4
DEPTH = 3
NY = 512
NX = 2048
BPD = 64
OB = 8192
ICE_BLOCKS = 512
ICE_CELLS = 65536
N_OCN = 8
N_GRP = 16


def draw_remap_count(key, part):
    busy_key = jax.random.fold_in(key, 11)
    drawn_key = jax.random.fold_in(key, 23)
    busy = jax.random.randint(busy_key, (ICE_BLOCKS,), K - 1, K + 1)
    drawn = jax.random.randint(drawn_key, (ICE_BLOCKS,), 1, max(2, K // 4) + 1)
    position = jnp.arange(ICE_BLOCKS)
    polar = (position < IBD) | (position >= ICE_BLOCKS - IBD)
    return jnp.where(polar, busy, drawn).astype(jnp.int32)


def draw_wind_stress(key, part):
    noise_key = jax.random.fold_in(key, 37)
    place = jnp.arange(ICE_CELLS, dtype=jnp.float32) / max(ICE_CELLS - 1, 1)
    ramp = 1.0 + 3.0 * place
    noise = jax.random.normal(noise_key, (2, ICE_CELLS), jnp.float32) * 0.5
    return jnp.clip(noise * ramp[None, :], -6.0, 6.0).astype(jnp.float32)


def plant(result, rng, low, largest):
    shape = result.shape
    spot = [jax.random.randint(jax.random.fold_in(rng, axis), (), 0, shape[axis]) for axis in range(len(shape))]
    result = result.at[tuple(spot)].set(low)
    longest = shape.index(max(shape))
    spot[longest] = (spot[longest] + 1) % shape[longest]
    return result.at[tuple(spot)].set(largest)


def shard_levels(own_key, shape, cuts, low, largest):
    loudness, own = 1.0, jax.random.fold_in(own_key, 6)
    for dim, parts in cuts:
        heights = jnp.exp(jax.random.uniform(jax.random.fold_in(own, dim), (parts,), jnp.float32, low / len(cuts), largest / len(cuts)))
        loudness = loudness * jnp.repeat(heights, shape[dim] // parts).reshape([-1 if axis == dim else 1 for axis in range(len(shape))])
    return loudness


def scatter_about(stream_key, extent, width, limit, split=(), kind=jnp.bfloat16):
    array = jax.random.normal(stream_key, extent, jnp.float32) * width
    if len(split) > 0:
        array = shard_levels(stream_key, extent, split, -0.22, 0.18) * array
    return jnp.clip(array, min=-limit, max=limit).astype(kind)


def setup_inputs(seed: int = 0) -> dict:
    arg_keys = jax.random.split(jax.random.key(seed), 10)
    tracers = scatter_about(arg_keys[0], (2, L, NY, NX), 1.0, 6.0, ((2, 16), (3, 8)), jnp.float32)
    velocity = scatter_about(arg_keys[1], (2, L, NY, NX), 0.5, 3.0, ((2, 16), (3, 8)), jnp.float32)
    remap_weights = scatter_about(arg_keys[2], (ICE_BLOCKS, K, BS, BS), (BS * K // 2) ** -0.5, 0.25, ((0, 16),))
    remap_blocks = plant(jax.random.randint(arg_keys[3], (ICE_BLOCKS, K), 0, OB), jax.random.fold_in(arg_keys[3], 1), 0, OB - 1).astype(jnp.int32)
    remap_count = draw_remap_count(jax.random.fold_in(arg_keys[9], 71), 0)
    ice_velocity = scatter_about(arg_keys[5], (2, ICE_CELLS), 0.5, 3.0, ((1, 16),), jnp.float32)
    ice_mass_rate = jnp.clip(jnp.exp(math.log(4.0) - 2.0794415 * jax.random.uniform(arg_keys[6], (ICE_CELLS,), jnp.float32) ** shard_levels(arg_keys[6], (ICE_CELLS,), ((0, 16),), -0.2, 0.2)), 0.5, 4.0)
    ice_strength = jnp.clip(jnp.exp(math.log(8.0) - 2.7725887 * jax.random.uniform(arg_keys[7], (ICE_CELLS,), jnp.float32) ** shard_levels(arg_keys[7], (ICE_CELLS,), ((0, 16),), -0.2, 0.2)), 0.5, 8.0)
    wind_stress = draw_wind_stress(jax.random.fold_in(arg_keys[9], 71), 0)
    return {"tracers": tracers, "velocity": velocity, "remap_weights": remap_weights, "remap_blocks": remap_blocks, "remap_count": remap_count, "ice_velocity": ice_velocity, "ice_mass_rate": ice_mass_rate, "ice_strength": ice_strength, "wind_stress": wind_stress}


def pack_surface(fields):
    count = fields.shape[0]
    grid = fields.reshape(count, N_GRP, CY, N_OCN, CX).transpose(3, 1, 0, 2, 4)
    grid = grid.reshape(N_OCN, N_GRP, count, BPD, BS).transpose(0, 1, 3, 2, 4)
    return grid.reshape(OB, count, BS)

def unpack_surface(blocks):
    count = blocks.shape[1]
    grid = blocks.reshape(N_OCN, N_GRP, BPD, count, BS).transpose(3, 1, 0, 2, 4)
    grid = grid.reshape(count, N_GRP, N_OCN, CY, CX).transpose(0, 1, 3, 2, 4)
    return grid.reshape(count, NY, NX)

def picard_map(u, base, rate, strength):
    padded = jnp.pad(u, ((0, 0), (1, 1)))
    left = padded[:, :-2]
    right = padded[:, 2:]
    strain = 0.5 * (right - left)
    zeta = strength / (2.0 * jnp.sqrt(lax.optimization_barrier(jnp.sum(strain * strain, axis=0)) + 0.25))
    return (base + zeta * (left + right)) / (rate + 1.0 + 2.0 * zeta)

def reference(tracers, velocity, remap_weights, remap_blocks, remap_count, ice_velocity, ice_mass_rate, ice_strength, wind_stress):
    live = (jnp.arange(K)[None, :] < remap_count[:, None]).astype(jnp.float32)
    surface = jnp.stack([tracers[0, 0], tracers[1, 0], velocity[0, 0], velocity[1, 0]]).astype(jnp.bfloat16)
    blocks = pack_surface(surface)
    source = blocks[remap_blocks].astype(jnp.float32) * live[:, :, None, None]
    weights = remap_weights.astype(jnp.float32)
    remapped = jnp.einsum('rkij,rkfj->rfi', weights, source, precision=lax.Precision.HIGHEST)
    remapped = remapped.transpose(1, 0, 2).reshape(4, ICE_CELLS)
    base = ice_mass_rate * ice_velocity + wind_stress + remapped[2:4]
    total = 2.0 * ICE_CELLS
    current = ice_velocity
    gvals = []
    fvals = []
    for step in range(ITERS):
        gnew = picard_map(current, base, ice_mass_rate, ice_strength)
        gvals.append(gnew)
        fvals.append(gnew - current)
        if step == 0:
            current = gnew
            continue
        depth = min(step, DEPTH)
        diffs = jnp.stack([fvals[j] - fvals[j - 1] for j in range(step - depth + 1, step + 1)])
        gdiffs = jnp.stack([gvals[j] - gvals[j - 1] for j in range(step - depth + 1, step + 1)])
        norms = jnp.sqrt(lax.optimization_barrier(jnp.sum(diffs * diffs, axis=(1, 2))) / total + 1e-06)
        gram = jnp.einsum('aij,bij->ab', diffs, diffs, precision=lax.Precision.HIGHEST) / total
        gram = gram / (norms[:, None] * norms[None, :])
        rhs = jnp.einsum('aij,ij->a', diffs, fvals[step], precision=lax.Precision.HIGHEST) / total / norms
        coef = jnp.linalg.solve(gram + 0.1 * jnp.eye(depth, dtype=jnp.float32), rhs)
        current = gnew - jnp.einsum('a,aij->ij', coef / norms, gdiffs, precision=lax.Precision.HIGHEST)
    ice_final = current
    heat = 0.5 * (-0.05 * remapped[1] - remapped[0])
    ice_flux = jnp.concatenate([ice_final - remapped[2:4], heat[None]], axis=0).astype(jnp.bfloat16)
    flux_blocks = ice_flux.astype(jnp.float32).reshape(3, ICE_BLOCKS, BS).transpose(1, 0, 2)
    contrib = jnp.einsum('rkij,rfi->rkfj', weights, flux_blocks, precision=lax.Precision.HIGHEST)
    contrib = (contrib * live[:, :, None, None]).reshape(ICE_BLOCKS * K, 3, BS)
    summed = jax.ops.segment_sum(contrib, remap_blocks.reshape(-1), num_segments=OB)
    surface_flux = unpack_surface(summed)
    padded = jnp.pad(tracers, ((0, 0), (1, 1), (1, 1), (1, 1)))
    centre = padded[:, 1:-1, 1:-1, 1:-1]
    east = padded[:, 1:-1, 1:-1, 2:]
    west = padded[:, 1:-1, 1:-1, :-2]
    north = padded[:, 1:-1, 2:, 1:-1]
    south = padded[:, 1:-1, :-2, 1:-1]
    upper = padded[:, :-2, 1:-1, 1:-1]
    lower = padded[:, 2:, 1:-1, 1:-1]
    advect = velocity[0][None] * (east - west) * 0.5 + velocity[1][None] * (north - south) * 0.5
    tracers_next = centre + 0.2 * (east + west + north + south - 4.0 * centre) - 0.5 * advect + 0.2 * (upper + lower - 2.0 * centre)
    tracers_next = tracers_next.at[0, 0].add(0.5 * surface_flux[2])
    return (tracers_next, surface_flux, ice_final)
```

```python
import functools

import jax
import jax.numpy as jnp
from jax import lax
from jax.experimental import pallas as pl
from jax.experimental.pallas import tpu as pltpu
from jax.sharding import PartitionSpec as P

MESH = pl.DeviceIdType.MESH
F32 = jnp.float32
BF16 = jnp.bfloat16
N_OCN = 8
N_GRP = 16
N_ALL = N_OCN * N_GRP
LAST = N_GRP - 1
L = 32
CHUNKS = 22
PADDED = 32
ITERS = 4


def chunk_of(g):
    return 0 if g == 0 else (CHUNKS - 4 if g == LAST else 3 + g)


def chunks_of(g):
    return 4 if g in (0, LAST) else 1


def landed(ref, sem):
    pltpu.make_async_copy(ref, ref, sem).wait()


def kernel(
    tracers,
    velocity,
    weights,
    blocks,
    counts,
    u_in,
    wind,
    mass,
    strength,
    pre,
    flux,
    ice,
    t_v,
    v_v,
    w_v,
    level0,
    surf,
    codes,
    hits,
    hits_t,
    sel,
    slots_in,
    xs,
    q,
    hx_s,
    hx_r,
    hy_s,
    hy_r,
    u_pad,
    m_r,
    st_r,
    m2,
    st2,
    base,
    gval,
    fval,
    dval,
    fx,
    cbuf,
    crecv,
    dense,
    dense_in,
    local_sem,
    send_sem,
    recv_sem,
    halo_send,
    halo_recv,
):
    o = lax.axis_index("ocn")
    g = lax.axis_index("grp")
    first, last = g == 0, g == LAST
    polar = jnp.logical_or(first, last)
    inner = jnp.logical_and(g > 0, g < LAST)

    def send(src, dst, phase, ocn, grp):
        pltpu.make_async_remote_copy(
            src_ref=src,
            dst_ref=dst,
            send_sem=send_sem.at[phase],
            recv_sem=recv_sem.at[phase],
            device_id={"ocn": ocn, "grp": grp},
            device_id_type=MESH,
        ).start()

    def over_grp(src, dst, phase):
        for i in range(1, N_GRP):
            send(src, dst, phase, o, lax.rem(g + i, N_GRP))

    small = [
        pltpu.make_async_copy(tracers.at[0, 0], level0.at[0], local_sem.at[0]),
        pltpu.make_async_copy(tracers.at[1, 0], level0.at[1], local_sem.at[1]),
        pltpu.make_async_copy(velocity.at[0, 0], level0.at[2], local_sem.at[2]),
        pltpu.make_async_copy(velocity.at[1, 0], level0.at[3], local_sem.at[3]),
    ]
    for copy in small:
        copy.start()
    t_copy = pltpu.make_async_copy(tracers, t_v, local_sem.at[4])
    v_copy = pltpu.make_async_copy(velocity, v_v, local_sem.at[5])
    w_copy = pltpu.make_async_copy(weights.at[pl.ds(4 * o, 4)], w_v, local_sem.at[6])
    t_copy.start()
    w_copy.start()
    v_copy.start()

    barrier = pltpu.get_barrier_semaphore()
    for i in range(1, N_GRP):
        pl.semaphore_signal(
            barrier, inc=1, device_id={"ocn": o, "grp": lax.rem(g + i, N_GRP)}, device_id_type=MESH
        )
    for i in range(1, N_OCN):
        pl.semaphore_signal(
            barrier, inc=1, device_id={"ocn": lax.rem(o + i, N_OCN), "grp": g}, device_id_type=MESH
        )

    def fill_codes(at, count):
        for k in range(2 * count):
            for r in range(4):
                block = blocks[4 * o + r, k]
                code = jnp.where(k < counts[4 * o + r], block, -1)
                codes[at + k // 2, pl.ds((k % 2) * 4 + r, 1), :] = jnp.full((1, 128), code, jnp.int32)

    @pl.when(first)
    def _():
        fill_codes(0, 4)

    @pl.when(last)
    def _():
        fill_codes(CHUNKS - 4, 4)

    @pl.when(inner)
    def _():
        fill_codes(3 + g, 1)

    codes[pl.ds(CHUNKS, PADDED - CHUNKS)] = jnp.full((PADDED - CHUNKS, 8, 128), -1, jnp.int32)
    crecv[pl.ds(CHUNKS, PADDED - CHUNKS)] = jnp.zeros((PADDED - CHUNKS, 24, 128), F32)
    u_pad[0] = jnp.zeros((8, 128), F32)
    u_pad[N_ALL + 1] = jnp.zeros((8, 128), F32)
    u_pad[pl.ds(1 + 8 * g, 8)] = u_in[...]
    m_r[pl.ds(8 * g, 8)] = mass[...]
    st_r[pl.ds(8 * g, 8)] = strength[...]

    @pl.when(o == N_OCN - 1)
    def _():
        hx_r[0] = jnp.zeros((2, L, 128), F32)

    @pl.when(o == 0)
    def _():
        hx_r[1] = jnp.zeros((2, L, 128), F32)

    @pl.when(last)
    def _():
        hy_r[0] = jnp.zeros((2, L, 256), F32)

    @pl.when(first)
    def _():
        hy_r[1] = jnp.zeros((2, L, 256), F32)

    for copy in small:
        copy.wait()
    for f in range(4):
        field = level0[f]
        surf[o, 0:32, f * 128 : (f + 1) * 128] = field[:, 0:128].astype(BF16)
        surf[o, 32:64, f * 128 : (f + 1) * 128] = field[:, 128:256].astype(BF16)
    pl.semaphore_wait(barrier, N_GRP - 1 + N_OCN - 1)

    for i in range(1, N_OCN):
        send(surf.at[o], surf.at[o], 0, lax.rem(o + i, N_OCN), g)

    @pl.when(first)
    def _():
        part = codes.at[pl.ds(0, 4)]
        over_grp(part, part, 1)

    @pl.when(last)
    def _():
        part = codes.at[pl.ds(CHUNKS - 4, 4)]
        over_grp(part, part, 1)

    @pl.when(inner)
    def _():
        part = codes.at[pl.ds(3 + g, 1)]
        over_grp(part, part, 1)

    over_grp(u_in, u_pad.at[pl.ds(1 + 8 * g, 8)], 2)

    t_copy.wait()
    lanes = lax.broadcasted_iota(jnp.int32, (L, 128), 1)
    for t in range(2):
        hy_s[0, t] = t_v[t, :, 0, :]
        hy_s[1, t] = t_v[t, :, 31, :]

        def gather(z, carry, t=t):
            west, east = carry
            tile = t_v[t, z]
            west = jnp.where(lanes == z, pltpu.roll(tile[:, 0:128], z, 1), west)
            east = jnp.where(lanes == z, pltpu.roll(tile[:, 128:256], z + 1, 1), east)
            return west, east

        zero = jnp.zeros((L, 128), F32)
        west, east = lax.fori_loop(0, L, gather, (zero, zero))
        hx_s[0, t] = west
        hx_s[1, t] = east

    def halo(src, dst, which, ocn, grp):
        return pltpu.make_async_remote_copy(
            src_ref=src,
            dst_ref=dst,
            send_sem=halo_send.at[which],
            recv_sem=halo_recv.at[which],
            device_id={"ocn": ocn, "grp": grp},
            device_id_type=MESH,
        )

    halos = (
        (o > 0, o < N_OCN - 1, halo(hx_s.at[0], hx_r.at[0], 0, jnp.maximum(o - 1, 0), g)),
        (o < N_OCN - 1, o > 0, halo(hx_s.at[1], hx_r.at[1], 1, jnp.minimum(o + 1, N_OCN - 1), g)),
        (g > 0, g < LAST, halo(hy_s.at[0], hy_r.at[0], 2, o, jnp.maximum(g - 1, 0))),
        (g < LAST, g > 0, halo(hy_s.at[1], hy_r.at[1], 3, o, jnp.minimum(g + 1, LAST))),
    )
    for sends, _, copy in halos:
        pl.when(sends)(lambda copy=copy: copy.start())

    @pl.when(polar)
    def _():
        landed(codes.at[pl.ds(0, CHUNKS - 4)], recv_sem.at[1])

    @pl.when(inner)
    def _():
        landed(codes.at[pl.ds(0, CHUNKS - 1)], recv_sem.at[1])

    code = codes[...].reshape(PADDED * 8, 128)
    here = jnp.logical_and(code >= 0, ((code >> 6) & (N_GRP - 1)) == g)
    row = ((code >> 10) << 6) + ((code & 1) << 5) + ((code & 63) >> 1)
    row = jnp.where(here, row, -1)
    lane8 = lax.broadcasted_iota(jnp.int32, (CHUNKS * 8, 128), 1)
    for part in range(4):
        hit = row[: CHUNKS * 8] == lane8 + 128 * part
        hits[part] = jnp.where(hit, 1.0, 0.0).astype(BF16)
    row_f = row.astype(F32)
    row_t = jnp.concatenate([row_f[0:128].T[0:1], row_f[128:256].T[0:1]], axis=1)
    for part in range(8):
        ids = lax.broadcasted_iota(jnp.int32, (64, 256), 0).astype(F32) + 64.0 * part
        hits_t[part * 64 : (part + 1) * 64] = jnp.where(ids == row_t, 1.0, 0.0).astype(BF16)

    landed(surf.at[pl.ds(0, N_OCN - 1)], recv_sem.at[0])
    chosen = jnp.zeros((CHUNKS * 8, 512), F32)
    for part in range(4):
        rows = surf[2 * part : 2 * part + 2].reshape(128, 512)
        chosen += jnp.dot(hits[part], rows, preferred_element_type=F32)
    sel[...] = jnp.concatenate(
        [chosen[:, f * 128 : (f + 1) * 128].reshape(CHUNKS, 8, 128) for f in range(4)], axis=1
    ).astype(BF16)
    for d in range(N_GRP):
        part = sel.at[pl.ds(chunk_of(d), chunks_of(d))]

        @pl.when(g != d)
        def _(d=d, part=part):
            send(part, slots_in.at[pl.ds(4 * g, chunks_of(d))], 3, o, d)

        @pl.when(g == d)
        def _(d=d):
            slots_in[4 * d : 4 * d + chunks_of(d)] = sel[chunk_of(d) : chunk_of(d) + chunks_of(d)]

    over_grp(mass, m_r.at[pl.ds(8 * g, 8)], 4)
    over_grp(strength, st_r.at[pl.ds(8 * g, 8)], 5)

    v_copy.wait()
    for _, arrives, copy in halos:
        pl.when(arrives)(lambda copy=copy: copy.wait_recv())
    ys = lax.broadcasted_iota(jnp.int32, (L, 256), 0)
    cols = lax.broadcasted_iota(jnp.int32, (L, 256), 1)

    def stencil(t):
        def level(z, _):
            c = t_v[t, z]
            up = jnp.where(z > 0, t_v[t, jnp.maximum(z - 1, 0)], 0.0)
            down = jnp.where(z < L - 1, t_v[t, jnp.minimum(z + 1, L - 1)], 0.0)
            he = pltpu.roll(hx_r[0, t], 127 - z, 1)
            hw = pltpu.roll(hx_r[1, t], lax.rem(128 - z, 128), 1)
            east = jnp.where(cols == 255, jnp.concatenate([he, he], axis=1), pltpu.roll(c, 255, 1))
            west = jnp.where(cols == 0, jnp.concatenate([hw, hw], axis=1), pltpu.roll(c, 1, 1))
            north = jnp.where(ys == L - 1, hy_r[0, t, pl.ds(z, 1), :], pltpu.roll(c, L - 1, 0))
            south = jnp.where(ys == 0, hy_r[1, t, pl.ds(z, 1), :], pltpu.roll(c, 1, 0))
            pre[t, z] = (
                c
                + 0.2 * (east + west + north + south - 4.0 * c)
                - 0.25 * (v_v[0, z] * (east - west) + v_v[1, z] * (north - south))
                + 0.2 * (up + down - 2.0 * c)
            )
            return 0

        lax.fori_loop(0, L, level, 0)

    stencil(0)

    w_copy.wait()

    def remap(count):
        for c in range(count):
            total = jnp.zeros((32, 128), F32)
            for s in range(N_GRP):
                total += slots_in[4 * s + c].astype(F32)
            xs[c] = total
        for r in range(4):
            out = jnp.zeros((8, 128), F32)
            for k in range(2 * count):
                x = xs[k // 2, pl.ds((k % 2) * 4 + r, 4, stride=8), :]
                x = jnp.concatenate([x, jnp.zeros((4, 128), F32)], axis=0).astype(BF16)
                out += lax.dot_general(x, w_v[r, k], (((1,), (1,)), ((), ())), preferred_element_type=F32)
            q[0, 2 * r : 2 * r + 2] = out[0:2]
            q[1, 2 * r : 2 * r + 2] = out[2:4]

    @pl.when(polar)
    def _():
        landed(slots_in.at[pl.ds(0, 4 * (N_GRP - 1))], recv_sem.at[3])
        remap(4)

    @pl.when(inner)
    def _():
        landed(slots_in.at[pl.ds(0, N_GRP - 1)], recv_sem.at[3])
        remap(1)

    tile = 8 * g + o
    m2[tile, pl.ds(0, 4, stride=2), :] = mass[o]
    m2[tile, pl.ds(1, 4, stride=2), :] = mass[o]
    base[tile] = m2[tile] * u_in[o] + wind[o] + q[1]

    def spread(i, _):
        to = lax.rem(o * N_GRP + g + i, N_ALL)
        send(base.at[tile], base.at[tile], 6, to // N_GRP, lax.rem(to, N_GRP))
        return 0

    lax.fori_loop(1, N_ALL, spread, 0)

    stencil(1)
    landed(u_pad.at[pl.ds(0, 8 * (N_GRP - 1))], recv_sem.at[2])
    landed(m_r.at[pl.ds(0, 8 * (N_GRP - 1))], recv_sem.at[4])
    landed(st_r.at[pl.ds(0, 8 * (N_GRP - 1))], recv_sem.at[5])

    def twice(i, _):
        at = pl.ds(8 * i, 8)
        m2[at, pl.ds(0, 4, stride=2), :] = m_r[at]
        m2[at, pl.ds(1, 4, stride=2), :] = m_r[at]
        st2[at, pl.ds(0, 4, stride=2), :] = st_r[at]
        st2[at, pl.ds(1, 4, stride=2), :] = st_r[at]
        return 0

    lax.fori_loop(0, N_GRP, twice, 0)
    landed(base.at[pl.ds(0, N_ALL - 1)], recv_sem.at[6])

    tiles = 4
    shape = (tiles, 8, 128)
    lane = lax.broadcasted_iota(jnp.int32, shape, 2)
    sub = lax.broadcasted_iota(jnp.int32, shape, 1)

    def dot(a, b):
        return jnp.sum(a * b, axis=0)

    def mean(acc):
        return jnp.sum(jnp.sum(acc, axis=1, keepdims=True), axis=0, keepdims=True) / (2.0 * 65536.0)

    for step in range(ITERS):

        def picard(i, sums, step=step):
            at = pl.ds(tiles * i, tiles)
            u = u_pad[pl.ds(tiles * i + 1, tiles)]
            before = u_pad[pl.ds(tiles * i, tiles)]
            after = u_pad[pl.ds(tiles * i + 2, tiles)]
            up = pltpu.roll(jnp.where(sub >= 6, before, u), 2, 1)
            down = pltpu.roll(jnp.where(sub < 2, after, u), 6, 1)
            left = pltpu.roll(jnp.where(lane == 127, up, u), 1, 2)
            right = pltpu.roll(jnp.where(lane == 0, down, u), 127, 2)
            strain = 0.5 * (right - left)
            square = strain * strain
            other = jnp.where((sub & 1) == 1, pltpu.roll(square, 1, 1), pltpu.roll(square, 7, 1))
            zeta = (0.5 * st2[at]) * lax.rsqrt(square + other + 0.25)
            new = (base[at] + zeta * (left + right)) / (m2[at] + 1.0 + 2.0 * zeta)
            res = new - u
            gval[step, at] = new
            fval[step % 2, at] = res
            if step == 0:
                return sums
            diff = res - fval[(step - 1) % 2, at]
            dval[step - 1, at] = diff
            diffs = [dval[j, at] for j in range(step - 1)] + [diff]
            terms = [dot(d, diff) for d in diffs] + [dot(d, res) for d in diffs]
            return tuple(s + t for s, t in zip(sums, terms))

        zeros = tuple(jnp.zeros((8, 128), F32) for _ in range(2 * step))
        sums = lax.fori_loop(0, N_ALL // tiles, picard, zeros)
        if step == 0:

            def first_update(i, _):
                u_pad[pl.ds(tiles * i + 1, tiles)] = gval[0, pl.ds(tiles * i, tiles)]
                return 0

            lax.fori_loop(0, N_ALL // tiles, first_update, 0)
            gram = {}
            continue
        means = [mean(s) for s in sums]
        for j in range(step):
            gram[(j, step - 1)] = means[j]
        norms = [jnp.sqrt(gram[(j, j)] + 1e-6) for j in range(step)]
        rows = [
            [
                gram[(min(a, b), max(a, b))] / (norms[a] * norms[b]) + (0.1 if a == b else 0.0)
                for b in range(step)
            ]
            + [means[step + a] / norms[a]]
            for a in range(step)
        ]
        for a in range(step):
            for b in range(a + 1, step):
                ratio = rows[b][a] / rows[a][a]
                rows[b] = [y - ratio * x for x, y in zip(rows[a], rows[b])]
        coef = [None] * step
        for a in reversed(range(step)):
            rest = rows[a][step]
            for b in range(a + 1, step):
                rest = rest - rows[a][b] * coef[b]
            coef[a] = rest / rows[a][a]
        scale = [jnp.broadcast_to(c / n, (8, 128))[None] for c, n in zip(coef, norms)]

        def combine(at, step=step, scale=scale):
            values = [gval[j, at] for j in range(step + 1)]
            out = values[step]
            for j in range(step):
                out = out - scale[j] * (values[j + 1] - values[j])
            return out

        if step < ITERS - 1:

            def update(i, _, combine=combine):
                u_pad[pl.ds(tiles * i + 1, tiles)] = combine(pl.ds(tiles * i, tiles))
                return 0

            lax.fori_loop(0, N_ALL // tiles, update, 0)
        else:
            ice[...] = combine(pl.ds(8 * g, 8))

    stress = ice[o] - q[1]
    for r in range(4):
        fx[r] = jnp.zeros((8, 128), F32)
        fx[r, 0:2] = stress[2 * r : 2 * r + 2]
        fx[r, 2:3] = 0.5 * (-0.05 * q[0, 2 * r + 1 : 2 * r + 2] - q[0, 2 * r : 2 * r + 1])

    def contribute(count):
        for r in range(4):
            x = fx[r].astype(BF16)
            for k in range(2 * count):
                out = jnp.dot(x, w_v[r, k], preferred_element_type=F32)
                cbuf[k // 2, pl.ds((k % 2) * 4 + r, 3, stride=8), :] = out[0:3]

    @pl.when(first)
    def _():
        contribute(4)
        over_grp(cbuf, crecv.at[pl.ds(0, 4)], 7)
        crecv[0:4] = cbuf[...]

    @pl.when(last)
    def _():
        contribute(4)
        over_grp(cbuf, crecv.at[pl.ds(CHUNKS - 4, 4)], 7)
        crecv[CHUNKS - 4 : CHUNKS] = cbuf[...]

    @pl.when(inner)
    def _():
        contribute(1)
        over_grp(cbuf.at[pl.ds(0, 1)], crecv.at[pl.ds(3 + g, 1)], 7)
        crecv[pl.ds(3 + g, 1)] = cbuf[0:1]

    @pl.when(polar)
    def _():
        landed(crecv.at[pl.ds(0, CHUNKS - 4)], recv_sem.at[7])

    @pl.when(inner)
    def _():
        landed(crecv.at[pl.ds(0, CHUNKS - 1)], recv_sem.at[7])

    for f in range(3):
        values = crecv[:, 8 * f : 8 * f + 8, :].reshape(PADDED * 8, 128)
        high = values.astype(BF16)
        low = (values - high.astype(F32)).astype(BF16)
        out = jnp.dot(hits_t[...], jnp.concatenate([high, low], axis=1), preferred_element_type=F32)
        out = out[:, 0:128] + out[:, 128:256]
        dense[:, f] = out.reshape(N_OCN, 64, 128)
    for i in range(1, N_OCN):
        to = lax.rem(o + i, N_OCN)
        send(dense.at[to], dense_in.at[o], 8, to, g)
    dense_in[o] = dense[o]
    landed(dense_in.at[pl.ds(0, N_OCN - 1)], recv_sem.at[8])
    for f in range(3):
        out = dense_in[0, f]
        for s in range(1, N_OCN):
            out += dense_in[s, f]
        flux[f, :, 0:128] = out[0:32]
        flux[f, :, 128:256] = out[32:64]

    landed(surf.at[pl.ds(0, N_OCN - 1)], send_sem.at[0])
    landed(u_pad.at[pl.ds(0, 8 * (N_GRP - 1))], send_sem.at[2])
    landed(m_r.at[pl.ds(0, 8 * (N_GRP - 1))], send_sem.at[4])
    landed(st_r.at[pl.ds(0, 8 * (N_GRP - 1))], send_sem.at[5])
    landed(base.at[pl.ds(0, N_ALL - 1)], send_sem.at[6])
    landed(dense_in.at[pl.ds(0, N_OCN - 1)], send_sem.at[8])

    @pl.when(polar)
    def _():
        landed(base.at[pl.ds(0, 4 * (N_GRP - 1))], send_sem.at[1])
        landed(sel.at[pl.ds(0, CHUNKS - 4)], send_sem.at[3])
        landed(gval.at[pl.ds(0, 3), pl.ds(0, 4 * (N_GRP - 1))], send_sem.at[7])

    @pl.when(inner)
    def _():
        landed(base.at[pl.ds(0, N_GRP - 1)], send_sem.at[1])
        landed(sel.at[pl.ds(0, CHUNKS - 1)], send_sem.at[3])
        landed(base.at[pl.ds(0, 3 * (N_GRP - 1))], send_sem.at[7])

    for sends, _, copy in halos:
        pl.when(sends)(lambda copy=copy: copy.wait_send())


def on_device(
    tracers,
    velocity,
    remap_weights,
    remap_blocks,
    remap_count,
    ice_velocity,
    ice_mass_rate,
    ice_strength,
    wind_stress,
):
    def tiled(x):
        return x.reshape(2, 32, 128).transpose(1, 0, 2).reshape(8, 8, 128)

    hbm = pl.BlockSpec(memory_space=pltpu.HBM)
    smem = pl.BlockSpec(memory_space=pltpu.SMEM)
    vmem = pl.BlockSpec(memory_space=pltpu.VMEM)
    scratch = [
        pltpu.VMEM((2, L, 32, 256), F32),
        pltpu.VMEM((2, L, 32, 256), F32),
        pltpu.VMEM((4, 8, 128, 128), BF16),
        pltpu.VMEM((4, 32, 256), F32),
        pltpu.VMEM((N_OCN, 64, 512), BF16),
        pltpu.VMEM((PADDED, 8, 128), jnp.int32),
        pltpu.VMEM((4, CHUNKS * 8, 128), BF16),
        pltpu.VMEM((512, 256), BF16),
        pltpu.VMEM((CHUNKS, 32, 128), BF16),
        pltpu.VMEM((4 * N_GRP, 32, 128), BF16),
        pltpu.VMEM((4, 32, 128), F32),
        pltpu.VMEM((2, 8, 128), F32),
        pltpu.VMEM((2, 2, L, 128), F32),
        pltpu.VMEM((2, 2, L, 128), F32),
        pltpu.VMEM((2, 2, L, 256), F32),
        pltpu.VMEM((2, 2, L, 256), F32),
        pltpu.VMEM((N_ALL + 2, 8, 128), F32),
        pltpu.VMEM((N_ALL, 4, 128), F32),
        pltpu.VMEM((N_ALL, 4, 128), F32),
        pltpu.VMEM((N_ALL, 8, 128), F32),
        pltpu.VMEM((N_ALL, 8, 128), F32),
        pltpu.VMEM((N_ALL, 8, 128), F32),
        pltpu.VMEM((ITERS, N_ALL, 8, 128), F32),
        pltpu.VMEM((2, N_ALL, 8, 128), F32),
        pltpu.VMEM((ITERS - 1, N_ALL, 8, 128), F32),
        pltpu.VMEM((4, 8, 128), F32),
        pltpu.VMEM((4, 24, 128), F32),
        pltpu.VMEM((PADDED, 24, 128), F32),
        pltpu.VMEM((N_OCN, 3, 64, 128), F32),
        pltpu.VMEM((N_OCN, 3, 64, 128), F32),
        pltpu.SemaphoreType.DMA((7,)),
        pltpu.SemaphoreType.DMA((9,)),
        pltpu.SemaphoreType.DMA((9,)),
        pltpu.SemaphoreType.DMA((4,)),
        pltpu.SemaphoreType.DMA((4,)),
    ]
    pre, flux, ice = pl.pallas_call(
        kernel,
        out_shape=(
            jax.ShapeDtypeStruct((2, L, 32, 256), F32),
            jax.ShapeDtypeStruct((3, 32, 256), F32),
            jax.ShapeDtypeStruct((8, 8, 128), F32),
        ),
        in_specs=[hbm, hbm, hbm, smem, smem, vmem, vmem, vmem, vmem],
        out_specs=(vmem, vmem, vmem),
        scratch_shapes=scratch,
        compiler_params=pltpu.CompilerParams(
            collective_id=0, has_side_effects=True, vmem_limit_bytes=40 * 1024 * 1024
        ),
    )(
        tracers,
        velocity,
        remap_weights,
        remap_blocks,
        remap_count,
        tiled(ice_velocity),
        tiled(wind_stress),
        ice_mass_rate.reshape(8, 4, 128),
        ice_strength.reshape(8, 4, 128),
    )
    tracers_next = pre.at[0, 0].add(0.5 * flux[2])
    ice_final = ice.reshape(32, 2, 128).transpose(1, 0, 2).reshape(2, 4096)
    return tracers_next, flux, ice_final


def solution(mesh):
    placed = (
        P(None, None, "grp", "ocn"),
        P(None, None, "grp", "ocn"),
        P("grp", None, None, None),
        P("grp", None),
        P("grp"),
        P(None, "grp"),
        P("grp"),
        P("grp"),
        P(None, "grp"),
    )
    return jax.shard_map(
        on_device,
        mesh=mesh,
        in_specs=placed,
        out_specs=(P(None, None, "grp", "ocn"), P(None, "grp", "ocn"), P(None, "grp")),
        check_vma=False,
    )
```

```python
import functools

import jax
import jax.numpy as jnp
from jax import lax
from jax.experimental import pallas as pl
from jax.experimental.pallas import tpu as pltpu
from jax.sharding import PartitionSpec as P

MESH = pl.DeviceIdType.MESH
F32 = jnp.float32
BF16 = jnp.bfloat16
N_OCN = 8
N_GRP = 16
N_ALL = N_OCN * N_GRP
LAST = N_GRP - 1
L = 32
CHUNKS = 22
PADDED = 32
ITERS = 4
TILES = 4
UNROLL = 8


def chunk_of(g):
    return 0 if g == 0 else (CHUNKS - 4 if g == LAST else 3 + g)


def chunks_of(g):
    return 4 if g in (0, LAST) else 1


def landed(ref, sem, name="left"):
    with jax.named_scope(name):
        pltpu.make_async_copy(ref, ref, sem).wait()


def kernel(
    tracers,
    velocity,
    weights,
    blocks_hbm,
    counts_hbm,
    u_hbm,
    wind_hbm,
    mass_hbm,
    strength_hbm,
    pre,
    flux,
    ice,
    blocks,
    counts,
    u_in,
    wind,
    mass,
    strength,
    t_v,
    v_v,
    w_v,
    level0,
    surf,
    codes,
    hits,
    hits_t,
    sel,
    slots_in,
    xs,
    q,
    hx_s,
    hx_r,
    hy_s,
    hy_r,
    u_r,
    u_pad,
    m_r,
    st_r,
    m2,
    st2,
    base,
    g0_pad,
    g1,
    g2,
    g3,
    f_a,
    f_b,
    d1,
    d2,
    fx,
    cbuf,
    crecv,
    dense,
    pair_in,
    dense_in,
    local_sem,
    send_sem,
    recv_sem,
    halo_send,
    halo_recv,
):
    o = lax.axis_index("ocn")
    g = lax.axis_index("grp")
    first, last = g == 0, g == LAST
    polar = jnp.logical_or(first, last)
    inner = jnp.logical_and(g > 0, g < LAST)
    z, core = o // 2, lax.rem(o, 2)
    partner = o + 1 - 2 * core
    chip = 4 * g + z

    def send(src, dst, phase, ocn, grp):
        pltpu.make_async_remote_copy(
            src_ref=src,
            dst_ref=dst,
            send_sem=send_sem.at[phase],
            recv_sem=recv_sem.at[phase],
            device_id={"ocn": ocn, "grp": grp},
            device_id_type=MESH,
        ).start()

    def over_grp(src, dst, phase):
        for i in range(1, N_GRP):
            send(src, dst, phase, o, lax.rem(g + i, N_GRP))

    small = [
        pltpu.make_async_copy(tracers.at[0, 0], level0.at[0], local_sem.at[0]),
        pltpu.make_async_copy(tracers.at[1, 0], level0.at[1], local_sem.at[1]),
        pltpu.make_async_copy(velocity.at[0, 0], level0.at[2], local_sem.at[2]),
        pltpu.make_async_copy(velocity.at[1, 0], level0.at[3], local_sem.at[3]),
    ]
    for copy in small:
        copy.start()
    index_copies = [
        pltpu.make_async_copy(blocks_hbm, blocks, local_sem.at[7]),
        pltpu.make_async_copy(counts_hbm, counts, local_sem.at[8]),
    ]
    ice_copies = [
        pltpu.make_async_copy(u_hbm, u_in, local_sem.at[9]),
        pltpu.make_async_copy(wind_hbm, wind, local_sem.at[10]),
        pltpu.make_async_copy(mass_hbm, mass, local_sem.at[11]),
        pltpu.make_async_copy(strength_hbm, strength, local_sem.at[12]),
    ]
    for copy in index_copies + ice_copies:
        copy.start()
    t_copy = pltpu.make_async_copy(tracers, t_v, local_sem.at[4])
    v_copy = pltpu.make_async_copy(velocity, v_v, local_sem.at[5])
    w_copy = pltpu.make_async_copy(weights.at[pl.ds(4 * o, 4)], w_v, local_sem.at[6])
    t_copy.start()
    w_copy.start()
    v_copy.start()

    barrier = pltpu.get_barrier_semaphore()
    for i in range(1, N_GRP):
        pl.semaphore_signal(
            barrier, inc=1, device_id={"ocn": o, "grp": lax.rem(g + i, N_GRP)}, device_id_type=MESH
        )
    for i in range(1, N_OCN):
        pl.semaphore_signal(
            barrier, inc=1, device_id={"ocn": lax.rem(o + i, N_OCN), "grp": g}, device_id_type=MESH
        )

    def fill_codes(at, count):
        for k in range(2 * count):
            for r in range(4):
                block = blocks[k, 4 * o + r]
                code = jnp.where(k < counts[4 * o + r], block, -1)
                codes[at + k // 2, pl.ds((k % 2) * 4 + r, 1), :] = jnp.full((1, 128), code, jnp.int32)

    for copy in index_copies:
        copy.wait()

    @pl.when(first)
    def _():
        fill_codes(0, 4)

    @pl.when(last)
    def _():
        fill_codes(CHUNKS - 4, 4)

    @pl.when(inner)
    def _():
        fill_codes(3 + g, 1)

    codes[pl.ds(CHUNKS, PADDED - CHUNKS)] = jnp.full((PADDED - CHUNKS, 8, 128), -1, jnp.int32)
    crecv[pl.ds(CHUNKS, PADDED - CHUNKS)] = jnp.zeros((PADDED - CHUNKS, 24, 128), F32)
    u_pad[0] = jnp.zeros((8, 128), F32)
    u_pad[N_ALL + 1] = jnp.zeros((8, 128), F32)
    for copy in ice_copies:
        copy.wait()
    g0_pad[0] = jnp.zeros((8, 128), F32)
    g0_pad[N_ALL + 1] = jnp.zeros((8, 128), F32)

    @pl.when(core == 0)
    def _():
        u_r[g, z] = u_in[z]

    @pl.when(core == 1)
    def _():
        m_r[g, z] = mass[z]
        st_r[g, z] = strength[z]


    @pl.when(o == N_OCN - 1)
    def _():
        hx_r[0] = jnp.zeros((2, L, 128), F32)

    @pl.when(o == 0)
    def _():
        hx_r[1] = jnp.zeros((2, L, 128), F32)

    @pl.when(last)
    def _():
        hy_r[0] = jnp.zeros((2, L, 256), F32)

    @pl.when(first)
    def _():
        hy_r[1] = jnp.zeros((2, L, 256), F32)

    for copy in small:
        copy.wait()
    for f in range(4):
        field = level0[f]
        surf[o, 0:32, f * 128 : (f + 1) * 128] = field[:, 0:128].astype(BF16)
        surf[o, 32:64, f * 128 : (f + 1) * 128] = field[:, 128:256].astype(BF16)
    with jax.named_scope("barrier"):
        pl.semaphore_wait(barrier, N_GRP - 1 + N_OCN - 1)

    for i in (2, 6, 3, 5, 7, 4, 1):
        send(surf.at[o], surf.at[o], 0, lax.rem(o + i, N_OCN), g)

    @pl.when(first)
    def _():
        part = codes.at[pl.ds(0, 4)]
        over_grp(part, part, 1)

    @pl.when(last)
    def _():
        part = codes.at[pl.ds(CHUNKS - 4, 4)]
        over_grp(part, part, 1)

    @pl.when(inner)
    def _():
        part = codes.at[pl.ds(3 + g, 1)]
        over_grp(part, part, 1)

    @pl.when(core == 0)
    def _():
        over_grp(u_in.at[z], u_r.at[g, z], 2)

    @pl.when(core == 1)
    def _():
        over_grp(mass.at[z], m_r.at[g, z], 2)
        over_grp(strength.at[z], st_r.at[g, z], 2)

    @pl.when(polar)
    def _():
        landed(codes.at[pl.ds(0, CHUNKS - 4)], recv_sem.at[1], "recv1")

    @pl.when(inner)
    def _():
        landed(codes.at[pl.ds(0, CHUNKS - 1)], recv_sem.at[1], "recv1")

    code = codes[...].reshape(PADDED * 8, 128)
    here = jnp.logical_and(code >= 0, ((code >> 6) & (N_GRP - 1)) == g)
    row = ((code >> 10) << 6) + ((code & 1) << 5) + ((code & 63) >> 1)
    row = jnp.where(here, row, -1)
    lane8 = lax.broadcasted_iota(jnp.int32, (CHUNKS * 8, 128), 1)
    for part in range(4):
        hit = row[: CHUNKS * 8] == lane8 + 128 * part
        hits[part] = jnp.where(hit, 1.0, 0.0).astype(BF16)
    row_f = row.astype(F32)
    row_t = jnp.concatenate([row_f[0:128].T[0:1], row_f[128:256].T[0:1]], axis=1)
    for part in range(8):
        ids = lax.broadcasted_iota(jnp.int32, (64, 256), 0).astype(F32) + 64.0 * part
        hits_t[part * 64 : (part + 1) * 64] = jnp.where(ids == row_t, 1.0, 0.0).astype(BF16)

    landed(surf.at[pl.ds(0, N_OCN - 1)], recv_sem.at[0], "recv0")
    chosen = jnp.zeros((CHUNKS * 8, 512), F32)
    for part in range(4):
        rows = surf[2 * part : 2 * part + 2].reshape(128, 512)
        chosen += jnp.dot(hits[part], rows, preferred_element_type=F32)
    sel[...] = jnp.concatenate(
        [chosen[:, f * 128 : (f + 1) * 128].reshape(CHUNKS, 8, 128) for f in range(4)], axis=1
    ).astype(BF16)
    for d in (0, LAST, *range(1, LAST)):
        for c in range(chunks_of(d)):

            @pl.when(g != d)
            def _(d=d, c=c):
                send(sel.at[chunk_of(d) + c], slots_in.at[c, g], (3, 9, 10, 12)[c], o, d)

            @pl.when(g == d)
            def _(d=d, c=c):
                slots_in[c, d] = sel[chunk_of(d) + c]

    mine = ((u_r,), (m_r, st_r))
    landed(u_r.at[pl.ds(0, N_GRP - 1), 0], recv_sem.at[2], "recv2")
    for c in range(2):

        @pl.when(core == c)
        def _(c=c):
            for i in (1, 3, 2):
                for part in mine[c]:
                    send(part.at[:, z], part.at[:, z], 4, 2 * lax.rem(z + i, 4) + core, g)

    with jax.named_scope("t_copy"):
        t_copy.wait()
    lanes = lax.broadcasted_iota(jnp.int32, (L, 128), 1)
    for t in range(2):
        hy_s[0, t] = t_v[t, :, 0, :]
        hy_s[1, t] = t_v[t, :, 31, :]

        def gather(z, carry, t=t):
            west, east = carry
            tile = t_v[t, z]
            west = jnp.where(lanes == z, pltpu.roll(tile[:, 0:128], z, 1), west)
            east = jnp.where(lanes == z, pltpu.roll(tile[:, 128:256], z + 1, 1), east)
            return west, east

        zero = jnp.zeros((L, 128), F32)
        west, east = lax.fori_loop(0, L, gather, (zero, zero), unroll=8)
        hx_s[0, t] = west
        hx_s[1, t] = east

    def halo(src, dst, which, ocn, grp):
        return pltpu.make_async_remote_copy(
            src_ref=src,
            dst_ref=dst,
            send_sem=halo_send.at[which],
            recv_sem=halo_recv.at[which],
            device_id={"ocn": ocn, "grp": grp},
            device_id_type=MESH,
        )

    halos = (
        (o > 0, o < N_OCN - 1, halo(hx_s.at[0], hx_r.at[0], 0, jnp.maximum(o - 1, 0), g)),
        (o < N_OCN - 1, o > 0, halo(hx_s.at[1], hx_r.at[1], 1, jnp.minimum(o + 1, N_OCN - 1), g)),
        (g > 0, g < LAST, halo(hy_s.at[0], hy_r.at[0], 2, o, jnp.maximum(g - 1, 0))),
        (g < LAST, g > 0, halo(hy_s.at[1], hy_r.at[1], 3, o, jnp.minimum(g + 1, LAST))),
    )
    with jax.named_scope("w_copy"):
        w_copy.wait()

    def remap(count):
        out = [jnp.zeros((8, 128), F32)] * 4
        for c in range(count):
            landed(slots_in.at[0, pl.ds(0, N_GRP - 1)], recv_sem.at[(3, 9, 10, 12)[c]], f"recv3_{c}")
            total = jnp.zeros((32, 128), F32)
            for s in range(N_GRP):
                total += slots_in[c, s].astype(F32)
            xs[c] = total
            for r in range(4):
                x = [xs[c, pl.ds(4 * k + r, 4, stride=8), :] for k in range(2)]
                x = jnp.concatenate(x, axis=1)
                x = jnp.concatenate([x, jnp.zeros(x.shape, F32)], axis=0).astype(BF16)
                w = jnp.concatenate([w_v[r, 2 * c + k] for k in range(2)], axis=1)
                out[r] += lax.dot_general(x, w, (((1,), (1,)), ((), ())), preferred_element_type=F32)
        for r in range(4):
            q[0, 2 * r : 2 * r + 2] = out[r][0:2]
            q[1, 2 * r : 2 * r + 2] = out[r][2:4]

    @pl.when(polar)
    def _():
        remap(4)

    @pl.when(inner)
    def _():
        remap(1)

    tile = 8 * g + o
    m2[tile, pl.ds(0, 4, stride=2), :] = mass[z, core]
    m2[tile, pl.ds(1, 4, stride=2), :] = mass[z, core]
    base[tile] = m2[tile] * u_in[z, core] + wind[z, core] + q[1]

    def spread(i, _):
        to = lax.rem(tile + i, N_ALL)
        send(base.at[tile], base.at[tile], 6, lax.rem(to, N_OCN), to // N_OCN)
        return 0

    lax.fori_loop(1, N_ALL, spread, 0)
    for sends, _, copy in halos:
        pl.when(sends)(lambda copy=copy: copy.start())


    landed(u_r.at[:, pl.ds(0, 3)], recv_sem.at[4], "recv4")
    for c in range(2):

        @pl.when(core == c)
        def _(c=c):
            for part in mine[c]:
                send(part, part, 5, partner, g)

    landed(u_r, recv_sem.at[5], "recv5")

    def twice(i, _):
        at = pl.ds(8 * i, 8)
        u_pad[pl.ds(8 * i + 1, 8)] = u_r[i].reshape(8, 8, 128)
        for to, part in ((m2, m_r), (st2, st_r)):
            once = part[i].reshape(8, 4, 128)
            to[at, pl.ds(0, 4, stride=2), :] = once
            to[at, pl.ds(1, 4, stride=2), :] = once
        return 0

    lax.fori_loop(0, N_GRP, twice, 0)
    landed(base.at[pl.ds(0, N_ALL - 1)], recv_sem.at[6], "recv6")

    tiles = TILES
    shape = (tiles, 8, 128)
    lane = lax.broadcasted_iota(jnp.int32, shape, 2)
    sub = lax.broadcasted_iota(jnp.int32, shape, 1)

    def dot(a, b):
        return jnp.sum(a * b, axis=0)

    def mean(acc):
        return jnp.sum(jnp.sum(acc, axis=1, keepdims=True), axis=0, keepdims=True) / (2.0 * 65536.0)

    us = (u_pad, g0_pad, u_pad, u_pad)
    fs = (f_a, f_b, f_a, None)
    ds = (None, d1, d2, None)
    gram = {}

    def g_at(k, i):
        return g0_pad[pl.ds(tiles * i + 1, tiles)] if k == 0 else (None, g1, g2, g3)[k][pl.ds(tiles * i, tiles)]

    for step in range(ITERS):

        def picard(i, sums, step=step):
            at = pl.ds(tiles * i, tiles)
            src = us[step]
            u = src[pl.ds(tiles * i + 1, tiles)]
            before = src[pl.ds(tiles * i, tiles)]
            after = src[pl.ds(tiles * i + 2, tiles)]
            up = pltpu.roll(jnp.where(sub >= 6, before, u), 2, 1)
            down = pltpu.roll(jnp.where(sub < 2, after, u), 6, 1)
            left = pltpu.roll(jnp.where(lane == 127, up, u), 1, 2)
            right = pltpu.roll(jnp.where(lane == 0, down, u), 127, 2)
            strain = 0.5 * (right - left)
            square = strain * strain
            other = jnp.where((sub & 1) == 1, pltpu.roll(square, 1, 1), pltpu.roll(square, 7, 1))
            zeta = (0.5 * st2[at]) * lax.rsqrt(square + other + 0.25)
            force = base[at]
            new = (force + zeta * (left + right)) / (m2[at] + 1.0 + 2.0 * zeta)
            res = new - u
            if step == 0:
                g0_pad[pl.ds(tiles * i + 1, tiles)] = new
                fs[0][at] = res
                return sums
            (None, g1, g2, g3)[step][at] = new
            diff = res - fs[step - 1][at]
            if step < ITERS - 1:
                fs[step][at] = res
                ds[step][at] = diff
            diffs = [ds[j][at] for j in range(1, step)] + [diff]
            terms = [dot(d, diff) for d in diffs] + [dot(d, res) for d in diffs]
            return tuple(s + t for s, t in zip(sums, terms))

        zeros = tuple(jnp.zeros((8, 128), F32) for _ in range(2 * step))
        with jax.named_scope(f"picard{step}"):
            sums = lax.fori_loop(0, N_ALL // tiles, picard, zeros, unroll=UNROLL)
        if step == 0:
            continue
        means = [mean(s) for s in sums]
        for j in range(step):
            gram[(j, step - 1)] = means[j]
        norms = [jnp.sqrt(gram[(j, j)] + 1e-6) for j in range(step)]
        rows = [
            [
                gram[(min(a, b), max(a, b))] / (norms[a] * norms[b]) + (0.1 if a == b else 0.0)
                for b in range(step)
            ]
            + [means[step + a] / norms[a]]
            for a in range(step)
        ]
        for a in range(step):
            for b in range(a + 1, step):
                ratio = rows[b][a] / rows[a][a]
                rows[b] = [y - ratio * x for x, y in zip(rows[a], rows[b])]
        coef = [None] * step
        for a in reversed(range(step)):
            rest = rows[a][step]
            for b in range(a + 1, step):
                rest = rest - rows[a][b] * coef[b]
            coef[a] = rest / rows[a][a]
        scale = [jnp.broadcast_to(c / n, (8, 128))[None] for c, n in zip(coef, norms)]

        def combine(i, step=step, scale=scale):
            values = [g_at(j, i) for j in range(step + 1)]
            out = values[step]
            for j in range(step):
                out = out - scale[j] * (values[j + 1] - values[j])
            return out

        if step < ITERS - 1:

            def update(i, _, combine=combine):
                u_pad[pl.ds(tiles * i + 1, tiles)] = combine(i)
                return 0

            with jax.named_scope(f"update{step}"):
                lax.fori_loop(0, N_ALL // tiles, update, 0, unroll=UNROLL)
        else:
            for i in range(8 // tiles):
                ice[tiles * i : tiles * (i + 1)] = combine(8 // tiles * g + i)

    stress = ice[o] - q[1]
    for r in range(4):
        fx[r] = jnp.zeros((8, 128), F32)
        fx[r, 0:2] = stress[2 * r : 2 * r + 2]
        fx[r, 2:3] = 0.5 * (-0.05 * q[0, 2 * r + 1 : 2 * r + 2] - q[0, 2 * r : 2 * r + 1])

    def contribute(count):
        for r in range(4):
            x = fx[r].astype(BF16)
            w = jnp.concatenate([w_v[r, k] for k in range(2 * count)], axis=1)
            out = jnp.dot(x, w, preferred_element_type=F32)
            for k in range(2 * count):
                cbuf[k // 2, pl.ds((k % 2) * 4 + r, 3, stride=8), :] = out[0:3, 128 * k : 128 * (k + 1)]

    @pl.when(first)
    def _():
        contribute(4)
        over_grp(cbuf, crecv.at[pl.ds(0, 4)], 7)
        crecv[0:4] = cbuf[...]

    @pl.when(last)
    def _():
        contribute(4)
        over_grp(cbuf, crecv.at[pl.ds(CHUNKS - 4, 4)], 7)
        crecv[CHUNKS - 4 : CHUNKS] = cbuf[...]

    @pl.when(inner)
    def _():
        contribute(1)
        over_grp(cbuf.at[pl.ds(0, 1)], crecv.at[pl.ds(3 + g, 1)], 7)
        crecv[pl.ds(3 + g, 1)] = cbuf[0:1]

    with jax.named_scope("v_copy"):
        v_copy.wait()
    with jax.named_scope("halos"):
        for _, arrives, copy in halos:
            pl.when(arrives)(lambda copy=copy: copy.wait_recv())
    ys = lax.broadcasted_iota(jnp.int32, (L, 256), 0)
    cols = lax.broadcasted_iota(jnp.int32, (L, 256), 1)

    def stencil(t):
        def level(z, _):
            c = t_v[t, z]
            up = jnp.where(z > 0, t_v[t, jnp.maximum(z - 1, 0)], 0.0)
            down = jnp.where(z < L - 1, t_v[t, jnp.minimum(z + 1, L - 1)], 0.0)
            he = pltpu.roll(hx_r[0, t], 127 - z, 1)
            hw = pltpu.roll(hx_r[1, t], lax.rem(128 - z, 128), 1)
            east = jnp.where(cols == 255, jnp.concatenate([he, he], axis=1), pltpu.roll(c, 255, 1))
            west = jnp.where(cols == 0, jnp.concatenate([hw, hw], axis=1), pltpu.roll(c, 1, 1))
            north = jnp.where(ys == L - 1, hy_r[0, t, pl.ds(z, 1), :], pltpu.roll(c, L - 1, 0))
            south = jnp.where(ys == 0, hy_r[1, t, pl.ds(z, 1), :], pltpu.roll(c, 1, 0))
            pre[t, z] = (
                c
                + 0.2 * (east + west + north + south - 4.0 * c)
                - 0.25 * (v_v[0, z] * (east - west) + v_v[1, z] * (north - south))
                + 0.2 * (up + down - 2.0 * c)
            )
            return 0

        lax.fori_loop(0, L, level, 0)

    with jax.named_scope("stencil0"):
        stencil(0)

    @pl.when(polar)
    def _():
        landed(crecv.at[pl.ds(0, CHUNKS - 4)], recv_sem.at[7], "recv7")

    @pl.when(inner)
    def _():
        landed(crecv.at[pl.ds(0, CHUNKS - 1)], recv_sem.at[7], "recv7")

    for f in range(3):
        values = crecv[:, 8 * f : 8 * f + 8, :].reshape(PADDED * 8, 128)
        high = values.astype(BF16)
        low = (values - high.astype(F32)).astype(BF16)
        out = jnp.dot(hits_t[...], jnp.concatenate([high, low], axis=1), preferred_element_type=F32)
        out = out[:, 0:128] + out[:, 128:256]
        out = out.reshape(4, 2, 64, 128)
        dense[0, :, f] = out[:, 0]
        dense[1, :, f] = out[:, 1]
    send(dense.at[1 - core], pair_in, 8, partner, g)
    landed(pair_in, recv_sem.at[8], "recv8")
    pair_in[...] = pair_in[...] + dense[core]
    for i in (1, 3, 2):
        to = lax.rem(z + i, 4)
        send(pair_in.at[to], dense_in.at[z], 11, 2 * to + core, g)
    dense_in[z] = pair_in[z]
    with jax.named_scope("stencil1"):
        stencil(1)
    landed(dense_in.at[pl.ds(0, 3)], recv_sem.at[11], "recv11")
    for f in range(3):
        out = dense_in[0, f] + dense_in[1, f] + dense_in[2, f] + dense_in[3, f]
        flux[f, :, 0:128] = out[0:32]
        flux[f, :, 128:256] = out[32:64]

    landed(surf.at[pl.ds(0, N_OCN - 1)], send_sem.at[0])
    landed(base.at[pl.ds(0, N_ALL - 1)], send_sem.at[6])
    landed(pair_in, send_sem.at[8])
    landed(dense_in.at[pl.ds(0, 3)], send_sem.at[11])

    landed(u_r.at[pl.ds(0, N_GRP - 1), 0], send_sem.at[2])
    landed(u_r.at[:, pl.ds(0, 3)], send_sem.at[4])
    landed(u_r, send_sem.at[5])

    @pl.when(polar)
    def _():
        landed(g1.at[pl.ds(0, 4 * (N_GRP - 1))], send_sem.at[1])
        landed(sel.at[pl.ds(0, 15)], send_sem.at[3])
        for phase in (9, 10, 12):
            landed(sel.at[0], send_sem.at[phase])
        landed(t_v.at[0, pl.ds(0, 30), 0:24], send_sem.at[7])

    @pl.when(inner)
    def _():
        landed(g1.at[pl.ds(0, N_GRP - 1)], send_sem.at[1])
        landed(sel.at[pl.ds(0, 15)], send_sem.at[3])
        for phase in (9, 10, 12):
            landed(sel.at[pl.ds(0, 2)], send_sem.at[phase])
        landed(g1.at[pl.ds(0, 3 * (N_GRP - 1))], send_sem.at[7])

    for sends, _, copy in halos:
        pl.when(sends)(lambda copy=copy: copy.wait_send())


def finish(pre, flux, ice, tracers_out, flux_out, ice_out, top, sem):
    copies = [
        pltpu.make_async_copy(pre.at[1], tracers_out.at[1], sem.at[0]),
        pltpu.make_async_copy(pre.at[0, pl.ds(1, L - 1)], tracers_out.at[0, pl.ds(1, L - 1)], sem.at[1]),
        pltpu.make_async_copy(flux, flux_out, sem.at[2]),
        pltpu.make_async_copy(ice, ice_out, sem.at[3]),
    ]
    for copy in copies:
        copy.start()
    top[...] = pre[0, 0] + 0.5 * flux[2]
    last = pltpu.make_async_copy(top, tracers_out.at[0, 0], sem.at[4])
    last.start()
    for copy in copies + [last]:
        copy.wait()


def on_device(
    tracers,
    velocity,
    remap_weights,
    remap_blocks,
    remap_count,
    ice_velocity,
    ice_mass_rate,
    ice_strength,
    wind_stress,
):
    def tiled(x):
        return x.reshape(2, 32, 128).transpose(1, 0, 2).reshape(4, 2, 8, 128)

    hbm = pl.BlockSpec(memory_space=pltpu.HBM)
    smem = pl.BlockSpec(memory_space=pltpu.SMEM)
    vmem = pl.BlockSpec(memory_space=pltpu.VMEM)
    scratch = [
        pltpu.SMEM((8, 32), jnp.int32),
        pltpu.SMEM((32,), jnp.int32),
        pltpu.VMEM((4, 2, 8, 128), F32),
        pltpu.VMEM((4, 2, 8, 128), F32),
        pltpu.VMEM((4, 2, 4, 128), F32),
        pltpu.VMEM((4, 2, 4, 128), F32),
        pltpu.VMEM((2, L, 32, 256), F32),
        pltpu.VMEM((2, L, 32, 256), F32),
        pltpu.VMEM((4, 8, 128, 128), BF16),
        pltpu.VMEM((4, 32, 256), F32),
        pltpu.VMEM((N_OCN, 64, 512), BF16),
        pltpu.VMEM((PADDED, 8, 128), jnp.int32),
        pltpu.VMEM((4, CHUNKS * 8, 128), BF16),
        pltpu.VMEM((512, 256), BF16),
        pltpu.VMEM((CHUNKS, 32, 128), BF16),
        pltpu.VMEM((4, N_GRP, 32, 128), BF16),
        pltpu.VMEM((4, 32, 128), F32),
        pltpu.VMEM((2, 8, 128), F32),
        pltpu.VMEM((2, 2, L, 128), F32),
        pltpu.VMEM((2, 2, L, 128), F32),
        pltpu.VMEM((2, 2, L, 256), F32),
        pltpu.VMEM((2, 2, L, 256), F32),
        pltpu.VMEM((N_GRP, 4, 2, 8, 128), F32),
        pltpu.VMEM((N_ALL + 2, 8, 128), F32),
        pltpu.VMEM((N_GRP, 4, 2, 4, 128), F32),
        pltpu.VMEM((N_GRP, 4, 2, 4, 128), F32),
        pltpu.VMEM((N_ALL, 8, 128), F32),
        pltpu.VMEM((N_ALL, 8, 128), F32),
        pltpu.VMEM((N_ALL, 8, 128), F32),
        pltpu.VMEM((N_ALL + 2, 8, 128), F32),
        *[pltpu.VMEM((N_ALL, 8, 128), F32)] * 7,
        pltpu.VMEM((4, 8, 128), F32),
        pltpu.VMEM((4, 24, 128), F32),
        pltpu.VMEM((PADDED, 24, 128), F32),
        pltpu.VMEM((2, 4, 3, 64, 128), F32),
        pltpu.VMEM((4, 3, 64, 128), F32),
        pltpu.VMEM((4, 3, 64, 128), F32),
        pltpu.SemaphoreType.DMA((16,)),
        pltpu.SemaphoreType.DMA((13,)),
        pltpu.SemaphoreType.DMA((13,)),
        pltpu.SemaphoreType.DMA((4,)),
        pltpu.SemaphoreType.DMA((4,)),
    ]
    pre, flux, ice = pl.pallas_call(
        kernel,
        out_shape=(
            jax.ShapeDtypeStruct((2, L, 32, 256), F32),
            jax.ShapeDtypeStruct((3, 32, 256), F32),
            jax.ShapeDtypeStruct((8, 8, 128), F32),
        ),
        in_specs=[hbm] * 9,
        out_specs=(vmem, vmem, vmem),
        scratch_shapes=scratch,
        compiler_params=pltpu.CompilerParams(
            collective_id=0, has_side_effects=True, vmem_limit_bytes=40 * 1024 * 1024
        ),
    )(
        *(
            pltpu.with_memory_space_constraint(x, pltpu.HBM)
            for x in (
                tracers,
                velocity,
                remap_weights,
                remap_blocks.T,
                remap_count,
                tiled(ice_velocity),
                tiled(wind_stress),
                ice_mass_rate.reshape(4, 2, 4, 128),
                ice_strength.reshape(4, 2, 4, 128),
            )
        )
    )
    tracers_next, flux, ice = pl.pallas_call(
        finish,
        out_shape=(
            jax.ShapeDtypeStruct((2, L, 32, 256), F32),
            jax.ShapeDtypeStruct((3, 32, 256), F32),
            jax.ShapeDtypeStruct((8, 8, 128), F32),
        ),
        in_specs=[vmem] * 3,
        out_specs=(hbm, hbm, hbm),
        scratch_shapes=[pltpu.VMEM((32, 256), F32), pltpu.SemaphoreType.DMA((5,))],
        compiler_params=pltpu.CompilerParams(vmem_limit_bytes=8 * 1024 * 1024),
    )(pre, flux, ice)
    ice_final = ice.reshape(32, 2, 128).transpose(1, 0, 2).reshape(2, 4096)
    return tracers_next, flux, ice_final


def solution(mesh):
    placed = (
        P(None, None, "grp", "ocn"),
        P(None, None, "grp", "ocn"),
        P("grp", None, None, None),
        P("grp", None),
        P("grp"),
        P(None, "grp"),
        P("grp"),
        P("grp"),
        P(None, "grp"),
    )
    return jax.shard_map(
        on_device,
        mesh=mesh,
        in_specs=placed,
        out_specs=(P(None, None, "grp", "ocn"), P(None, "grp", "ocn"), P(None, "grp")),
        check_vma=False,
    )
```

```python
import functools

import jax
import jax.numpy as jnp
from jax import lax
from jax.experimental import pallas as pl
from jax.experimental.pallas import tpu as pltpu
from jax.sharding import PartitionSpec as P

MESH = pl.DeviceIdType.MESH
F32 = jnp.float32
BF16 = jnp.bfloat16
N_OCN = 8
N_GRP = 16
N_ALL = N_OCN * N_GRP
LAST = N_GRP - 1
L = 32
CHUNKS = 22
PADDED = 32
PLANES_1, PLANES_4 = 4, 14
PLANES = 2 * PLANES_4 + (N_GRP - 2) * PLANES_1
ITERS = 4
TILES = 4
UNROLL = 8


def hops(*shifts):
    return sum(min(i, 4 - i) for i in shifts)


FAR_GRP = sorted(range(1, N_GRP), key=lambda i: -hops(i // 4, i % 4))
FAR_ALL = sorted(range(1, N_ALL), key=lambda i: (i * 37) % 128)


def chunk_of(g):
    return 0 if g == 0 else (CHUNKS - 4 if g == LAST else 3 + g)


def chunks_of(g):
    return 4 if g in (0, LAST) else 1


def power(x):
    return jnp.exp2(0.125 * x).astype(BF16).astype(F32)


def eighths(x):
    top = jnp.max(jnp.abs(x), axis=-1, keepdims=True)
    return jnp.ceil(8.0 * jnp.log2(jnp.maximum(top * (1.0 / 32000.0), 1e-37)))


def counted(x, step):
    return jnp.floor(x * (1.0 / step) + 0.5).astype(jnp.int32).astype(jnp.int16)


def halves(x):
    high = x.astype(BF16)
    return jnp.concatenate([high, (x - high.astype(F32)).astype(BF16)], axis=-1)


def landed(ref, sem, name="left"):
    with jax.named_scope(name):
        pltpu.make_async_copy(ref, ref, sem).wait()


def kernel(
    tracers,
    velocity,
    weights,
    blocks_hbm,
    counts_hbm,
    u_hbm,
    wind_hbm,
    mass_hbm,
    strength_hbm,
    pre,
    flux,
    ice,
    blocks,
    counts,
    u_in,
    wind,
    mass,
    strength,
    t_v,
    v_v,
    w_v,
    level0,
    surf,
    codes,
    hits,
    hits_t,
    sel,
    slots_in,
    xs,
    q,
    hx_s,
    hx_r,
    hy_s,
    hy_r,
    u_r,
    u_pad,
    m_r,
    st_r,
    m2,
    st2,
    base,
    g0_pad,
    g1,
    g2,
    g3,
    f_a,
    f_b,
    d1,
    d2,
    fx,
    cbuf,
    cq,
    crecv,
    dense,
    pair_in,
    pair_q,
    dense_in,
    pair_steps,
    dense_steps,
    local_sem,
    send_sem,
    recv_sem,
    halo_send,
    halo_recv,
):
    o = lax.axis_index("ocn")
    g = lax.axis_index("grp")
    z, core = o // 2, lax.rem(o, 2)
    partner = o + 1 - 2 * core
    first, last = g == 0, g == LAST
    polar = jnp.logical_or(first, last)
    inner = jnp.logical_and(g > 0, g < LAST)

    def send(src, dst, phase, ocn, grp):
        pltpu.make_async_remote_copy(
            src_ref=src,
            dst_ref=dst,
            send_sem=send_sem.at[phase],
            recv_sem=recv_sem.at[phase],
            device_id={"ocn": ocn, "grp": grp},
            device_id_type=MESH,
        ).start()

    gx, gy = g // 4, lax.rem(g, 4)
    to_x = [lax.rem(gx + i, 4) for i in range(4)]
    to_y = [lax.rem(gy + i, 4) for i in range(4)]
    to_o = [2 * lax.rem(z + i, 4) + (core if c == 0 else 1 - core) for i in range(4) for c in range(2)]
    to_g = [4 * to_x[i] + to_y[j] for i in range(4) for j in range(4)]

    def over_grp(src, dst, phase):
        for i in FAR_GRP:
            send(src, dst, phase, o, to_g[i])

    barrier = pltpu.get_barrier_semaphore()
    for i in range(1, N_GRP):
        pl.semaphore_signal(
            barrier, inc=1, device_id={"ocn": o, "grp": lax.rem(g + i, N_GRP)}, device_id_type=MESH
        )
    for i in range(1, N_OCN):
        pl.semaphore_signal(
            barrier, inc=1, device_id={"ocn": lax.rem(o + i, N_OCN), "grp": g}, device_id_type=MESH
        )

    small = [
        pltpu.make_async_copy(tracers.at[0, 0], level0.at[0], local_sem.at[0]),
        pltpu.make_async_copy(tracers.at[1, 0], level0.at[1], local_sem.at[1]),
        pltpu.make_async_copy(velocity.at[0, 0], level0.at[2], local_sem.at[2]),
        pltpu.make_async_copy(velocity.at[1, 0], level0.at[3], local_sem.at[3]),
    ]
    for copy in small:
        copy.start()
    index_copies = [
        pltpu.make_async_copy(blocks_hbm, blocks, local_sem.at[7]),
        pltpu.make_async_copy(counts_hbm, counts, local_sem.at[8]),
    ]
    ice_copies = [
        pltpu.make_async_copy(u_hbm, u_in, local_sem.at[9]),
        pltpu.make_async_copy(wind_hbm, wind, local_sem.at[10]),
        pltpu.make_async_copy(mass_hbm, mass, local_sem.at[11]),
        pltpu.make_async_copy(strength_hbm, strength, local_sem.at[12]),
    ]
    for copy in index_copies + ice_copies:
        copy.start()
    t_copy = pltpu.make_async_copy(tracers, t_v, local_sem.at[4])
    v_copy = pltpu.make_async_copy(velocity, v_v, local_sem.at[5])
    w_copy = pltpu.make_async_copy(weights.at[pl.ds(4 * o, 4)], w_v, local_sem.at[6])
    t_copy.start()
    w_copy.start()
    v_copy.start()

    def fill_codes(at, count):
        for k in range(2 * count):
            for r in range(4):
                block = blocks[k, 4 * o + r]
                code = jnp.where(k < counts[4 * o + r], block, -1)
                codes[at + k // 2, pl.ds((k % 2) * 4 + r, 1), :] = jnp.full((1, 128), code, jnp.int32)

    for copy in index_copies:
        copy.wait()

    @pl.when(first)
    def _():
        fill_codes(0, 4)

    @pl.when(last)
    def _():
        fill_codes(CHUNKS - 4, 4)

    @pl.when(inner)
    def _():
        fill_codes(3 + g, 1)

    codes[pl.ds(CHUNKS, PADDED - CHUNKS)] = jnp.full((PADDED - CHUNKS, 8, 128), -1, jnp.int32)
    u_pad[0] = jnp.zeros((8, 128), F32)
    u_pad[N_ALL + 1] = jnp.zeros((8, 128), F32)
    for copy in ice_copies:
        copy.wait()
    g0_pad[0] = jnp.zeros((8, 128), F32)
    g0_pad[N_ALL + 1] = jnp.zeros((8, 128), F32)

    @pl.when(core == 0)
    def _():
        u_r[g, z] = u_in[z]

    @pl.when(core == 1)
    def _():
        m_r[g, z] = mass[z]
        st_r[g, z] = strength[z]


    @pl.when(o == N_OCN - 1)
    def _():
        hx_r[0] = jnp.zeros((2, L, 128), F32)

    @pl.when(o == 0)
    def _():
        hx_r[1] = jnp.zeros((2, L, 128), F32)

    @pl.when(last)
    def _():
        hy_r[0] = jnp.zeros((2, L, 256), F32)

    @pl.when(first)
    def _():
        hy_r[1] = jnp.zeros((2, L, 256), F32)

    for copy in small:
        copy.wait()
    for f in range(4):
        field = level0[f]
        surf[o, 0:32, f * 128 : (f + 1) * 128] = field[:, 0:128].astype(BF16)
        surf[o, 32:64, f * 128 : (f + 1) * 128] = field[:, 128:256].astype(BF16)
    with jax.named_scope("barrier"):
        pl.semaphore_wait(barrier, N_GRP - 1 + N_OCN - 1)

    for i in (2, 6, 3, 5, 7, 4, 1):
        send(surf.at[o], surf.at[o], 0, lax.rem(o + i, N_OCN), g)

    @pl.when(first)
    def _():
        part = codes.at[pl.ds(0, 4)]
        over_grp(part, part, 1)

    @pl.when(last)
    def _():
        part = codes.at[pl.ds(CHUNKS - 4, 4)]
        over_grp(part, part, 1)

    @pl.when(inner)
    def _():
        part = codes.at[pl.ds(3 + g, 1)]
        over_grp(part, part, 1)

    @pl.when(core == 0)
    def _():
        over_grp(u_in.at[z], u_r.at[g, z], 2)

    @pl.when(core == 1)
    def _():
        over_grp(mass.at[z], m_r.at[g, z], 2)
        over_grp(strength.at[z], st_r.at[g, z], 2)

    @pl.when(polar)
    def _():
        landed(codes.at[pl.ds(0, CHUNKS - 4)], recv_sem.at[1], "recv1")

    @pl.when(inner)
    def _():
        landed(codes.at[pl.ds(0, CHUNKS - 1)], recv_sem.at[1], "recv1")

    code = codes[...].reshape(PADDED * 8, 128)
    here = jnp.logical_and(code >= 0, ((code >> 6) & (N_GRP - 1)) == g)
    row = ((code >> 10) << 6) + ((code & 1) << 5) + ((code & 63) >> 1)
    row = jnp.where(here, row, -1)
    lane8 = lax.broadcasted_iota(jnp.int32, (CHUNKS * 8, 128), 1)
    for part in range(4):
        hit = row[: CHUNKS * 8] == lane8 + 128 * part
        hits[part] = jnp.where(hit, 1.0, 0.0).astype(BF16)
    row_f = row.astype(F32)
    row_t = jnp.concatenate([row_f[0:128].T[0:1], row_f[128:256].T[0:1]], axis=1)
    for part in range(8):
        ids = lax.broadcasted_iota(jnp.int32, (64, 256), 0).astype(F32) + 64.0 * part
        hits_t[part * 64 : (part + 1) * 64] = jnp.where(ids == row_t, 1.0, 0.0).astype(BF16)

    landed(surf.at[pl.ds(0, N_OCN - 1)], recv_sem.at[0], "recv0")
    chosen = jnp.zeros((CHUNKS * 8, 512), F32)
    for part in range(4):
        rows = surf[2 * part : 2 * part + 2].reshape(128, 512)
        chosen += jnp.dot(hits[part], rows, preferred_element_type=F32)
    sel[...] = jnp.concatenate(
        [chosen[:, f * 128 : (f + 1) * 128].reshape(CHUNKS, 8, 128) for f in range(4)], axis=1
    ).astype(BF16)
    for d in (0, LAST, *range(1, LAST)):
        for c in range(chunks_of(d)):

            @pl.when(g != d)
            def _(d=d, c=c):
                send(sel.at[chunk_of(d) + c], slots_in.at[c, g], (3, 9, 10, 12)[c], o, d)

            @pl.when(g == d)
            def _(d=d, c=c):
                slots_in[c, d] = sel[chunk_of(d) + c]

    mine = ((u_r,), (m_r, st_r))
    landed(u_r.at[pl.ds(0, N_GRP - 1), 0], recv_sem.at[2], "recv2")
    for c in range(2):

        @pl.when(core == c)
        def _(c=c):
            for i in (1, 3, 2):
                for part in mine[c]:
                    send(part.at[:, z], part.at[:, z], 4, 2 * lax.rem(z + i, 4) + core, g)

    with jax.named_scope("t_copy"):
        t_copy.wait()
    lanes = lax.broadcasted_iota(jnp.int32, (L, 128), 1)
    for t in range(2):
        hy_s[0, t] = t_v[t, :, 0, :]
        hy_s[1, t] = t_v[t, :, 31, :]

        def gather(z, carry, t=t):
            west, east = carry
            tile = t_v[t, z]
            west = jnp.where(lanes == z, pltpu.roll(tile[:, 0:128], z, 1), west)
            east = jnp.where(lanes == z, pltpu.roll(tile[:, 128:256], z + 1, 1), east)
            return west, east

        zero = jnp.zeros((L, 128), F32)
        west, east = lax.fori_loop(0, L, gather, (zero, zero), unroll=8)
        hx_s[0, t] = west
        hx_s[1, t] = east

    def halo(src, dst, which, ocn, grp):
        return pltpu.make_async_remote_copy(
            src_ref=src,
            dst_ref=dst,
            send_sem=halo_send.at[which],
            recv_sem=halo_recv.at[which],
            device_id={"ocn": ocn, "grp": grp},
            device_id_type=MESH,
        )

    halos = (
        (o > 0, o < N_OCN - 1, halo(hx_s.at[0], hx_r.at[0], 0, jnp.maximum(o - 1, 0), g)),
        (o < N_OCN - 1, o > 0, halo(hx_s.at[1], hx_r.at[1], 1, jnp.minimum(o + 1, N_OCN - 1), g)),
        (g > 0, g < LAST, halo(hy_s.at[0], hy_r.at[0], 2, o, jnp.maximum(g - 1, 0))),
        (g < LAST, g > 0, halo(hy_s.at[1], hy_r.at[1], 3, o, jnp.minimum(g + 1, LAST))),
    )
    with jax.named_scope("w_copy"):
        w_copy.wait()

    def remap(count):
        out = [jnp.zeros((8, 128), F32)] * 4
        for c in range(count):
            landed(slots_in.at[0, pl.ds(0, N_GRP - 1)], recv_sem.at[(3, 9, 10, 12)[c]], f"recv3_{c}")
            total = jnp.zeros((32, 128), F32)
            for s in range(N_GRP):
                total += slots_in[c, s].astype(F32)
            xs[c] = total
            for r in range(4):
                x = [xs[c, pl.ds(4 * k + r, 4, stride=8), :] for k in range(2)]
                x = jnp.concatenate(x, axis=1)
                x = jnp.concatenate([x, jnp.zeros(x.shape, F32)], axis=0).astype(BF16)
                w = jnp.concatenate([w_v[r, 2 * c + k] for k in range(2)], axis=1)
                out[r] += lax.dot_general(x, w, (((1,), (1,)), ((), ())), preferred_element_type=F32)
        for r in range(4):
            q[0, 2 * r : 2 * r + 2] = out[r][0:2]
            q[1, 2 * r : 2 * r + 2] = out[r][2:4]

    @pl.when(polar)
    def _():
        remap(4)

    @pl.when(inner)
    def _():
        remap(1)

    tile = 8 * g + o
    m2[tile, pl.ds(0, 4, stride=2), :] = mass[z, core]
    m2[tile, pl.ds(1, 4, stride=2), :] = mass[z, core]
    base[tile] = m2[tile] * u_in[z, core] + wind[z, core] + q[1]

    for i in FAR_ALL:
        send(base.at[tile], base.at[tile], 6, to_o[i % 8], to_g[i // 8])
    for sends, _, copy in halos:
        pl.when(sends)(lambda copy=copy: copy.start())


    landed(u_r.at[:, pl.ds(0, 3)], recv_sem.at[4], "recv4")
    for c in range(2):

        @pl.when(core == c)
        def _(c=c):
            for part in mine[c]:
                send(part, part, 5, partner, g)

    landed(u_r, recv_sem.at[5], "recv5")

    def twice(i, _):
        at = pl.ds(8 * i, 8)
        u_pad[pl.ds(8 * i + 1, 8)] = u_r[i].reshape(8, 8, 128)
        for to, part in ((m2, m_r), (st2, st_r)):
            once = part[i].reshape(8, 4, 128)
            to[at, pl.ds(0, 4, stride=2), :] = once
            to[at, pl.ds(1, 4, stride=2), :] = once
        return 0

    lax.fori_loop(0, N_GRP, twice, 0)
    landed(base.at[pl.ds(0, N_ALL - 1)], recv_sem.at[6], "recv6")

    tiles = TILES
    shape = (tiles, 8, 128)
    lane = lax.broadcasted_iota(jnp.int32, shape, 2)
    sub = lax.broadcasted_iota(jnp.int32, shape, 1)

    def dot(a, b):
        return jnp.sum(a * b, axis=0)

    def mean(acc):
        return jnp.sum(jnp.sum(acc, axis=1, keepdims=True), axis=0, keepdims=True) / (2.0 * 65536.0)

    us = (u_pad, g0_pad, u_pad, u_pad)
    fs = (f_a, f_b, f_a, None)
    ds = (None, d1, d2, None)
    gram = {}

    def g_at(k, i):
        return g0_pad[pl.ds(tiles * i + 1, tiles)] if k == 0 else (None, g1, g2, g3)[k][pl.ds(tiles * i, tiles)]

    for step in range(ITERS):

        def picard(i, sums, step=step):
            at = pl.ds(tiles * i, tiles)
            src = us[step]
            u = src[pl.ds(tiles * i + 1, tiles)]
            before = src[pl.ds(tiles * i, tiles)]
            after = src[pl.ds(tiles * i + 2, tiles)]
            up = pltpu.roll(jnp.where(sub >= 6, before, u), 2, 1)
            down = pltpu.roll(jnp.where(sub < 2, after, u), 6, 1)
            left = pltpu.roll(jnp.where(lane == 127, up, u), 1, 2)
            right = pltpu.roll(jnp.where(lane == 0, down, u), 127, 2)
            strain = 0.5 * (right - left)
            square = strain * strain
            other = jnp.where((sub & 1) == 1, pltpu.roll(square, 1, 1), pltpu.roll(square, 7, 1))
            zeta = (0.5 * st2[at]) * lax.rsqrt(square + other + 0.25)
            force = base[at]
            new = (force + zeta * (left + right)) / (m2[at] + 1.0 + 2.0 * zeta)
            res = new - u
            if step == 0:
                g0_pad[pl.ds(tiles * i + 1, tiles)] = new
                fs[0][at] = res
                return sums
            (None, g1, g2, g3)[step][at] = new
            diff = res - fs[step - 1][at]
            if step < ITERS - 1:
                fs[step][at] = res
                ds[step][at] = diff
            diffs = [ds[j][at] for j in range(1, step)] + [diff]
            terms = [dot(d, diff) for d in diffs] + [dot(d, res) for d in diffs]
            return tuple(s + t for s, t in zip(sums, terms))

        zeros = tuple(jnp.zeros((8, 128), F32) for _ in range(2 * step))
        with jax.named_scope(f"picard{step}"):
            sums = lax.fori_loop(0, N_ALL // tiles, picard, zeros, unroll=UNROLL)
        if step == 0:
            continue
        means = [mean(s) for s in sums]
        for j in range(step):
            gram[(j, step - 1)] = means[j]
        norms = [jnp.sqrt(gram[(j, j)] + 1e-6) for j in range(step)]
        rows = [
            [
                gram[(min(a, b), max(a, b))] / (norms[a] * norms[b]) + (0.1 if a == b else 0.0)
                for b in range(step)
            ]
            + [means[step + a] / norms[a]]
            for a in range(step)
        ]
        for a in range(step):
            for b in range(a + 1, step):
                ratio = rows[b][a] / rows[a][a]
                rows[b] = [y - ratio * x for x, y in zip(rows[a], rows[b])]
        coef = [None] * step
        for a in reversed(range(step)):
            rest = rows[a][step]
            for b in range(a + 1, step):
                rest = rest - rows[a][b] * coef[b]
            coef[a] = rest / rows[a][a]
        scale = [jnp.broadcast_to(c / n, (8, 128))[None] for c, n in zip(coef, norms)]

        def combine(i, step=step, scale=scale):
            values = [g_at(j, i) for j in range(step + 1)]
            out = values[step]
            for j in range(step):
                out = out - scale[j] * (values[j + 1] - values[j])
            return out

        if step < ITERS - 1:

            def update(i, _, combine=combine):
                u_pad[pl.ds(tiles * i + 1, tiles)] = combine(i)
                return 0

            with jax.named_scope(f"update{step}"):
                lax.fori_loop(0, N_ALL // tiles, update, 0, unroll=UNROLL)
        else:
            for i in range(8 // tiles):
                ice[tiles * i : tiles * (i + 1)] = combine(8 // tiles * g + i)

    stress = ice[o] - q[1]
    for r in range(4):
        fx[r] = jnp.zeros((8, 128), F32)
        fx[r, 0:2] = stress[2 * r : 2 * r + 2]
        fx[r, 2:3] = 0.5 * (-0.05 * q[0, 2 * r + 1 : 2 * r + 2] - q[0, 2 * r : 2 * r + 1])

    lane1 = lax.broadcasted_iota(jnp.int32, (8, 128), 1)
    sub1 = lax.broadcasted_iota(jnp.int32, (8, 128), 0)

    def contribute(at, count, to):
        for r in range(4):
            x = fx[r].astype(BF16)
            w = jnp.concatenate([w_v[r, k] for k in range(2 * count)], axis=1)
            out = jnp.dot(x, w, preferred_element_type=F32)
            for k in range(2 * count):
                cbuf[k // 2, pl.ds((k % 2) * 4 + r, 3, stride=8), :] = out[0:3, 128 * k : 128 * (k + 1)]
        table = jnp.zeros((8, 128), F32)
        for c in range(count):
            values = cbuf[c].reshape(3, 8, 128)
            exponent = eighths(values)
            cq[1 + 3 * c : 4 + 3 * c] = counted(values, power(exponent))
            chunk = at + c
            own = lane1 == lax.rem(chunk, 16) * 8 + sub1
            for f in range(3):
                line = jnp.sum(jnp.where(own, exponent[f], 0.0), axis=0, keepdims=True)
                table += jnp.where(sub1 == 2 * f + chunk // 16, line, 0.0)
        cq[0] = table.astype(jnp.int32).astype(jnp.int16)
        planes = PLANES_1 if count == 1 else PLANES_4
        if planes > 1 + 3 * count:
            cq[planes - 1] = jnp.zeros((8, 128), jnp.int16)
        dst = crecv.at[pl.ds(to, planes)]
        over_grp(cq.at[pl.ds(0, planes)], dst, 7)
        crecv[pl.ds(to, planes)] = cq[0:planes]

    @pl.when(first)
    def _():
        contribute(0, 4, 0)

    @pl.when(last)
    def _():
        contribute(CHUNKS - 4, 4, PLANES - PLANES_4)

    @pl.when(inner)
    def _():
        contribute(3 + g, 1, PLANES_4 + PLANES_1 * (g - 1))

    with jax.named_scope("v_copy"):
        v_copy.wait()
    with jax.named_scope("halos"):
        for _, arrives, copy in halos:
            pl.when(arrives)(lambda copy=copy: copy.wait_recv())
    ys = lax.broadcasted_iota(jnp.int32, (L, 256), 0)
    cols = lax.broadcasted_iota(jnp.int32, (L, 256), 1)

    def stencil(t):
        def level(z, _):
            c = t_v[t, z]
            up = jnp.where(z > 0, t_v[t, jnp.maximum(z - 1, 0)], 0.0)
            down = jnp.where(z < L - 1, t_v[t, jnp.minimum(z + 1, L - 1)], 0.0)
            he = pltpu.roll(hx_r[0, t], 127 - z, 1)
            hw = pltpu.roll(hx_r[1, t], lax.rem(128 - z, 128), 1)
            east = jnp.where(cols == 255, jnp.concatenate([he, he], axis=1), pltpu.roll(c, 255, 1))
            west = jnp.where(cols == 0, jnp.concatenate([hw, hw], axis=1), pltpu.roll(c, 1, 1))
            north = jnp.where(ys == L - 1, hy_r[0, t, pl.ds(z, 1), :], pltpu.roll(c, L - 1, 0))
            south = jnp.where(ys == 0, hy_r[1, t, pl.ds(z, 1), :], pltpu.roll(c, 1, 0))
            pre[t, z] = (
                c
                + 0.2 * (east + west + north + south - 4.0 * c)
                - 0.25 * (v_v[0, z] * (east - west) + v_v[1, z] * (north - south))
                + 0.2 * (up + down - 2.0 * c)
            )
            return 0

        lax.fori_loop(0, L, level, 0)

    with jax.named_scope("stencil0"):
        stencil(0)

    @pl.when(polar)
    def _():
        landed(crecv.at[pl.ds(0, PLANES - PLANES_4)], recv_sem.at[7], "recv7")

    @pl.when(inner)
    def _():
        landed(crecv.at[pl.ds(0, PLANES - PLANES_1)], recv_sem.at[7], "recv7")

    starts = [0] + [PLANES_4 + PLANES_1 * i for i in range(N_GRP - 2)] + [PLANES - PLANES_4]
    table = jnp.zeros((8, 128), F32)
    for start in starts:
        table += crecv[start].astype(jnp.int32).astype(F32)
    table = power(table)
    for f in range(3):
        values = []
        for d, start in enumerate(starts):
            values += [crecv[start + 1 + 3 * c + f] for c in range(chunks_of(d))]
        values = [x.astype(jnp.int32).astype(F32) for x in values]
        values = jnp.concatenate(values + [jnp.zeros((8 * (PADDED - CHUNKS), 128), F32)], axis=0)
        values = halves(values)
        step = jnp.concatenate([table[2 * f : 2 * f + 1], table[2 * f + 1 : 2 * f + 2]], axis=1)
        out = jnp.dot(hits_t[...] * step.astype(BF16), values, preferred_element_type=F32)
        out = (out[:, 0:128] + out[:, 128:256]).reshape(4, 2, 64, 128)
        dense[0, :, f] = out[:, 0]
        dense[1, :, f] = out[:, 1]
    send(dense.at[1 - core], pair_in, 8, partner, g)
    landed(pair_in, recv_sem.at[8], "recv8")
    lane64 = lax.broadcasted_iota(jnp.int32, (64, 128), 1)
    row64 = lax.broadcasted_iota(jnp.int32, (64, 128), 0)
    for i in (1, 3, 2):
        to = lax.rem(z + i, 4)
        total = pair_in[to] + dense[core, to]
        step = power(eighths(total))
        pair_q[to] = counted(total, step)
        for f in range(3):
            line = jnp.sum(jnp.where(lane64 == row64, step[f], 0.0), axis=0, keepdims=True)
            pair_steps[to, f : f + 1] = line
        send(pair_q.at[to], dense_in.at[i - 1], 11, 2 * to + core, g)
        send(pair_steps.at[to], dense_steps.at[i - 1], 14, 2 * to + core, g)
    with jax.named_scope("stencil1"):
        stencil(1)
    landed(dense_in.at[pl.ds(0, 3)], recv_sem.at[11], "recv11")
    landed(dense_steps.at[pl.ds(0, 3)], recv_sem.at[14], "recv14")
    for f in range(3):
        out = pair_in[z, f] + dense[core, z, f]
        for i in range(3):
            step = jnp.where(lane64 == row64, dense_steps[i, f : f + 1], 0.0)
            step = jnp.sum(step, axis=1, keepdims=True)
            out += step * dense_in[i, f].astype(jnp.int32).astype(F32)
        flux[f, :, 0:128] = out[0:32]
        flux[f, :, 128:256] = out[32:64]

    landed(surf.at[pl.ds(0, N_OCN - 1)], send_sem.at[0])
    landed(base.at[pl.ds(0, N_ALL - 1)], send_sem.at[6])
    landed(pair_in, send_sem.at[8])
    landed(dense_in.at[pl.ds(0, 3)], send_sem.at[11])
    landed(dense_steps.at[pl.ds(0, 3)], send_sem.at[14])

    landed(u_r.at[pl.ds(0, N_GRP - 1), 0], send_sem.at[2])
    landed(u_r.at[:, pl.ds(0, 3)], send_sem.at[4])
    landed(u_r, send_sem.at[5])

    @pl.when(polar)
    def _():
        landed(g1.at[pl.ds(0, 4 * (N_GRP - 1))], send_sem.at[1])
        landed(sel.at[pl.ds(0, 15)], send_sem.at[3])
        for phase in (9, 10, 12):
            landed(sel.at[0], send_sem.at[phase])
        landed(g1.at[pl.ds(0, 7 * (N_GRP - 1))], send_sem.at[7])

    @pl.when(inner)
    def _():
        landed(g1.at[pl.ds(0, N_GRP - 1)], send_sem.at[1])
        landed(sel.at[pl.ds(0, 15)], send_sem.at[3])
        for phase in (9, 10, 12):
            landed(sel.at[pl.ds(0, 2)], send_sem.at[phase])
        landed(crecv.at[pl.ds(0, 4 * (N_GRP - 1))], send_sem.at[7])

    for sends, _, copy in halos:
        pl.when(sends)(lambda copy=copy: copy.wait_send())


def finish(pre, flux, ice, tracers_out, flux_out, ice_out, top, sem):
    copies = [
        pltpu.make_async_copy(pre.at[1], tracers_out.at[1], sem.at[0]),
        pltpu.make_async_copy(pre.at[0, pl.ds(1, L - 1)], tracers_out.at[0, pl.ds(1, L - 1)], sem.at[1]),
        pltpu.make_async_copy(flux, flux_out, sem.at[2]),
        pltpu.make_async_copy(ice, ice_out, sem.at[3]),
    ]
    for copy in copies:
        copy.start()
    top[...] = pre[0, 0] + 0.5 * flux[2]
    last = pltpu.make_async_copy(top, tracers_out.at[0, 0], sem.at[4])
    last.start()
    for copy in copies + [last]:
        copy.wait()


def on_device(
    tracers,
    velocity,
    remap_weights,
    remap_blocks,
    remap_count,
    ice_velocity,
    ice_mass_rate,
    ice_strength,
    wind_stress,
):
    def tiled(x):
        return x.reshape(2, 32, 128).transpose(1, 0, 2).reshape(4, 2, 8, 128)

    hbm = pl.BlockSpec(memory_space=pltpu.HBM)
    smem = pl.BlockSpec(memory_space=pltpu.SMEM)
    vmem = pl.BlockSpec(memory_space=pltpu.VMEM)
    scratch = [
        pltpu.SMEM((8, 32), jnp.int32),
        pltpu.SMEM((32,), jnp.int32),
        pltpu.VMEM((4, 2, 8, 128), F32),
        pltpu.VMEM((4, 2, 8, 128), F32),
        pltpu.VMEM((4, 2, 4, 128), F32),
        pltpu.VMEM((4, 2, 4, 128), F32),
        pltpu.VMEM((2, L, 32, 256), F32),
        pltpu.VMEM((2, L, 32, 256), F32),
        pltpu.VMEM((4, 8, 128, 128), BF16),
        pltpu.VMEM((4, 32, 256), F32),
        pltpu.VMEM((N_OCN, 64, 512), BF16),
        pltpu.VMEM((PADDED, 8, 128), jnp.int32),
        pltpu.VMEM((4, CHUNKS * 8, 128), BF16),
        pltpu.VMEM((512, 256), BF16),
        pltpu.VMEM((CHUNKS, 32, 128), BF16),
        pltpu.VMEM((4, N_GRP, 32, 128), BF16),
        pltpu.VMEM((4, 32, 128), F32),
        pltpu.VMEM((2, 8, 128), F32),
        pltpu.VMEM((2, 2, L, 128), F32),
        pltpu.VMEM((2, 2, L, 128), F32),
        pltpu.VMEM((2, 2, L, 256), F32),
        pltpu.VMEM((2, 2, L, 256), F32),
        pltpu.VMEM((N_GRP, 4, 2, 8, 128), F32),
        pltpu.VMEM((N_ALL + 2, 8, 128), F32),
        pltpu.VMEM((N_GRP, 4, 2, 4, 128), F32),
        pltpu.VMEM((N_GRP, 4, 2, 4, 128), F32),
        pltpu.VMEM((N_ALL, 8, 128), F32),
        pltpu.VMEM((N_ALL, 8, 128), F32),
        pltpu.VMEM((N_ALL, 8, 128), F32),
        pltpu.VMEM((N_ALL + 2, 8, 128), F32),
        *[pltpu.VMEM((N_ALL, 8, 128), F32)] * 7,
        pltpu.VMEM((4, 8, 128), F32),
        pltpu.VMEM((4, 24, 128), F32),
        pltpu.VMEM((PLANES_4, 8, 128), jnp.int16),
        pltpu.VMEM((PLANES, 8, 128), jnp.int16),
        pltpu.VMEM((2, 4, 3, 64, 128), F32),
        pltpu.VMEM((4, 3, 64, 128), F32),
        pltpu.VMEM((4, 3, 64, 128), jnp.int16),
        pltpu.VMEM((4, 3, 64, 128), jnp.int16),
        pltpu.VMEM((4, 8, 128), F32),
        pltpu.VMEM((4, 8, 128), F32),
        pltpu.SemaphoreType.DMA((16,)),
        pltpu.SemaphoreType.DMA((15,)),
        pltpu.SemaphoreType.DMA((15,)),
        pltpu.SemaphoreType.DMA((4,)),
        pltpu.SemaphoreType.DMA((4,)),
    ]
    pre, flux, ice = pl.pallas_call(
        kernel,
        out_shape=(
            jax.ShapeDtypeStruct((2, L, 32, 256), F32),
            jax.ShapeDtypeStruct((3, 32, 256), F32),
            jax.ShapeDtypeStruct((8, 8, 128), F32),
        ),
        in_specs=[hbm] * 9,
        out_specs=(vmem, vmem, vmem),
        scratch_shapes=scratch,
        compiler_params=pltpu.CompilerParams(
            collective_id=0, has_side_effects=True, vmem_limit_bytes=40 * 1024 * 1024
        ),
    )(
        *(
            pltpu.with_memory_space_constraint(x, pltpu.HBM)
            for x in (
                tracers,
                velocity,
                remap_weights,
                remap_blocks.T,
                remap_count,
                tiled(ice_velocity),
                tiled(wind_stress),
                ice_mass_rate.reshape(4, 2, 4, 128),
                ice_strength.reshape(4, 2, 4, 128),
            )
        )
    )
    tracers_next, flux, ice = pl.pallas_call(
        finish,
        out_shape=(
            jax.ShapeDtypeStruct((2, L, 32, 256), F32),
            jax.ShapeDtypeStruct((3, 32, 256), F32),
            jax.ShapeDtypeStruct((8, 8, 128), F32),
        ),
        in_specs=[vmem] * 3,
        out_specs=(hbm, hbm, hbm),
        scratch_shapes=[pltpu.VMEM((32, 256), F32), pltpu.SemaphoreType.DMA((5,))],
        compiler_params=pltpu.CompilerParams(vmem_limit_bytes=8 * 1024 * 1024),
    )(pre, flux, ice)
    ice_final = ice.reshape(32, 2, 128).transpose(1, 0, 2).reshape(2, 4096)
    return tracers_next, flux, ice_final


def solution(mesh):
    placed = (
        P(None, None, "grp", "ocn"),
        P(None, None, "grp", "ocn"),
        P("grp", None, None, None),
        P("grp", None),
        P("grp"),
        P(None, "grp"),
        P("grp"),
        P("grp"),
        P(None, "grp"),
    )
    return jax.shard_map(
        on_device,
        mesh=mesh,
        in_specs=placed,
        out_specs=(P(None, None, "grp", "ocn"), P(None, "grp", "ocn"), P(None, "grp")),
        check_vma=False,
    )
```

```python
import functools

import jax
import jax.numpy as jnp
from jax import lax
from jax.experimental import pallas as pl
from jax.experimental.pallas import tpu as pltpu
from jax.sharding import PartitionSpec as P

MESH = pl.DeviceIdType.MESH
F32 = jnp.float32
BF16 = jnp.bfloat16
N_OCN = 8
N_GRP = 16
N_ALL = N_OCN * N_GRP
LAST = N_GRP - 1
L = 32
CHUNKS = 22
PADDED = 32
PLANES_1, PLANES_4 = 4, 14
PLANES = 2 * PLANES_4 + (N_GRP - 2) * PLANES_1
ITERS = 4
TILES = 4
UNROLL = 32


def hops(*shifts):
    return sum(min(i, 4 - i) for i in shifts)


FAR_GRP = sorted(range(1, N_GRP), key=lambda i: -hops(i // 4, i % 4))
FAR_ALL = sorted(range(1, N_ALL), key=lambda i: (i * 37) % 128)


def chunk_of(g):
    return 0 if g == 0 else (CHUNKS - 4 if g == LAST else 3 + g)


def chunks_of(g):
    return 4 if g in (0, LAST) else 1


def power(x):
    return jnp.exp2(0.125 * x).astype(BF16).astype(F32)


def eighths(x):
    top = jnp.max(jnp.abs(x), axis=-1, keepdims=True)
    return jnp.ceil(8.0 * jnp.log2(jnp.maximum(top * (1.0 / 32000.0), 1e-37)))


def counted(x, step):
    return jnp.floor(x * (1.0 / step) + 0.5).astype(jnp.int32).astype(jnp.int16)


def halves(x):
    high = x.astype(BF16)
    return jnp.concatenate([high, (x - high.astype(F32)).astype(BF16)], axis=-1)


def landed(ref, sem, name="left"):
    with jax.named_scope(name):
        pltpu.make_async_copy(ref, ref, sem).wait()


def kernel(
    tracers,
    velocity,
    weights,
    blocks_hbm,
    counts_hbm,
    u_hbm,
    wind_hbm,
    mass_hbm,
    strength_hbm,
    pre,
    flux,
    ice,
    blocks,
    counts,
    u_in,
    wind,
    mass,
    strength,
    t_v,
    v_v,
    w_v,
    level0,
    surf,
    codes,
    hits,
    hits_t,
    sel,
    slots_in,
    xs,
    q,
    hx_s,
    hx_r,
    hy_s,
    hy_r,
    u_r,
    u_pad,
    m_r,
    st_r,
    m2,
    st2,
    base,
    g0_pad,
    g1,
    g2,
    g3,
    f_a,
    f_b,
    d1,
    d2,
    fx,
    cbuf,
    cq,
    crecv,
    dense,
    pair_in,
    pair_q,
    dense_in,
    pair_steps,
    dense_steps,
    local_sem,
    send_sem,
    recv_sem,
    halo_send,
    halo_recv,
):
    o = lax.axis_index("ocn")
    g = lax.axis_index("grp")
    z, core = o // 2, lax.rem(o, 2)
    partner = o + 1 - 2 * core
    first, last = g == 0, g == LAST
    polar = jnp.logical_or(first, last)
    inner = jnp.logical_and(g > 0, g < LAST)

    def send(src, dst, phase, ocn, grp):
        pltpu.make_async_remote_copy(
            src_ref=src,
            dst_ref=dst,
            send_sem=send_sem.at[phase],
            recv_sem=recv_sem.at[phase],
            device_id={"ocn": ocn, "grp": grp},
            device_id_type=MESH,
        ).start()

    gx, gy = g // 4, lax.rem(g, 4)
    to_x = [lax.rem(gx + i, 4) for i in range(4)]
    to_y = [lax.rem(gy + i, 4) for i in range(4)]
    to_o = [2 * lax.rem(z + i, 4) + (core if c == 0 else 1 - core) for i in range(4) for c in range(2)]
    to_g = [4 * to_x[i] + to_y[j] for i in range(4) for j in range(4)]

    def over_grp(src, dst, phase):
        for i in FAR_GRP:
            send(src, dst, phase, o, to_g[i])

    barrier = pltpu.get_barrier_semaphore()
    for i in range(1, N_GRP):
        pl.semaphore_signal(
            barrier, inc=1, device_id={"ocn": o, "grp": lax.rem(g + i, N_GRP)}, device_id_type=MESH
        )
    for i in range(1, N_OCN):
        pl.semaphore_signal(
            barrier, inc=1, device_id={"ocn": lax.rem(o + i, N_OCN), "grp": g}, device_id_type=MESH
        )

    small = [
        pltpu.make_async_copy(tracers.at[0, 0], level0.at[0], local_sem.at[0]),
        pltpu.make_async_copy(tracers.at[1, 0], level0.at[1], local_sem.at[1]),
        pltpu.make_async_copy(velocity.at[0, 0], level0.at[2], local_sem.at[2]),
        pltpu.make_async_copy(velocity.at[1, 0], level0.at[3], local_sem.at[3]),
    ]
    for copy in small:
        copy.start()
    index_copies = [
        pltpu.make_async_copy(blocks_hbm, blocks, local_sem.at[7]),
        pltpu.make_async_copy(counts_hbm, counts, local_sem.at[8]),
    ]
    ice_copies = [
        pltpu.make_async_copy(u_hbm, u_in, local_sem.at[9]),
        pltpu.make_async_copy(wind_hbm, wind, local_sem.at[10]),
        pltpu.make_async_copy(mass_hbm, mass, local_sem.at[11]),
        pltpu.make_async_copy(strength_hbm, strength, local_sem.at[12]),
    ]
    for copy in index_copies + ice_copies:
        copy.start()
    t_copy = pltpu.make_async_copy(tracers, t_v, local_sem.at[4])
    v_copy = pltpu.make_async_copy(velocity, v_v, local_sem.at[5])
    w_copy = pltpu.make_async_copy(weights.at[pl.ds(4 * o, 4)], w_v, local_sem.at[6])
    t_copy.start()
    w_copy.start()
    v_copy.start()

    def fill_codes(at, count):
        for k in range(2 * count):
            for r in range(4):
                block = blocks[k, 4 * o + r]
                code = jnp.where(k < counts[4 * o + r], block, -1)
                codes[at + k // 2, pl.ds((k % 2) * 4 + r, 1), :] = jnp.full((1, 128), code, jnp.int32)

    for copy in index_copies:
        copy.wait()

    @pl.when(first)
    def _():
        fill_codes(0, 4)

    @pl.when(last)
    def _():
        fill_codes(CHUNKS - 4, 4)

    @pl.when(inner)
    def _():
        fill_codes(3 + g, 1)

    codes[pl.ds(CHUNKS, PADDED - CHUNKS)] = jnp.full((PADDED - CHUNKS, 8, 128), -1, jnp.int32)
    u_pad[0] = jnp.zeros((8, 128), F32)
    u_pad[N_ALL + 1] = jnp.zeros((8, 128), F32)
    for copy in ice_copies:
        copy.wait()
    g0_pad[0] = jnp.zeros((8, 128), F32)
    g0_pad[N_ALL + 1] = jnp.zeros((8, 128), F32)

    @pl.when(core == 0)
    def _():
        u_r[g, z] = u_in[z]

    @pl.when(core == 1)
    def _():
        m_r[g, z] = mass[z]
        st_r[g, z] = strength[z]


    @pl.when(o == N_OCN - 1)
    def _():
        hx_r[0] = jnp.zeros((2, L, 128), F32)

    @pl.when(o == 0)
    def _():
        hx_r[1] = jnp.zeros((2, L, 128), F32)

    @pl.when(last)
    def _():
        hy_r[0] = jnp.zeros((2, L, 256), F32)

    @pl.when(first)
    def _():
        hy_r[1] = jnp.zeros((2, L, 256), F32)

    for copy in small:
        copy.wait()
    for f in range(4):
        field = level0[f]
        surf[o, 0:32, f * 128 : (f + 1) * 128] = field[:, 0:128].astype(BF16)
        surf[o, 32:64, f * 128 : (f + 1) * 128] = field[:, 128:256].astype(BF16)
    with jax.named_scope("barrier"):
        pl.semaphore_wait(barrier, N_GRP - 1 + N_OCN - 1)

    for i in (2, 1, 3):
        send(surf.at[o], surf.at[o], 14 + i, 2 * lax.rem(z + i, 4) + core, g)
    send(surf.at[o], surf.at[o], 18, partner, g)

    @pl.when(first)
    def _():
        part = codes.at[pl.ds(0, 4)]
        over_grp(part, part, 1)

    @pl.when(last)
    def _():
        part = codes.at[pl.ds(CHUNKS - 4, 4)]
        over_grp(part, part, 1)

    @pl.when(inner)
    def _():
        part = codes.at[pl.ds(3 + g, 1)]
        over_grp(part, part, 1)

    @pl.when(core == 0)
    def _():
        over_grp(u_in.at[z], u_r.at[g, z], 2)

    @pl.when(core == 1)
    def _():
        over_grp(mass.at[z], m_r.at[g, z], 2)
        over_grp(strength.at[z], st_r.at[g, z], 2)

    def pass_on(i):
        part = surf.at[2 * lax.rem(z + 4 - i, 4) + core]
        landed(part, recv_sem.at[14 + i], f"recv0_{i}")
        send(part, part, 18 + i, partner, g)

    pass_on(1)
    pass_on(3)
    pass_on(2)

    @pl.when(polar)
    def _():
        landed(codes.at[pl.ds(0, CHUNKS - 4)], recv_sem.at[1], "recv1")

    @pl.when(inner)
    def _():
        landed(codes.at[pl.ds(0, CHUNKS - 1)], recv_sem.at[1], "recv1")

    code = codes[...].reshape(PADDED * 8, 128)
    here = jnp.logical_and(code >= 0, ((code >> 6) & (N_GRP - 1)) == g)
    row = ((code >> 10) << 6) + ((code & 1) << 5) + ((code & 63) >> 1)
    row = jnp.where(here, row, -1)
    lane8 = lax.broadcasted_iota(jnp.int32, (CHUNKS * 8, 128), 1)
    for part in range(4):
        hit = row[: CHUNKS * 8] == lane8 + 128 * part
        hits[part] = jnp.where(hit, 1.0, 0.0).astype(BF16)
    row_f = row.astype(F32)
    row_t = jnp.concatenate([row_f[0:128].T[0:1], row_f[128:256].T[0:1]], axis=1)
    for part in range(8):
        ids = lax.broadcasted_iota(jnp.int32, (64, 256), 0).astype(F32) + 64.0 * part
        hits_t[part * 64 : (part + 1) * 64] = jnp.where(ids == row_t, 1.0, 0.0).astype(BF16)

    def select(i):
        part = lax.rem(z + 4 - i, 4)
        landed(surf.at[0], recv_sem.at[18 + i], f"recv18_{i}")
        rows = surf[pl.ds(2 * part, 2)].reshape(128, 512)
        return jnp.dot(hits[part], rows, preferred_element_type=F32)

    chosen = select(0)
    chosen += select(1)
    chosen += select(3)
    chosen += select(2)
    sel[...] = jnp.concatenate(
        [chosen[:, f * 128 : (f + 1) * 128].reshape(CHUNKS, 8, 128) for f in range(4)], axis=1
    ).astype(BF16)
    for d in (0, LAST, *range(1, LAST)):
        for c in range(chunks_of(d)):

            @pl.when(g != d)
            def _(d=d, c=c):
                send(sel.at[chunk_of(d) + c], slots_in.at[c, g], (3, 9, 10, 12)[c], o, d)

            @pl.when(g == d)
            def _(d=d, c=c):
                slots_in[c, d] = sel[chunk_of(d) + c]

    mine = ((u_r,), (m_r, st_r))
    landed(u_r.at[pl.ds(0, N_GRP - 1), 0], recv_sem.at[2], "recv2")
    for c in range(2):

        @pl.when(core == c)
        def _(c=c):
            for i in (1, 3, 2):
                for part in mine[c]:
                    send(part.at[:, z], part.at[:, z], 4, 2 * lax.rem(z + i, 4) + core, g)

    with jax.named_scope("t_copy"):
        t_copy.wait()
    lanes = lax.broadcasted_iota(jnp.int32, (L, 128), 1)
    for t in range(2):
        hy_s[0, t] = t_v[t, :, 0, :]
        hy_s[1, t] = t_v[t, :, 31, :]

        def gather(z, carry, t=t):
            west, east = carry
            tile = t_v[t, z]
            west = jnp.where(lanes == z, pltpu.roll(tile[:, 0:128], z, 1), west)
            east = jnp.where(lanes == z, pltpu.roll(tile[:, 128:256], z + 1, 1), east)
            return west, east

        zero = jnp.zeros((L, 128), F32)
        west, east = lax.fori_loop(0, L, gather, (zero, zero), unroll=8)
        hx_s[0, t] = west
        hx_s[1, t] = east

    def halo(src, dst, which, ocn, grp):
        return pltpu.make_async_remote_copy(
            src_ref=src,
            dst_ref=dst,
            send_sem=halo_send.at[which],
            recv_sem=halo_recv.at[which],
            device_id={"ocn": ocn, "grp": grp},
            device_id_type=MESH,
        )

    halos = (
        (o > 0, o < N_OCN - 1, halo(hx_s.at[0], hx_r.at[0], 0, jnp.maximum(o - 1, 0), g)),
        (o < N_OCN - 1, o > 0, halo(hx_s.at[1], hx_r.at[1], 1, jnp.minimum(o + 1, N_OCN - 1), g)),
        (g > 0, g < LAST, halo(hy_s.at[0], hy_r.at[0], 2, o, jnp.maximum(g - 1, 0))),
        (g < LAST, g > 0, halo(hy_s.at[1], hy_r.at[1], 3, o, jnp.minimum(g + 1, LAST))),
    )
    with jax.named_scope("w_copy"):
        w_copy.wait()

    def remap(count):
        out = [jnp.zeros((8, 128), F32)] * 4
        for c in range(count):
            landed(slots_in.at[0, pl.ds(0, N_GRP - 1)], recv_sem.at[(3, 9, 10, 12)[c]], f"recv3_{c}")
            total = jnp.zeros((32, 128), F32)
            for s in range(N_GRP):
                total += slots_in[c, s].astype(F32)
            xs[c] = total
            for r in range(4):
                x = [xs[c, pl.ds(4 * k + r, 4, stride=8), :] for k in range(2)]
                x = jnp.concatenate(x, axis=1)
                x = jnp.concatenate([x, jnp.zeros(x.shape, F32)], axis=0).astype(BF16)
                w = jnp.concatenate([w_v[r, 2 * c + k] for k in range(2)], axis=1)
                out[r] += lax.dot_general(x, w, (((1,), (1,)), ((), ())), preferred_element_type=F32)
        for r in range(4):
            q[0, 2 * r : 2 * r + 2] = out[r][0:2]
            q[1, 2 * r : 2 * r + 2] = out[r][2:4]

    @pl.when(polar)
    def _():
        remap(4)

    @pl.when(inner)
    def _():
        remap(1)

    tile = 8 * g + o
    m2[tile, pl.ds(0, 4, stride=2), :] = mass[z, core]
    m2[tile, pl.ds(1, 4, stride=2), :] = mass[z, core]
    base[tile] = m2[tile] * u_in[z, core] + wind[z, core] + q[1]

    for i in FAR_ALL:
        send(base.at[tile], base.at[tile], 6, to_o[i % 8], to_g[i // 8])
    for sends, _, copy in halos:
        pl.when(sends)(lambda copy=copy: copy.start())


    landed(u_r.at[:, pl.ds(0, 3)], recv_sem.at[4], "recv4")
    for c in range(2):

        @pl.when(core == c)
        def _(c=c):
            for part in mine[c]:
                send(part, part, 5, partner, g)

    landed(u_r, recv_sem.at[5], "recv5")

    def twice(i, _):
        at = pl.ds(8 * i, 8)
        u_pad[pl.ds(8 * i + 1, 8)] = u_r[i].reshape(8, 8, 128)
        for to, part in ((m2, m_r), (st2, st_r)):
            once = part[i].reshape(8, 4, 128)
            to[at, pl.ds(0, 4, stride=2), :] = once
            to[at, pl.ds(1, 4, stride=2), :] = once
        return 0

    lax.fori_loop(0, N_GRP, twice, 0)

    tiles = TILES
    shape = (tiles, 8, 128)
    lane = lax.broadcasted_iota(jnp.int32, shape, 2)
    sub = lax.broadcasted_iota(jnp.int32, shape, 1)

    def dot(a, b):
        return jnp.sum(a * b, axis=0)

    def mean(acc):
        return jnp.sum(jnp.sum(acc, axis=1, keepdims=True), axis=0, keepdims=True) / (2.0 * 65536.0)

    us = (u_pad, g0_pad, u_pad, u_pad)
    fs = (f_a, f_b, f_a, None)
    ds = (None, d1, d2, None)
    gram = {}

    def g_at(k, i):
        return g0_pad[pl.ds(tiles * i + 1, tiles)] if k == 0 else (None, g1, g2, g3)[k][pl.ds(tiles * i, tiles)]

    def drag(src, i, u):
        at = pl.ds(tiles * i, tiles)
        before = src[pl.ds(tiles * i, tiles)]
        after = src[pl.ds(tiles * i + 2, tiles)]
        up = pltpu.roll(jnp.where(sub >= 6, before, u), 2, 1)
        down = pltpu.roll(jnp.where(sub < 2, after, u), 6, 1)
        left = pltpu.roll(jnp.where(lane == 127, up, u), 1, 2)
        right = pltpu.roll(jnp.where(lane == 0, down, u), 127, 2)
        strain = 0.5 * (right - left)
        square = strain * strain
        other = jnp.where((sub & 1) == 1, pltpu.roll(square, 1, 1), pltpu.roll(square, 7, 1))
        return (0.5 * st2[at]) * lax.rsqrt(square + other + 0.25), left + right

    def ahead(i, _):
        at = pl.ds(tiles * i, tiles)
        zeta, both = drag(u_pad, i, u_pad[pl.ds(tiles * i + 1, tiles)])
        share = 1.0 / (m2[at] + 1.0 + 2.0 * zeta)
        d1[at] = share
        d2[at] = zeta * both * share
        return 0

    with jax.named_scope("ahead"):
        lax.fori_loop(0, N_ALL // tiles, ahead, 0, unroll=8)
    landed(base.at[pl.ds(0, N_ALL - 1)], recv_sem.at[6], "recv6")

    for step in range(ITERS):

        def picard(i, sums, step=step):
            at = pl.ds(tiles * i, tiles)
            src = us[step]
            u = src[pl.ds(tiles * i + 1, tiles)]
            if step == 0:
                new = base[at] * d1[at] + d2[at]
                g0_pad[pl.ds(tiles * i + 1, tiles)] = new
                fs[0][at] = new - u
                return sums
            zeta, both = drag(src, i, u)
            new = (base[at] + zeta * both) / (m2[at] + 1.0 + 2.0 * zeta)
            res = new - u
            (None, g1, g2, g3)[step][at] = new
            diff = res - fs[step - 1][at]
            if step < ITERS - 1:
                fs[step][at] = res
                ds[step][at] = diff
            diffs = [ds[j][at] for j in range(1, step)] + [diff]
            terms = [dot(d, diff) for d in diffs] + [dot(d, res) for d in diffs]
            return tuple(s + t for s, t in zip(sums, terms))

        zeros = tuple(jnp.zeros((8, 128), F32) for _ in range(2 * step))
        with jax.named_scope(f"picard{step}"):
            sums = lax.fori_loop(0, N_ALL // tiles, picard, zeros, unroll=UNROLL)
        if step == 0:
            continue
        means = [mean(s) for s in sums]
        for j in range(step):
            gram[(j, step - 1)] = means[j]
        norms = [jnp.sqrt(gram[(j, j)] + 1e-6) for j in range(step)]
        rows = [
            [
                gram[(min(a, b), max(a, b))] / (norms[a] * norms[b]) + (0.1 if a == b else 0.0)
                for b in range(step)
            ]
            + [means[step + a] / norms[a]]
            for a in range(step)
        ]
        for a in range(step):
            for b in range(a + 1, step):
                ratio = rows[b][a] / rows[a][a]
                rows[b] = [y - ratio * x for x, y in zip(rows[a], rows[b])]
        coef = [None] * step
        for a in reversed(range(step)):
            rest = rows[a][step]
            for b in range(a + 1, step):
                rest = rest - rows[a][b] * coef[b]
            coef[a] = rest / rows[a][a]
        scale = [jnp.broadcast_to(c / n, (8, 128))[None] for c, n in zip(coef, norms)]

        def combine(i, step=step, scale=scale):
            values = [g_at(j, i) for j in range(step + 1)]
            out = values[step]
            for j in range(step):
                out = out - scale[j] * (values[j + 1] - values[j])
            return out

        if step < ITERS - 1:

            def update(i, _, combine=combine):
                u_pad[pl.ds(tiles * i + 1, tiles)] = combine(i)
                return 0

            with jax.named_scope(f"update{step}"):
                lax.fori_loop(0, N_ALL // tiles, update, 0, unroll=UNROLL)
        else:
            for i in range(8 // tiles):
                ice[tiles * i : tiles * (i + 1)] = combine(8 // tiles * g + i)

    stress = ice[o] - q[1]
    for r in range(4):
        fx[r] = jnp.zeros((8, 128), F32)
        fx[r, 0:2] = stress[2 * r : 2 * r + 2]
        fx[r, 2:3] = 0.5 * (-0.05 * q[0, 2 * r + 1 : 2 * r + 2] - q[0, 2 * r : 2 * r + 1])

    lane1 = lax.broadcasted_iota(jnp.int32, (8, 128), 1)
    sub1 = lax.broadcasted_iota(jnp.int32, (8, 128), 0)

    def contribute(at, count, to):
        for r in range(4):
            x = fx[r].astype(BF16)
            w = jnp.concatenate([w_v[r, k] for k in range(2 * count)], axis=1)
            out = jnp.dot(x, w, preferred_element_type=F32)
            for k in range(2 * count):
                cbuf[k // 2, pl.ds((k % 2) * 4 + r, 3, stride=8), :] = out[0:3, 128 * k : 128 * (k + 1)]
        table = jnp.zeros((8, 128), F32)
        for c in range(count):
            values = cbuf[c].reshape(3, 8, 128)
            exponent = eighths(values)
            cq[1 + 3 * c : 4 + 3 * c] = counted(values, power(exponent))
            chunk = at + c
            own = lane1 == lax.rem(chunk, 16) * 8 + sub1
            for f in range(3):
                line = jnp.sum(jnp.where(own, exponent[f], 0.0), axis=0, keepdims=True)
                table += jnp.where(sub1 == 2 * f + chunk // 16, line, 0.0)
        cq[0] = table.astype(jnp.int32).astype(jnp.int16)
        planes = PLANES_1 if count == 1 else PLANES_4
        if planes > 1 + 3 * count:
            cq[planes - 1] = jnp.zeros((8, 128), jnp.int16)
        dst = crecv.at[pl.ds(to, planes)]
        over_grp(cq.at[pl.ds(0, planes)], dst, 7)
        crecv[pl.ds(to, planes)] = cq[0:planes]

    @pl.when(first)
    def _():
        contribute(0, 4, 0)

    @pl.when(last)
    def _():
        contribute(CHUNKS - 4, 4, PLANES - PLANES_4)

    @pl.when(inner)
    def _():
        contribute(3 + g, 1, PLANES_4 + PLANES_1 * (g - 1))

    with jax.named_scope("v_copy"):
        v_copy.wait()
    with jax.named_scope("halos"):
        for _, arrives, copy in halos:
            pl.when(arrives)(lambda copy=copy: copy.wait_recv())
    ys = lax.broadcasted_iota(jnp.int32, (L, 256), 0)
    cols = lax.broadcasted_iota(jnp.int32, (L, 256), 1)

    def stencil(t):
        def level(z, _):
            c = t_v[t, z]
            up = jnp.where(z > 0, t_v[t, jnp.maximum(z - 1, 0)], 0.0)
            down = jnp.where(z < L - 1, t_v[t, jnp.minimum(z + 1, L - 1)], 0.0)
            he = pltpu.roll(hx_r[0, t], 127 - z, 1)
            hw = pltpu.roll(hx_r[1, t], lax.rem(128 - z, 128), 1)
            east = jnp.where(cols == 255, jnp.concatenate([he, he], axis=1), pltpu.roll(c, 255, 1))
            west = jnp.where(cols == 0, jnp.concatenate([hw, hw], axis=1), pltpu.roll(c, 1, 1))
            north = jnp.where(ys == L - 1, hy_r[0, t, pl.ds(z, 1), :], pltpu.roll(c, L - 1, 0))
            south = jnp.where(ys == 0, hy_r[1, t, pl.ds(z, 1), :], pltpu.roll(c, 1, 0))
            pre[t, z] = (
                c
                + 0.2 * (east + west + north + south - 4.0 * c)
                - 0.25 * (v_v[0, z] * (east - west) + v_v[1, z] * (north - south))
                + 0.2 * (up + down - 2.0 * c)
            )
            return 0

        lax.fori_loop(0, L, level, 0)

    with jax.named_scope("stencil0"):
        stencil(0)

    @pl.when(polar)
    def _():
        landed(crecv.at[pl.ds(0, PLANES - PLANES_4)], recv_sem.at[7], "recv7")

    @pl.when(inner)
    def _():
        landed(crecv.at[pl.ds(0, PLANES - PLANES_1)], recv_sem.at[7], "recv7")

    starts = [0] + [PLANES_4 + PLANES_1 * i for i in range(N_GRP - 2)] + [PLANES - PLANES_4]
    table = jnp.zeros((8, 128), F32)
    for start in starts:
        table += crecv[start].astype(jnp.int32).astype(F32)
    table = power(table)
    for f in range(3):
        values = []
        for d, start in enumerate(starts):
            values += [crecv[start + 1 + 3 * c + f] for c in range(chunks_of(d))]
        values = [x.astype(jnp.int32).astype(F32) for x in values]
        values = jnp.concatenate(values + [jnp.zeros((8 * (PADDED - CHUNKS), 128), F32)], axis=0)
        values = halves(values)
        step = jnp.concatenate([table[2 * f : 2 * f + 1], table[2 * f + 1 : 2 * f + 2]], axis=1)
        out = jnp.dot(hits_t[...] * step.astype(BF16), values, preferred_element_type=F32)
        out = (out[:, 0:128] + out[:, 128:256]).reshape(4, 2, 64, 128)
        dense[0, :, f] = out[:, 0]
        dense[1, :, f] = out[:, 1]
    send(dense.at[1 - core], pair_in, 8, partner, g)
    landed(pair_in, recv_sem.at[8], "recv8")
    lane64 = lax.broadcasted_iota(jnp.int32, (64, 128), 1)
    row64 = lax.broadcasted_iota(jnp.int32, (64, 128), 0)
    for i in (1, 3, 2):
        to = lax.rem(z + i, 4)
        total = pair_in[to] + dense[core, to]
        step = power(eighths(total))
        pair_q[to] = counted(total, step)
        for f in range(3):
            line = jnp.sum(jnp.where(lane64 == row64, step[f], 0.0), axis=0, keepdims=True)
            pair_steps[to, f : f + 1] = line
        send(pair_q.at[to], dense_in.at[i - 1], 11, 2 * to + core, g)
        send(pair_steps.at[to], dense_steps.at[i - 1], 14, 2 * to + core, g)
    with jax.named_scope("stencil1"):
        stencil(1)
    landed(dense_in.at[pl.ds(0, 3)], recv_sem.at[11], "recv11")
    landed(dense_steps.at[pl.ds(0, 3)], recv_sem.at[14], "recv14")
    for f in range(3):
        out = pair_in[z, f] + dense[core, z, f]
        for i in range(3):
            step = jnp.where(lane64 == row64, dense_steps[i, f : f + 1], 0.0)
            step = jnp.sum(step, axis=1, keepdims=True)
            out += step * dense_in[i, f].astype(jnp.int32).astype(F32)
        flux[f, :, 0:128] = out[0:32]
        flux[f, :, 128:256] = out[32:64]

    for phase in (15, 16, 17, 18, 19, 20, 21):
        landed(surf.at[0], send_sem.at[phase])
    landed(base.at[pl.ds(0, N_ALL - 1)], send_sem.at[6])
    landed(pair_in, send_sem.at[8])
    landed(dense_in.at[pl.ds(0, 3)], send_sem.at[11])
    landed(dense_steps.at[pl.ds(0, 3)], send_sem.at[14])

    landed(u_r.at[pl.ds(0, N_GRP - 1), 0], send_sem.at[2])
    landed(u_r.at[:, pl.ds(0, 3)], send_sem.at[4])
    landed(u_r, send_sem.at[5])

    @pl.when(polar)
    def _():
        landed(g1.at[pl.ds(0, 4 * (N_GRP - 1))], send_sem.at[1])
        landed(sel.at[pl.ds(0, 15)], send_sem.at[3])
        for phase in (9, 10, 12):
            landed(sel.at[0], send_sem.at[phase])
        landed(g1.at[pl.ds(0, 7 * (N_GRP - 1))], send_sem.at[7])

    @pl.when(inner)
    def _():
        landed(g1.at[pl.ds(0, N_GRP - 1)], send_sem.at[1])
        landed(sel.at[pl.ds(0, 15)], send_sem.at[3])
        for phase in (9, 10, 12):
            landed(sel.at[pl.ds(0, 2)], send_sem.at[phase])
        landed(crecv.at[pl.ds(0, 4 * (N_GRP - 1))], send_sem.at[7])

    for sends, _, copy in halos:
        pl.when(sends)(lambda copy=copy: copy.wait_send())


def finish(pre, flux, ice, tracers_out, flux_out, ice_out, top, sem):
    copies = [
        pltpu.make_async_copy(pre.at[1], tracers_out.at[1], sem.at[0]),
        pltpu.make_async_copy(pre.at[0, pl.ds(1, L - 1)], tracers_out.at[0, pl.ds(1, L - 1)], sem.at[1]),
        pltpu.make_async_copy(flux, flux_out, sem.at[2]),
        pltpu.make_async_copy(ice, ice_out, sem.at[3]),
    ]
    for copy in copies:
        copy.start()
    top[...] = pre[0, 0] + 0.5 * flux[2]
    last = pltpu.make_async_copy(top, tracers_out.at[0, 0], sem.at[4])
    last.start()
    for copy in copies + [last]:
        copy.wait()


def on_device(
    tracers,
    velocity,
    remap_weights,
    remap_blocks,
    remap_count,
    ice_velocity,
    ice_mass_rate,
    ice_strength,
    wind_stress,
):
    def tiled(x):
        return x.reshape(2, 32, 128).transpose(1, 0, 2).reshape(4, 2, 8, 128)

    hbm = pl.BlockSpec(memory_space=pltpu.HBM)
    smem = pl.BlockSpec(memory_space=pltpu.SMEM)
    vmem = pl.BlockSpec(memory_space=pltpu.VMEM)
    scratch = [
        pltpu.SMEM((8, 32), jnp.int32),
        pltpu.SMEM((32,), jnp.int32),
        pltpu.VMEM((4, 2, 8, 128), F32),
        pltpu.VMEM((4, 2, 8, 128), F32),
        pltpu.VMEM((4, 2, 4, 128), F32),
        pltpu.VMEM((4, 2, 4, 128), F32),
        pltpu.VMEM((2, L, 32, 256), F32),
        pltpu.VMEM((2, L, 32, 256), F32),
        pltpu.VMEM((4, 8, 128, 128), BF16),
        pltpu.VMEM((4, 32, 256), F32),
        pltpu.VMEM((N_OCN, 64, 512), BF16),
        pltpu.VMEM((PADDED, 8, 128), jnp.int32),
        pltpu.VMEM((4, CHUNKS * 8, 128), BF16),
        pltpu.VMEM((512, 256), BF16),
        pltpu.VMEM((CHUNKS, 32, 128), BF16),
        pltpu.VMEM((4, N_GRP, 32, 128), BF16),
        pltpu.VMEM((4, 32, 128), F32),
        pltpu.VMEM((2, 8, 128), F32),
        pltpu.VMEM((2, 2, L, 128), F32),
        pltpu.VMEM((2, 2, L, 128), F32),
        pltpu.VMEM((2, 2, L, 256), F32),
        pltpu.VMEM((2, 2, L, 256), F32),
        pltpu.VMEM((N_GRP, 4, 2, 8, 128), F32),
        pltpu.VMEM((N_ALL + 2, 8, 128), F32),
        pltpu.VMEM((N_GRP, 4, 2, 4, 128), F32),
        pltpu.VMEM((N_GRP, 4, 2, 4, 128), F32),
        pltpu.VMEM((N_ALL, 8, 128), F32),
        pltpu.VMEM((N_ALL, 8, 128), F32),
        pltpu.VMEM((N_ALL, 8, 128), F32),
        pltpu.VMEM((N_ALL + 2, 8, 128), F32),
        *[pltpu.VMEM((N_ALL, 8, 128), F32)] * 7,
        pltpu.VMEM((4, 8, 128), F32),
        pltpu.VMEM((4, 24, 128), F32),
        pltpu.VMEM((PLANES_4, 8, 128), jnp.int16),
        pltpu.VMEM((PLANES, 8, 128), jnp.int16),
        pltpu.VMEM((2, 4, 3, 64, 128), F32),
        pltpu.VMEM((4, 3, 64, 128), F32),
        pltpu.VMEM((4, 3, 64, 128), jnp.int16),
        pltpu.VMEM((4, 3, 64, 128), jnp.int16),
        pltpu.VMEM((4, 8, 128), F32),
        pltpu.VMEM((4, 8, 128), F32),
        pltpu.SemaphoreType.DMA((16,)),
        pltpu.SemaphoreType.DMA((22,)),
        pltpu.SemaphoreType.DMA((22,)),
        pltpu.SemaphoreType.DMA((4,)),
        pltpu.SemaphoreType.DMA((4,)),
    ]
    pre, flux, ice = pl.pallas_call(
        kernel,
        out_shape=(
            jax.ShapeDtypeStruct((2, L, 32, 256), F32),
            jax.ShapeDtypeStruct((3, 32, 256), F32),
            jax.ShapeDtypeStruct((8, 8, 128), F32),
        ),
        in_specs=[hbm] * 9,
        out_specs=(vmem, vmem, vmem),
        scratch_shapes=scratch,
        compiler_params=pltpu.CompilerParams(
            collective_id=0, has_side_effects=True, vmem_limit_bytes=40 * 1024 * 1024
        ),
    )(
        *(
            pltpu.with_memory_space_constraint(x, pltpu.HBM)
            for x in (
                tracers,
                velocity,
                remap_weights,
                remap_blocks.T,
                remap_count,
                tiled(ice_velocity),
                tiled(wind_stress),
                ice_mass_rate.reshape(4, 2, 4, 128),
                ice_strength.reshape(4, 2, 4, 128),
            )
        )
    )
    tracers_next, flux, ice = pl.pallas_call(
        finish,
        out_shape=(
            jax.ShapeDtypeStruct((2, L, 32, 256), F32),
            jax.ShapeDtypeStruct((3, 32, 256), F32),
            jax.ShapeDtypeStruct((8, 8, 128), F32),
        ),
        in_specs=[vmem] * 3,
        out_specs=(hbm, hbm, hbm),
        scratch_shapes=[pltpu.VMEM((32, 256), F32), pltpu.SemaphoreType.DMA((5,))],
        compiler_params=pltpu.CompilerParams(vmem_limit_bytes=8 * 1024 * 1024),
    )(pre, flux, ice)
    ice_final = ice.reshape(32, 2, 128).transpose(1, 0, 2).reshape(2, 4096)
    return tracers_next, flux, ice_final


def solution(mesh):
    placed = (
        P(None, None, "grp", "ocn"),
        P(None, None, "grp", "ocn"),
        P("grp", None, None, None),
        P("grp", None),
        P("grp"),
        P(None, "grp"),
        P("grp"),
        P("grp"),
        P(None, "grp"),
    )
    return jax.shard_map(
        on_device,
        mesh=mesh,
        in_specs=placed,
        out_specs=(P(None, None, "grp", "ocn"), P(None, "grp", "ocn"), P(None, "grp")),
        check_vma=False,
    )
```

```python
import functools

import jax
import jax.numpy as jnp
from jax import lax
from jax.experimental import pallas as pl
from jax.experimental.pallas import tpu as pltpu
from jax.sharding import PartitionSpec as P

MESH = pl.DeviceIdType.MESH
F32 = jnp.float32
BF16 = jnp.bfloat16
N_OCN = 8
N_GRP = 16
N_ALL = N_OCN * N_GRP
LAST = N_GRP - 1
L = 32
CHUNKS = 22
PADDED = 32
PLANES_1, PLANES_4 = 4, 14
PLANES = 2 * PLANES_4 + (N_GRP - 2) * PLANES_1
ITERS = 4
TILES = 4
UNROLL = 32


def hops(*shifts):
    return sum(min(i, 4 - i) for i in shifts)


FAR_GRP = sorted(range(1, N_GRP), key=lambda i: -hops(i // 4, i % 4))
FAR_ALL = sorted(range(1, N_ALL), key=lambda i: (-hops(i // 32, i // 8 % 4, i // 2 % 4) // 2, (i * 37) % 128))
HELPERS = {(0, 2): 1, (0, 3): 4, (LAST, 2): LAST - 1, (LAST, 3): LAST - 4}
FAR_FIRST = sorted(range(1, N_ALL), key=lambda i: -hops(i // 32, i // 8 % 4, i // 2 % 4))


def chunk_of(g):
    return 0 if g == 0 else (CHUNKS - 4 if g == LAST else 3 + g)


def chunks_of(g):
    return 4 if g in (0, LAST) else 1


def power(x):
    return jnp.exp2(0.125 * x).astype(BF16).astype(F32)


def eighths(x):
    top = jnp.max(jnp.abs(x), axis=-1, keepdims=True)
    return jnp.ceil(8.0 * jnp.log2(jnp.maximum(top * (1.0 / 32000.0), 1e-37)))


def counted(x, step):
    return jnp.floor(x * (1.0 / step) + 0.5).astype(jnp.int32).astype(jnp.int16)


def halves(x):
    high = x.astype(BF16)
    return jnp.concatenate([high, (x - high.astype(F32)).astype(BF16)], axis=-1)


def landed(ref, sem, name="left"):
    with jax.named_scope(name):
        pltpu.make_async_copy(ref, ref, sem).wait()


def kernel(
    tracers,
    velocity,
    weights,
    blocks_hbm,
    counts_hbm,
    u_hbm,
    wind_hbm,
    mass_hbm,
    strength_hbm,
    pre,
    flux,
    ice,
    blocks,
    counts,
    u_in,
    wind,
    mass,
    strength,
    t_v,
    v_v,
    w_v,
    level0,
    surf,
    codes,
    hits,
    hits_t,
    sel,
    slots_in,
    help_in,
    help_out,
    helped,
    xs,
    q,
    hx_s,
    hx_r,
    hy_s,
    hy_r,
    u_r,
    u_pad,
    m_r,
    st_r,
    m2,
    st2,
    base,
    g0_pad,
    g1,
    g2,
    g3,
    f_a,
    f_b,
    d1,
    d2,
    fx,
    cbuf,
    cq,
    crecv,
    dense,
    pair_in,
    pair_q,
    dense_in,
    pair_steps,
    dense_steps,
    local_sem,
    send_sem,
    recv_sem,
    halo_send,
    halo_recv,
):
    o = lax.axis_index("ocn")
    g = lax.axis_index("grp")
    z, core = o // 2, lax.rem(o, 2)
    partner = o + 1 - 2 * core
    first, last = g == 0, g == LAST
    polar = jnp.logical_or(first, last)
    inner = jnp.logical_and(g > 0, g < LAST)

    def send(src, dst, phase, ocn, grp):
        pltpu.make_async_remote_copy(
            src_ref=src,
            dst_ref=dst,
            send_sem=send_sem.at[phase],
            recv_sem=recv_sem.at[phase],
            device_id={"ocn": ocn, "grp": grp},
            device_id_type=MESH,
        ).start()

    gx, gy = g // 4, lax.rem(g, 4)
    to_x = [lax.rem(gx + i, 4) for i in range(4)]
    to_y = [lax.rem(gy + i, 4) for i in range(4)]
    to_o = [2 * lax.rem(z + i, 4) + (core if c == 0 else 1 - core) for i in range(4) for c in range(2)]
    to_g = [4 * to_x[i] + to_y[j] for i in range(4) for j in range(4)]

    def over_grp(src, dst, phase):
        for i in FAR_GRP:
            send(src, dst, phase, o, to_g[i])

    barrier = pltpu.get_barrier_semaphore()
    for i in range(1, N_GRP):
        pl.semaphore_signal(
            barrier, inc=1, device_id={"ocn": o, "grp": lax.rem(g + i, N_GRP)}, device_id_type=MESH
        )
    for i in range(1, N_OCN):
        pl.semaphore_signal(
            barrier, inc=1, device_id={"ocn": lax.rem(o + i, N_OCN), "grp": g}, device_id_type=MESH
        )

    small = [
        pltpu.make_async_copy(tracers.at[0, 0], level0.at[0], local_sem.at[0]),
        pltpu.make_async_copy(tracers.at[1, 0], level0.at[1], local_sem.at[1]),
        pltpu.make_async_copy(velocity.at[0, 0], level0.at[2], local_sem.at[2]),
        pltpu.make_async_copy(velocity.at[1, 0], level0.at[3], local_sem.at[3]),
    ]
    for copy in small:
        copy.start()
    index_copies = [
        pltpu.make_async_copy(blocks_hbm, blocks, local_sem.at[7]),
        pltpu.make_async_copy(counts_hbm, counts, local_sem.at[8]),
    ]
    ice_copies = [
        pltpu.make_async_copy(u_hbm, u_in, local_sem.at[9]),
        pltpu.make_async_copy(wind_hbm, wind, local_sem.at[10]),
        pltpu.make_async_copy(mass_hbm, mass, local_sem.at[11]),
        pltpu.make_async_copy(strength_hbm, strength, local_sem.at[12]),
    ]
    for copy in index_copies + ice_copies:
        copy.start()
    t_copy = pltpu.make_async_copy(tracers, t_v, local_sem.at[4])
    v_copy = pltpu.make_async_copy(velocity, v_v, local_sem.at[5])
    w_copy = pltpu.make_async_copy(weights.at[pl.ds(4 * o, 4)], w_v, local_sem.at[6])
    t_copy.start()
    w_copy.start()
    v_copy.start()

    def fill_codes(at, count):
        for k in range(2 * count):
            for r in range(4):
                block = blocks[k, 4 * o + r]
                code = jnp.where(k < counts[4 * o + r], block, -1)
                codes[at + k // 2, pl.ds((k % 2) * 4 + r, 1), :] = jnp.full((1, 128), code, jnp.int32)

    for copy in index_copies:
        copy.wait()

    @pl.when(first)
    def _():
        fill_codes(0, 4)

    @pl.when(last)
    def _():
        fill_codes(CHUNKS - 4, 4)

    @pl.when(inner)
    def _():
        fill_codes(3 + g, 1)

    codes[pl.ds(CHUNKS, PADDED - CHUNKS)] = jnp.full((PADDED - CHUNKS, 8, 128), -1, jnp.int32)
    u_pad[0] = jnp.zeros((8, 128), F32)
    u_pad[N_ALL + 1] = jnp.zeros((8, 128), F32)
    for copy in ice_copies:
        copy.wait()
    g0_pad[0] = jnp.zeros((8, 128), F32)
    g0_pad[N_ALL + 1] = jnp.zeros((8, 128), F32)

    @pl.when(core == 0)
    def _():
        u_r[g, z] = u_in[z]

    @pl.when(core == 1)
    def _():
        m_r[g, z] = mass[z]
        st_r[g, z] = strength[z]


    @pl.when(o == N_OCN - 1)
    def _():
        hx_r[0] = jnp.zeros((2, L, 128), F32)

    @pl.when(o == 0)
    def _():
        hx_r[1] = jnp.zeros((2, L, 128), F32)

    @pl.when(last)
    def _():
        hy_r[0] = jnp.zeros((2, L, 256), F32)

    @pl.when(first)
    def _():
        hy_r[1] = jnp.zeros((2, L, 256), F32)

    for copy in small:
        copy.wait()
    for f in range(4):
        field = level0[f]
        surf[o, 0:32, f * 128 : (f + 1) * 128] = field[:, 0:128].astype(BF16)
        surf[o, 32:64, f * 128 : (f + 1) * 128] = field[:, 128:256].astype(BF16)
    with jax.named_scope("barrier"):
        pl.semaphore_wait(barrier, N_GRP - 1 + N_OCN - 1)

    for i in (2, 1, 3):
        send(surf.at[o], surf.at[o], 14 + i, 2 * lax.rem(z + i, 4) + core, g)
    send(surf.at[o], surf.at[o], 18, partner, g)

    @pl.when(first)
    def _():
        part = codes.at[pl.ds(0, 4)]
        over_grp(part, part, 1)

    @pl.when(last)
    def _():
        part = codes.at[pl.ds(CHUNKS - 4, 4)]
        over_grp(part, part, 1)

    @pl.when(inner)
    def _():
        part = codes.at[pl.ds(3 + g, 1)]
        over_grp(part, part, 1)

    @pl.when(core == 0)
    def _():
        over_grp(u_in.at[z], u_r.at[g, z], 2)

    @pl.when(core == 1)
    def _():
        over_grp(mass.at[z], m_r.at[g, z], 2)
        over_grp(strength.at[z], st_r.at[g, z], 2)

    def pass_on(i):
        part = surf.at[2 * lax.rem(z + 4 - i, 4) + core]
        landed(part, recv_sem.at[14 + i], f"recv0_{i}")
        send(part, part, 18 + i, partner, g)

    pass_on(1)
    pass_on(3)
    pass_on(2)

    @pl.when(polar)
    def _():
        landed(codes.at[pl.ds(0, CHUNKS - 4)], recv_sem.at[1], "recv1")

    @pl.when(inner)
    def _():
        landed(codes.at[pl.ds(0, CHUNKS - 1)], recv_sem.at[1], "recv1")

    code = codes[...].reshape(PADDED * 8, 128)
    here = jnp.logical_and(code >= 0, ((code >> 6) & (N_GRP - 1)) == g)
    row = ((code >> 10) << 6) + ((code & 1) << 5) + ((code & 63) >> 1)
    row = jnp.where(here, row, -1)
    lane8 = lax.broadcasted_iota(jnp.int32, (CHUNKS * 8, 128), 1)
    for part in range(4):
        hit = row[: CHUNKS * 8] == lane8 + 128 * part
        hits[part] = jnp.where(hit, 1.0, 0.0).astype(BF16)
    row_f = row.astype(F32)
    row_t = jnp.concatenate([row_f[0:128].T[0:1], row_f[128:256].T[0:1]], axis=1)
    for part in range(8):
        ids = lax.broadcasted_iota(jnp.int32, (64, 256), 0).astype(F32) + 64.0 * part
        hits_t[part * 64 : (part + 1) * 64] = jnp.where(ids == row_t, 1.0, 0.0).astype(BF16)

    mine = ((u_r,), (m_r, st_r))
    landed(u_r.at[pl.ds(0, N_GRP - 1), 0], recv_sem.at[2], "recv2")
    for c in range(2):

        @pl.when(core == c)
        def _(c=c):
            for i in (1, 3, 2):
                for part in mine[c]:
                    send(part.at[:, z], part.at[:, z], 4, 2 * lax.rem(z + i, 4) + core, g)

    def select(i):
        part = lax.rem(z + 4 - i, 4)
        landed(surf.at[0], recv_sem.at[18 + i], f"recv18_{i}")
        rows = surf[pl.ds(2 * part, 2)].reshape(128, 512)
        return jnp.dot(hits[part], rows, preferred_element_type=F32)

    chosen = select(0)
    chosen += select(1)
    chosen += select(3)
    chosen += select(2)
    sel[...] = jnp.concatenate(
        [chosen[:, f * 128 : (f + 1) * 128].reshape(CHUNKS, 8, 128) for f in range(4)], axis=1
    ).astype(BF16)
    def give(at, dst, own, phase, d):
        @pl.when(g != d)
        def _():
            send(sel.at[at], dst.at[g], phase, o, d)

        @pl.when(g == d)
        def _():
            own[d] = sel[at]

    for (d, c), helper in HELPERS.items():
        give(chunk_of(d) + c, help_in, help_in, 10, helper)
    for c in range(2):
        for d in (0, LAST):
            give(chunk_of(d) + c, slots_in.at[c], slots_in.at[c], (3, 9)[c], d)
    for d in range(1, LAST):
        give(chunk_of(d), slots_in.at[0], slots_in.at[0], 3, d)

    with jax.named_scope("t_copy"):
        t_copy.wait()
    lanes = lax.broadcasted_iota(jnp.int32, (L, 128), 1)
    for t in range(2):
        hy_s[0, t] = t_v[t, :, 0, :]
        hy_s[1, t] = t_v[t, :, 31, :]

        def gather(z, carry, t=t):
            west, east = carry
            tile = t_v[t, z]
            west = jnp.where(lanes == z, pltpu.roll(tile[:, 0:128], z, 1), west)
            east = jnp.where(lanes == z, pltpu.roll(tile[:, 128:256], z + 1, 1), east)
            return west, east

        zero = jnp.zeros((L, 128), F32)
        west, east = lax.fori_loop(0, L, gather, (zero, zero), unroll=8)
        hx_s[0, t] = west
        hx_s[1, t] = east

    def halo(src, dst, which, ocn, grp):
        return pltpu.make_async_remote_copy(
            src_ref=src,
            dst_ref=dst,
            send_sem=halo_send.at[which],
            recv_sem=halo_recv.at[which],
            device_id={"ocn": ocn, "grp": grp},
            device_id_type=MESH,
        )

    halos = (
        (o > 0, o < N_OCN - 1, halo(hx_s.at[0], hx_r.at[0], 0, jnp.maximum(o - 1, 0), g)),
        (o < N_OCN - 1, o > 0, halo(hx_s.at[1], hx_r.at[1], 1, jnp.minimum(o + 1, N_OCN - 1), g)),
        (g > 0, g < LAST, halo(hy_s.at[0], hy_r.at[0], 2, o, jnp.maximum(g - 1, 0))),
        (g < LAST, g > 0, halo(hy_s.at[1], hy_r.at[1], 3, o, jnp.minimum(g + 1, LAST))),
    )
    def collected(part):
        total = jnp.zeros((32, 128), F32)
        for s in range(N_GRP):
            total += part[s].astype(F32)
        return total

    for (d, c), helper in HELPERS.items():

        @pl.when(g == helper)
        def _(d=d, c=c):
            landed(help_in.at[pl.ds(0, N_GRP - 1)], recv_sem.at[10], "recv10")
            help_out[...] = collected(help_in).astype(BF16)
            send(help_out, helped.at[c - 2], 12, o, d)

    with jax.named_scope("w_copy"):
        w_copy.wait()

    def remap(count):
        out = [jnp.zeros((8, 128), F32)] * 4
        for c in range(count):
            if c < 2:
                landed(slots_in.at[0, pl.ds(0, N_GRP - 1)], recv_sem.at[(3, 9)[c]], f"recv3_{c}")
                xs[c] = collected(slots_in.at[c])
            else:
                if c == 2:
                    landed(helped, recv_sem.at[12], "recv3_3")
                xs[c] = helped[c - 2].astype(F32)
            for r in range(4):
                x = [xs[c, pl.ds(4 * k + r, 4, stride=8), :] for k in range(2)]
                x = jnp.concatenate(x, axis=1)
                x = jnp.concatenate([x, jnp.zeros(x.shape, F32)], axis=0).astype(BF16)
                w = jnp.concatenate([w_v[r, 2 * c + k] for k in range(2)], axis=1)
                out[r] += lax.dot_general(x, w, (((1,), (1,)), ((), ())), preferred_element_type=F32)
        for r in range(4):
            q[0, 2 * r : 2 * r + 2] = out[r][0:2]
            q[1, 2 * r : 2 * r + 2] = out[r][2:4]

    @pl.when(polar)
    def _():
        remap(4)

    @pl.when(inner)
    def _():
        remap(1)

    tile = 8 * g + o
    m2[tile, pl.ds(0, 4, stride=2), :] = mass[z, core]
    m2[tile, pl.ds(1, 4, stride=2), :] = mass[z, core]
    base[tile] = m2[tile] * u_in[z, core] + wind[z, core] + q[1]

    def spread(order):
        for i in order:
            send(base.at[tile], base.at[tile], 6, to_o[i % 8], to_g[i // 8])

    pl.when(polar)(lambda: spread(FAR_FIRST))
    pl.when(inner)(lambda: spread(FAR_ALL))
    for sends, _, copy in halos:
        pl.when(sends)(lambda copy=copy: copy.start())


    landed(u_r.at[:, pl.ds(0, 3)], recv_sem.at[4], "recv4")
    for c in range(2):

        @pl.when(core == c)
        def _(c=c):
            for part in mine[c]:
                send(part, part, 5, partner, g)

    landed(u_r, recv_sem.at[5], "recv5")

    def twice(i, _):
        at = pl.ds(8 * i, 8)
        u_pad[pl.ds(8 * i + 1, 8)] = u_r[i].reshape(8, 8, 128)
        for to, part in ((m2, m_r), (st2, st_r)):
            once = part[i].reshape(8, 4, 128)
            to[at, pl.ds(0, 4, stride=2), :] = once
            to[at, pl.ds(1, 4, stride=2), :] = once
        return 0

    lax.fori_loop(0, N_GRP, twice, 0)

    tiles = TILES
    shape = (tiles, 8, 128)
    lane = lax.broadcasted_iota(jnp.int32, shape, 2)
    sub = lax.broadcasted_iota(jnp.int32, shape, 1)

    def dot(a, b):
        return jnp.sum(a * b, axis=0)

    def mean(acc):
        return jnp.sum(jnp.sum(acc, axis=1, keepdims=True), axis=0, keepdims=True) / (2.0 * 65536.0)

    us = (u_pad, g0_pad, u_pad, u_pad)
    fs = (f_a, f_b, f_a, None)
    ds = (None, d1, d2, None)
    gram = {}

    def g_at(k, i):
        return g0_pad[pl.ds(tiles * i + 1, tiles)] if k == 0 else (None, g1, g2, g3)[k][pl.ds(tiles * i, tiles)]

    def drag(src, i, u):
        at = pl.ds(tiles * i, tiles)
        before = src[pl.ds(tiles * i, tiles)]
        after = src[pl.ds(tiles * i + 2, tiles)]
        up = pltpu.roll(jnp.where(sub >= 6, before, u), 2, 1)
        down = pltpu.roll(jnp.where(sub < 2, after, u), 6, 1)
        left = pltpu.roll(jnp.where(lane == 127, up, u), 1, 2)
        right = pltpu.roll(jnp.where(lane == 0, down, u), 127, 2)
        strain = 0.5 * (right - left)
        square = strain * strain
        other = jnp.where((sub & 1) == 1, pltpu.roll(square, 1, 1), pltpu.roll(square, 7, 1))
        return (0.5 * st2[at]) * lax.rsqrt(square + other + 0.25), left + right

    def ahead(i, _):
        at = pl.ds(tiles * i, tiles)
        zeta, both = drag(u_pad, i, u_pad[pl.ds(tiles * i + 1, tiles)])
        share = 1.0 / (m2[at] + 1.0 + 2.0 * zeta)
        d1[at] = share
        d2[at] = zeta * both * share
        return 0

    with jax.named_scope("ahead"):
        lax.fori_loop(0, N_ALL // tiles, ahead, 0, unroll=8)
    landed(base.at[pl.ds(0, N_ALL - 1)], recv_sem.at[6], "recv6")

    for step in range(ITERS):

        def picard(i, sums, step=step):
            at = pl.ds(tiles * i, tiles)
            src = us[step]
            u = src[pl.ds(tiles * i + 1, tiles)]
            if step == 0:
                new = base[at] * d1[at] + d2[at]
                g0_pad[pl.ds(tiles * i + 1, tiles)] = new
                fs[0][at] = new - u
                return sums
            zeta, both = drag(src, i, u)
            new = (base[at] + zeta * both) / (m2[at] + 1.0 + 2.0 * zeta)
            res = new - u
            (None, g1, g2, g3)[step][at] = new
            diff = res - fs[step - 1][at]
            if step < ITERS - 1:
                fs[step][at] = res
                ds[step][at] = diff
            diffs = [ds[j][at] for j in range(1, step)] + [diff]
            terms = [dot(d, diff) for d in diffs] + [dot(d, res) for d in diffs]
            return tuple(s + t for s, t in zip(sums, terms))

        zeros = tuple(jnp.zeros((8, 128), F32) for _ in range(2 * step))
        with jax.named_scope(f"picard{step}"):
            sums = lax.fori_loop(0, N_ALL // tiles, picard, zeros, unroll=UNROLL)
        if step == 0:
            continue
        means = [mean(s) for s in sums]
        for j in range(step):
            gram[(j, step - 1)] = means[j]
        norms = [jnp.sqrt(gram[(j, j)] + 1e-6) for j in range(step)]
        rows = [
            [
                gram[(min(a, b), max(a, b))] / (norms[a] * norms[b]) + (0.1 if a == b else 0.0)
                for b in range(step)
            ]
            + [means[step + a] / norms[a]]
            for a in range(step)
        ]
        for a in range(step):
            for b in range(a + 1, step):
                ratio = rows[b][a] / rows[a][a]
                rows[b] = [y - ratio * x for x, y in zip(rows[a], rows[b])]
        coef = [None] * step
        for a in reversed(range(step)):
            rest = rows[a][step]
            for b in range(a + 1, step):
                rest = rest - rows[a][b] * coef[b]
            coef[a] = rest / rows[a][a]
        scale = [jnp.broadcast_to(c / n, (8, 128))[None] for c, n in zip(coef, norms)]

        def combine(i, step=step, scale=scale):
            values = [g_at(j, i) for j in range(step + 1)]
            out = values[step]
            for j in range(step):
                out = out - scale[j] * (values[j + 1] - values[j])
            return out

        if step < ITERS - 1:

            def update(i, _, combine=combine):
                u_pad[pl.ds(tiles * i + 1, tiles)] = combine(i)
                return 0

            with jax.named_scope(f"update{step}"):
                lax.fori_loop(0, N_ALL // tiles, update, 0, unroll=UNROLL)
        else:
            for i in range(8 // tiles):
                ice[tiles * i : tiles * (i + 1)] = combine(8 // tiles * g + i)

    stress = ice[o] - q[1]
    for r in range(4):
        fx[r] = jnp.zeros((8, 128), F32)
        fx[r, 0:2] = stress[2 * r : 2 * r + 2]
        fx[r, 2:3] = 0.5 * (-0.05 * q[0, 2 * r + 1 : 2 * r + 2] - q[0, 2 * r : 2 * r + 1])

    lane1 = lax.broadcasted_iota(jnp.int32, (8, 128), 1)
    sub1 = lax.broadcasted_iota(jnp.int32, (8, 128), 0)

    def contribute(at, count, to):
        for r in range(4):
            x = fx[r].astype(BF16)
            w = jnp.concatenate([w_v[r, k] for k in range(2 * count)], axis=1)
            out = jnp.dot(x, w, preferred_element_type=F32)
            for k in range(2 * count):
                cbuf[k // 2, pl.ds((k % 2) * 4 + r, 3, stride=8), :] = out[0:3, 128 * k : 128 * (k + 1)]
        table = jnp.zeros((8, 128), F32)
        for c in range(count):
            values = cbuf[c].reshape(3, 8, 128)
            exponent = eighths(values)
            cq[1 + 3 * c : 4 + 3 * c] = counted(values, power(exponent))
            chunk = at + c
            own = lane1 == lax.rem(chunk, 16) * 8 + sub1
            for f in range(3):
                line = jnp.sum(jnp.where(own, exponent[f], 0.0), axis=0, keepdims=True)
                table += jnp.where(sub1 == 2 * f + chunk // 16, line, 0.0)
        cq[0] = table.astype(jnp.int32).astype(jnp.int16)
        planes = PLANES_1 if count == 1 else PLANES_4
        if planes > 1 + 3 * count:
            cq[planes - 1] = jnp.zeros((8, 128), jnp.int16)
        dst = crecv.at[pl.ds(to, planes)]
        over_grp(cq.at[pl.ds(0, planes)], dst, 7)
        crecv[pl.ds(to, planes)] = cq[0:planes]

    @pl.when(first)
    def _():
        contribute(0, 4, 0)

    @pl.when(last)
    def _():
        contribute(CHUNKS - 4, 4, PLANES - PLANES_4)

    @pl.when(inner)
    def _():
        contribute(3 + g, 1, PLANES_4 + PLANES_1 * (g - 1))

    with jax.named_scope("v_copy"):
        v_copy.wait()
    with jax.named_scope("halos"):
        for _, arrives, copy in halos:
            pl.when(arrives)(lambda copy=copy: copy.wait_recv())
    ys = lax.broadcasted_iota(jnp.int32, (L, 256), 0)
    cols = lax.broadcasted_iota(jnp.int32, (L, 256), 1)

    def stencil(t):
        def level(z, _):
            c = t_v[t, z]
            up = jnp.where(z > 0, t_v[t, jnp.maximum(z - 1, 0)], 0.0)
            down = jnp.where(z < L - 1, t_v[t, jnp.minimum(z + 1, L - 1)], 0.0)
            he = pltpu.roll(hx_r[0, t], 127 - z, 1)
            hw = pltpu.roll(hx_r[1, t], lax.rem(128 - z, 128), 1)
            east = jnp.where(cols == 255, jnp.concatenate([he, he], axis=1), pltpu.roll(c, 255, 1))
            west = jnp.where(cols == 0, jnp.concatenate([hw, hw], axis=1), pltpu.roll(c, 1, 1))
            north = jnp.where(ys == L - 1, hy_r[0, t, pl.ds(z, 1), :], pltpu.roll(c, L - 1, 0))
            south = jnp.where(ys == 0, hy_r[1, t, pl.ds(z, 1), :], pltpu.roll(c, 1, 0))
            pre[t, z] = (
                c
                + 0.2 * (east + west + north + south - 4.0 * c)
                - 0.25 * (v_v[0, z] * (east - west) + v_v[1, z] * (north - south))
                + 0.2 * (up + down - 2.0 * c)
            )
            return 0

        lax.fori_loop(0, L, level, 0)

    with jax.named_scope("stencil0"):
        stencil(0)

    @pl.when(polar)
    def _():
        landed(crecv.at[pl.ds(0, PLANES - PLANES_4)], recv_sem.at[7], "recv7")

    @pl.when(inner)
    def _():
        landed(crecv.at[pl.ds(0, PLANES - PLANES_1)], recv_sem.at[7], "recv7")

    starts = [0] + [PLANES_4 + PLANES_1 * i for i in range(N_GRP - 2)] + [PLANES - PLANES_4]
    table = jnp.zeros((8, 128), F32)
    for start in starts:
        table += crecv[start].astype(jnp.int32).astype(F32)
    table = power(table)
    for f in range(3):
        values = []
        for d, start in enumerate(starts):
            values += [crecv[start + 1 + 3 * c + f] for c in range(chunks_of(d))]
        values = [x.astype(jnp.int32).astype(F32) for x in values]
        values = jnp.concatenate(values + [jnp.zeros((8 * (PADDED - CHUNKS), 128), F32)], axis=0)
        values = halves(values)
        step = jnp.concatenate([table[2 * f : 2 * f + 1], table[2 * f + 1 : 2 * f + 2]], axis=1)
        out = jnp.dot(hits_t[...] * step.astype(BF16), values, preferred_element_type=F32)
        out = (out[:, 0:128] + out[:, 128:256]).reshape(4, 2, 64, 128)
        dense[0, :, f] = out[:, 0]
        dense[1, :, f] = out[:, 1]
    send(dense.at[1 - core], pair_in, 8, partner, g)
    landed(pair_in, recv_sem.at[8], "recv8")
    lane64 = lax.broadcasted_iota(jnp.int32, (64, 128), 1)
    row64 = lax.broadcasted_iota(jnp.int32, (64, 128), 0)
    for i in (1, 3, 2):
        to = lax.rem(z + i, 4)
        total = pair_in[to] + dense[core, to]
        step = power(eighths(total))
        pair_q[to] = counted(total, step)
        for f in range(3):
            line = jnp.sum(jnp.where(lane64 == row64, step[f], 0.0), axis=0, keepdims=True)
            pair_steps[to, f : f + 1] = line
        send(pair_q.at[to], dense_in.at[i - 1], 11, 2 * to + core, g)
        send(pair_steps.at[to], dense_steps.at[i - 1], 14, 2 * to + core, g)
    with jax.named_scope("stencil1"):
        stencil(1)
    landed(dense_in.at[pl.ds(0, 3)], recv_sem.at[11], "recv11")
    landed(dense_steps.at[pl.ds(0, 3)], recv_sem.at[14], "recv14")
    for f in range(3):
        out = pair_in[z, f] + dense[core, z, f]
        for i in range(3):
            step = jnp.where(lane64 == row64, dense_steps[i, f : f + 1], 0.0)
            step = jnp.sum(step, axis=1, keepdims=True)
            out += step * dense_in[i, f].astype(jnp.int32).astype(F32)
        flux[f, :, 0:128] = out[0:32]
        flux[f, :, 128:256] = out[32:64]

    for phase in (15, 16, 17, 18, 19, 20, 21):
        landed(surf.at[0], send_sem.at[phase])
    landed(base.at[pl.ds(0, N_ALL - 1)], send_sem.at[6])
    landed(pair_in, send_sem.at[8])
    landed(dense_in.at[pl.ds(0, 3)], send_sem.at[11])
    landed(dense_steps.at[pl.ds(0, 3)], send_sem.at[14])

    landed(u_r.at[pl.ds(0, N_GRP - 1), 0], send_sem.at[2])
    landed(u_r.at[:, pl.ds(0, 3)], send_sem.at[4])
    landed(u_r, send_sem.at[5])

    @pl.when(polar)
    def _():
        landed(g1.at[pl.ds(0, 4 * (N_GRP - 1))], send_sem.at[1])
        landed(sel.at[pl.ds(0, 15)], send_sem.at[3])
        landed(sel.at[0], send_sem.at[9])
        landed(sel.at[pl.ds(0, 4)], send_sem.at[10])
        landed(g1.at[pl.ds(0, 7 * (N_GRP - 1))], send_sem.at[7])

    @pl.when(inner)
    def _():
        landed(g1.at[pl.ds(0, N_GRP - 1)], send_sem.at[1])
        landed(sel.at[pl.ds(0, 15)], send_sem.at[3])
        landed(sel.at[pl.ds(0, 2)], send_sem.at[9])
        landed(crecv.at[pl.ds(0, 4 * (N_GRP - 1))], send_sem.at[7])

    helps = functools.reduce(jnp.logical_or, [g == d for d in HELPERS.values()])

    @pl.when(helps)
    def _():
        landed(sel.at[pl.ds(0, 3)], send_sem.at[10])
        landed(sel.at[0], send_sem.at[12])

    @pl.when(jnp.logical_and(inner, jnp.logical_not(helps)))
    def _():
        landed(sel.at[pl.ds(0, 4)], send_sem.at[10])

    for sends, _, copy in halos:
        pl.when(sends)(lambda copy=copy: copy.wait_send())


def finish(pre, flux, ice, tracers_out, flux_out, ice_out, top, sem):
    copies = [
        pltpu.make_async_copy(pre.at[1], tracers_out.at[1], sem.at[0]),
        pltpu.make_async_copy(pre.at[0, pl.ds(1, L - 1)], tracers_out.at[0, pl.ds(1, L - 1)], sem.at[1]),
        pltpu.make_async_copy(flux, flux_out, sem.at[2]),
        pltpu.make_async_copy(ice, ice_out, sem.at[3]),
    ]
    for copy in copies:
        copy.start()
    top[...] = pre[0, 0] + 0.5 * flux[2]
    last = pltpu.make_async_copy(top, tracers_out.at[0, 0], sem.at[4])
    last.start()
    for copy in copies + [last]:
        copy.wait()


def on_device(
    tracers,
    velocity,
    remap_weights,
    remap_blocks,
    remap_count,
    ice_velocity,
    ice_mass_rate,
    ice_strength,
    wind_stress,
):
    def tiled(x):
        return x.reshape(2, 32, 128).transpose(1, 0, 2).reshape(4, 2, 8, 128)

    hbm = pl.BlockSpec(memory_space=pltpu.HBM)
    smem = pl.BlockSpec(memory_space=pltpu.SMEM)
    vmem = pl.BlockSpec(memory_space=pltpu.VMEM)
    scratch = [
        pltpu.SMEM((8, 32), jnp.int32),
        pltpu.SMEM((32,), jnp.int32),
        pltpu.VMEM((4, 2, 8, 128), F32),
        pltpu.VMEM((4, 2, 8, 128), F32),
        pltpu.VMEM((4, 2, 4, 128), F32),
        pltpu.VMEM((4, 2, 4, 128), F32),
        pltpu.VMEM((2, L, 32, 256), F32),
        pltpu.VMEM((2, L, 32, 256), F32),
        pltpu.VMEM((4, 8, 128, 128), BF16),
        pltpu.VMEM((4, 32, 256), F32),
        pltpu.VMEM((N_OCN, 64, 512), BF16),
        pltpu.VMEM((PADDED, 8, 128), jnp.int32),
        pltpu.VMEM((4, CHUNKS * 8, 128), BF16),
        pltpu.VMEM((512, 256), BF16),
        pltpu.VMEM((CHUNKS, 32, 128), BF16),
        pltpu.VMEM((2, N_GRP, 32, 128), BF16),
        pltpu.VMEM((N_GRP, 32, 128), BF16),
        pltpu.VMEM((32, 128), BF16),
        pltpu.VMEM((2, 32, 128), BF16),
        pltpu.VMEM((4, 32, 128), F32),
        pltpu.VMEM((2, 8, 128), F32),
        pltpu.VMEM((2, 2, L, 128), F32),
        pltpu.VMEM((2, 2, L, 128), F32),
        pltpu.VMEM((2, 2, L, 256), F32),
        pltpu.VMEM((2, 2, L, 256), F32),
        pltpu.VMEM((N_GRP, 4, 2, 8, 128), F32),
        pltpu.VMEM((N_ALL + 2, 8, 128), F32),
        pltpu.VMEM((N_GRP, 4, 2, 4, 128), F32),
        pltpu.VMEM((N_GRP, 4, 2, 4, 128), F32),
        pltpu.VMEM((N_ALL, 8, 128), F32),
        pltpu.VMEM((N_ALL, 8, 128), F32),
        pltpu.VMEM((N_ALL, 8, 128), F32),
        pltpu.VMEM((N_ALL + 2, 8, 128), F32),
        *[pltpu.VMEM((N_ALL, 8, 128), F32)] * 7,
        pltpu.VMEM((4, 8, 128), F32),
        pltpu.VMEM((4, 24, 128), F32),
        pltpu.VMEM((PLANES_4, 8, 128), jnp.int16),
        pltpu.VMEM((PLANES, 8, 128), jnp.int16),
        pltpu.VMEM((2, 4, 3, 64, 128), F32),
        pltpu.VMEM((4, 3, 64, 128), F32),
        pltpu.VMEM((4, 3, 64, 128), jnp.int16),
        pltpu.VMEM((4, 3, 64, 128), jnp.int16),
        pltpu.VMEM((4, 8, 128), F32),
        pltpu.VMEM((4, 8, 128), F32),
        pltpu.SemaphoreType.DMA((16,)),
        pltpu.SemaphoreType.DMA((22,)),
        pltpu.SemaphoreType.DMA((22,)),
        pltpu.SemaphoreType.DMA((4,)),
        pltpu.SemaphoreType.DMA((4,)),
    ]
    pre, flux, ice = pl.pallas_call(
        kernel,
        out_shape=(
            jax.ShapeDtypeStruct((2, L, 32, 256), F32),
            jax.ShapeDtypeStruct((3, 32, 256), F32),
            jax.ShapeDtypeStruct((8, 8, 128), F32),
        ),
        in_specs=[hbm] * 9,
        out_specs=(vmem, vmem, vmem),
        scratch_shapes=scratch,
        compiler_params=pltpu.CompilerParams(
            collective_id=0, has_side_effects=True, vmem_limit_bytes=40 * 1024 * 1024
        ),
    )(
        *(
            pltpu.with_memory_space_constraint(x, pltpu.HBM)
            for x in (
                tracers,
                velocity,
                remap_weights,
                remap_blocks.T,
                remap_count,
                tiled(ice_velocity),
                tiled(wind_stress),
                ice_mass_rate.reshape(4, 2, 4, 128),
                ice_strength.reshape(4, 2, 4, 128),
            )
        )
    )
    tracers_next, flux, ice = pl.pallas_call(
        finish,
        out_shape=(
            jax.ShapeDtypeStruct((2, L, 32, 256), F32),
            jax.ShapeDtypeStruct((3, 32, 256), F32),
            jax.ShapeDtypeStruct((8, 8, 128), F32),
        ),
        in_specs=[vmem] * 3,
        out_specs=(hbm, hbm, hbm),
        scratch_shapes=[pltpu.VMEM((32, 256), F32), pltpu.SemaphoreType.DMA((5,))],
        compiler_params=pltpu.CompilerParams(vmem_limit_bytes=8 * 1024 * 1024),
    )(pre, flux, ice)
    ice_final = ice.reshape(32, 2, 128).transpose(1, 0, 2).reshape(2, 4096)
    return tracers_next, flux, ice_final


def solution(mesh):
    placed = (
        P(None, None, "grp", "ocn"),
        P(None, None, "grp", "ocn"),
        P("grp", None, None, None),
        P("grp", None),
        P("grp"),
        P(None, "grp"),
        P("grp"),
        P("grp"),
        P(None, "grp"),
    )
    return jax.shard_map(
        on_device,
        mesh=mesh,
        in_specs=placed,
        out_specs=(P(None, None, "grp", "ocn"), P(None, "grp", "ocn"), P(None, "grp")),
        check_vma=False,
    )
```

```python
import functools

import jax
import jax.numpy as jnp
from jax import lax
from jax.experimental import pallas as pl
from jax.experimental.pallas import tpu as pltpu
from jax.sharding import PartitionSpec as P

MESH = pl.DeviceIdType.MESH
F32 = jnp.float32
BF16 = jnp.bfloat16
N_OCN = 8
N_GRP = 16
N_ALL = N_OCN * N_GRP
LAST = N_GRP - 1
L = 32
CHUNKS = 22
PADDED = 32
PLANES_1, PLANES_4 = 4, 14
PLANES = 2 * PLANES_4 + (N_GRP - 2) * PLANES_1
ITERS = 4
TILES = 4
UNROLL = 32


def hops(*shifts):
    return sum(min(i, 4 - i) for i in shifts)


FAR_GRP = sorted(range(1, N_GRP), key=lambda i: -hops(i // 4, i % 4))
FAR_ALL = sorted(range(1, N_ALL), key=lambda i: (-hops(i // 32, i // 8 % 4, i // 2 % 4) // 2, (i * 37) % 128))
HELPERS = {(0, 2): 1, (0, 3): 4, (LAST, 2): LAST - 1, (LAST, 3): LAST - 4}
FAR_FIRST = sorted(range(1, N_ALL), key=lambda i: -hops(i // 32, i // 8 % 4, i // 2 % 4))


def chunk_of(g):
    return 0 if g == 0 else (CHUNKS - 4 if g == LAST else 3 + g)


def chunks_of(g):
    return 4 if g in (0, LAST) else 1


def power(x):
    return jnp.exp2(0.125 * x).astype(BF16).astype(F32)


def eighths(x):
    top = jnp.max(jnp.abs(x), axis=-1, keepdims=True)
    return jnp.ceil(8.0 * jnp.log2(jnp.maximum(top * (1.0 / 32000.0), 1e-37)))


def counted(x, step):
    return jnp.floor(x * (1.0 / step) + 0.5).astype(jnp.int32).astype(jnp.int16)


def halves(x):
    high = x.astype(BF16)
    return jnp.concatenate([high, (x - high.astype(F32)).astype(BF16)], axis=-1)


def landed(ref, sem, name="left"):
    with jax.named_scope(name):
        pltpu.make_async_copy(ref, ref, sem).wait()


def kernel(
    tracers,
    velocity,
    weights,
    blocks_hbm,
    counts_hbm,
    u_hbm,
    wind_hbm,
    mass_hbm,
    strength_hbm,
    pre,
    flux,
    ice,
    blocks,
    counts,
    u_in,
    wind,
    mass,
    strength,
    t_v,
    v_v,
    w_v,
    level0,
    surf,
    codes,
    hits,
    hits_t,
    sel,
    slots_in,
    help_in,
    help_out,
    helped,
    xs,
    q,
    hx_s,
    hx_r,
    hy_s,
    hy_r,
    u_r,
    u_pad,
    m_r,
    st_r,
    m2,
    st2,
    base,
    g0_pad,
    g1,
    g2,
    g3,
    f_a,
    f_b,
    d1,
    d2,
    fx,
    cbuf,
    cq,
    crecv,
    dense,
    pair_in,
    pair_q,
    dense_in,
    pair_steps,
    dense_steps,
    local_sem,
    send_sem,
    recv_sem,
    halo_send,
    halo_recv,
):
    o = lax.axis_index("ocn")
    g = lax.axis_index("grp")
    z, core = o // 2, lax.rem(o, 2)
    partner = o + 1 - 2 * core
    first, last = g == 0, g == LAST
    polar = jnp.logical_or(first, last)
    inner = jnp.logical_and(g > 0, g < LAST)

    def send(src, dst, phase, ocn, grp):
        pltpu.make_async_remote_copy(
            src_ref=src,
            dst_ref=dst,
            send_sem=send_sem.at[phase],
            recv_sem=recv_sem.at[phase],
            device_id={"ocn": ocn, "grp": grp},
            device_id_type=MESH,
        ).start()

    gx, gy = g // 4, lax.rem(g, 4)
    to_x = [lax.rem(gx + i, 4) for i in range(4)]
    to_y = [lax.rem(gy + i, 4) for i in range(4)]
    to_o = [2 * lax.rem(z + i, 4) + (core if c == 0 else 1 - core) for i in range(4) for c in range(2)]
    to_g = [4 * to_x[i] + to_y[j] for i in range(4) for j in range(4)]

    def over_grp(src, dst, phase):
        for i in FAR_GRP:
            send(src, dst, phase, o, to_g[i])

    barrier = pltpu.get_barrier_semaphore()
    for i in range(1, N_GRP):
        pl.semaphore_signal(
            barrier, inc=1, device_id={"ocn": o, "grp": lax.rem(g + i, N_GRP)}, device_id_type=MESH
        )
    for i in range(1, N_OCN):
        pl.semaphore_signal(
            barrier, inc=1, device_id={"ocn": lax.rem(o + i, N_OCN), "grp": g}, device_id_type=MESH
        )

    small = [
        pltpu.make_async_copy(tracers.at[0, 0], level0.at[0], local_sem.at[0]),
        pltpu.make_async_copy(tracers.at[1, 0], level0.at[1], local_sem.at[1]),
        pltpu.make_async_copy(velocity.at[0, 0], level0.at[2], local_sem.at[2]),
        pltpu.make_async_copy(velocity.at[1, 0], level0.at[3], local_sem.at[3]),
    ]
    for copy in small:
        copy.start()
    index_copies = [
        pltpu.make_async_copy(blocks_hbm, blocks, local_sem.at[7]),
        pltpu.make_async_copy(counts_hbm, counts, local_sem.at[8]),
    ]
    ice_copies = [
        pltpu.make_async_copy(u_hbm, u_in, local_sem.at[9]),
        pltpu.make_async_copy(wind_hbm, wind, local_sem.at[10]),
        pltpu.make_async_copy(mass_hbm, mass, local_sem.at[11]),
        pltpu.make_async_copy(strength_hbm, strength, local_sem.at[12]),
    ]
    for copy in index_copies + ice_copies:
        copy.start()
    t_copy = pltpu.make_async_copy(tracers, t_v, local_sem.at[4])
    v_copy = pltpu.make_async_copy(velocity, v_v, local_sem.at[5])
    w_copy = pltpu.make_async_copy(weights.at[pl.ds(4 * o, 4)], w_v, local_sem.at[6])
    t_copy.start()
    w_copy.start()
    v_copy.start()

    def fill_codes(at, count):
        for k in range(2 * count):
            for r in range(4):
                block = blocks[k, 4 * o + r]
                code = jnp.where(k < counts[4 * o + r], block, -1)
                codes[at + k // 2, pl.ds((k % 2) * 4 + r, 1), :] = jnp.full((1, 128), code, jnp.int32)

    for copy in index_copies:
        copy.wait()

    @pl.when(first)
    def _():
        fill_codes(0, 4)

    @pl.when(last)
    def _():
        fill_codes(CHUNKS - 4, 4)

    @pl.when(inner)
    def _():
        fill_codes(3 + g, 1)

    codes[pl.ds(CHUNKS, PADDED - CHUNKS)] = jnp.full((PADDED - CHUNKS, 8, 128), -1, jnp.int32)
    u_pad[0] = jnp.zeros((8, 128), F32)
    u_pad[N_ALL + 1] = jnp.zeros((8, 128), F32)
    for copy in ice_copies:
        copy.wait()
    g0_pad[0] = jnp.zeros((8, 128), F32)
    g0_pad[N_ALL + 1] = jnp.zeros((8, 128), F32)

    @pl.when(core == 0)
    def _():
        u_r[g, z] = u_in[z]

    @pl.when(core == 1)
    def _():
        m_r[g, z] = mass[z]
        st_r[g, z] = strength[z]


    @pl.when(o == N_OCN - 1)
    def _():
        hx_r[0] = jnp.zeros((2, L, 128), F32)

    @pl.when(o == 0)
    def _():
        hx_r[1] = jnp.zeros((2, L, 128), F32)

    @pl.when(last)
    def _():
        hy_r[0] = jnp.zeros((2, L, 256), F32)

    @pl.when(first)
    def _():
        hy_r[1] = jnp.zeros((2, L, 256), F32)

    for copy in small:
        copy.wait()
    for f in range(4):
        field = level0[f]
        surf[o, 0:32, f * 128 : (f + 1) * 128] = field[:, 0:128].astype(BF16)
        surf[o, 32:64, f * 128 : (f + 1) * 128] = field[:, 128:256].astype(BF16)
    with jax.named_scope("barrier"):
        pl.semaphore_wait(barrier, N_GRP - 1 + N_OCN - 1)

    for i in (2, 1, 3):
        send(surf.at[o], surf.at[o], 14 + i, 2 * lax.rem(z + i, 4) + core, g)
    send(surf.at[o], surf.at[o], 18, partner, g)

    @pl.when(first)
    def _():
        part = codes.at[pl.ds(0, 4)]
        over_grp(part, part, 1)

    @pl.when(last)
    def _():
        part = codes.at[pl.ds(CHUNKS - 4, 4)]
        over_grp(part, part, 1)

    @pl.when(inner)
    def _():
        part = codes.at[pl.ds(3 + g, 1)]
        over_grp(part, part, 1)

    @pl.when(core == 0)
    def _():
        over_grp(u_in.at[z], u_r.at[g, z], 2)

    @pl.when(core == 1)
    def _():
        over_grp(mass.at[z], m_r.at[g, z], 2)
        over_grp(strength.at[z], st_r.at[g, z], 2)

    def pass_on(i):
        part = surf.at[2 * lax.rem(z + 4 - i, 4) + core]
        landed(part, recv_sem.at[14 + i], f"recv0_{i}")
        send(part, part, 18 + i, partner, g)

    pass_on(1)
    pass_on(3)
    pass_on(2)

    @pl.when(polar)
    def _():
        landed(codes.at[pl.ds(0, CHUNKS - 4)], recv_sem.at[1], "recv1")

    @pl.when(inner)
    def _():
        landed(codes.at[pl.ds(0, CHUNKS - 1)], recv_sem.at[1], "recv1")

    code = codes[...].reshape(PADDED * 8, 128)
    here = jnp.logical_and(code >= 0, ((code >> 6) & (N_GRP - 1)) == g)
    row = ((code >> 10) << 6) + ((code & 1) << 5) + ((code & 63) >> 1)
    row = jnp.where(here, row, -1)
    lane8 = lax.broadcasted_iota(jnp.int32, (CHUNKS * 8, 128), 1)
    for part in range(4):
        hit = row[: CHUNKS * 8] == lane8 + 128 * part
        hits[part] = jnp.where(hit, 1.0, 0.0).astype(BF16)
    row_f = row.astype(F32)
    row_t = jnp.concatenate([row_f[0:128].T[0:1], row_f[128:256].T[0:1]], axis=1)
    for part in range(8):
        ids = lax.broadcasted_iota(jnp.int32, (64, 256), 0).astype(F32) + 64.0 * part
        hits_t[part * 64 : (part + 1) * 64] = jnp.where(ids == row_t, 1.0, 0.0).astype(BF16)

    mine = ((u_r,), (m_r, st_r))
    landed(u_r.at[pl.ds(0, N_GRP - 1), 0], recv_sem.at[2], "recv2")
    for c in range(2):

        @pl.when(core == c)
        def _(c=c):
            for i in (1, 3, 2):
                for part in mine[c]:
                    send(part.at[:, z], part.at[:, z], 4, 2 * lax.rem(z + i, 4) + core, g)

    def select(i):
        part = lax.rem(z + 4 - i, 4)
        landed(surf.at[0], recv_sem.at[18 + i], f"recv18_{i}")
        rows = surf[pl.ds(2 * part, 2)].reshape(128, 512)
        return jnp.dot(hits[part], rows, preferred_element_type=F32)

    chosen = select(0)
    chosen += select(1)
    chosen += select(3)
    chosen += select(2)
    sel[...] = jnp.concatenate(
        [chosen[:, f * 128 : (f + 1) * 128].reshape(CHUNKS, 8, 128) for f in range(4)], axis=1
    ).astype(BF16)
    def give(at, dst, own, phase, d):
        @pl.when(g != d)
        def _():
            send(sel.at[at], dst.at[g], phase, o, d)

        @pl.when(g == d)
        def _():
            own[d] = sel[at]

    for (d, c), helper in HELPERS.items():
        at = chunk_of(d) + c
        alone = jnp.logical_and(g == helper, core == 1)

        @pl.when(jnp.logical_not(alone))
        def _(at=at, helper=helper):
            send(sel.at[at], help_in.at[core, g], 22 + core, 2 * z + 1, helper)

        @pl.when(alone)
        def _(at=at, helper=helper):
            help_in[1, helper] = sel[at]

    for c in range(2):
        for d in (0, LAST):
            give(chunk_of(d) + c, slots_in.at[c], slots_in.at[c], (3, 9)[c], d)
    for d in range(1, LAST):
        give(chunk_of(d), slots_in.at[0], slots_in.at[0], 3, d)

    with jax.named_scope("t_copy"):
        t_copy.wait()
    lanes = lax.broadcasted_iota(jnp.int32, (L, 128), 1)
    for t in range(2):
        hy_s[0, t] = t_v[t, :, 0, :]
        hy_s[1, t] = t_v[t, :, 31, :]

        def gather(z, carry, t=t):
            west, east = carry
            tile = t_v[t, z]
            west = jnp.where(lanes == z, pltpu.roll(tile[:, 0:128], z, 1), west)
            east = jnp.where(lanes == z, pltpu.roll(tile[:, 128:256], z + 1, 1), east)
            return west, east

        zero = jnp.zeros((L, 128), F32)
        west, east = lax.fori_loop(0, L, gather, (zero, zero), unroll=8)
        hx_s[0, t] = west
        hx_s[1, t] = east

    def halo(src, dst, which, ocn, grp):
        return pltpu.make_async_remote_copy(
            src_ref=src,
            dst_ref=dst,
            send_sem=halo_send.at[which],
            recv_sem=halo_recv.at[which],
            device_id={"ocn": ocn, "grp": grp},
            device_id_type=MESH,
        )

    halos = (
        (o > 0, o < N_OCN - 1, halo(hx_s.at[0], hx_r.at[0], 0, jnp.maximum(o - 1, 0), g)),
        (o < N_OCN - 1, o > 0, halo(hx_s.at[1], hx_r.at[1], 1, jnp.minimum(o + 1, N_OCN - 1), g)),
        (g > 0, g < LAST, halo(hy_s.at[0], hy_r.at[0], 2, o, jnp.maximum(g - 1, 0))),
        (g < LAST, g > 0, halo(hy_s.at[1], hy_r.at[1], 3, o, jnp.minimum(g + 1, LAST))),
    )
    def collected(part):
        total = jnp.zeros((32, 128), F32)
        for s in range(N_GRP):
            total += part[s].astype(F32)
        return total

    for (d, c), helper in HELPERS.items():

        @pl.when(jnp.logical_and(g == helper, core == 1))
        def _(d=d, c=c):
            landed(help_in.at[1, pl.ds(0, N_GRP - 1)], recv_sem.at[23], "recv23")
            help_out[1] = collected(help_in.at[1]).astype(BF16)
            send(help_out.at[1], helped.at[c - 2], 12, 2 * z + 1, d)
            landed(help_in.at[0], recv_sem.at[22], "recv22")
            help_out[0] = collected(help_in.at[0]).astype(BF16)
            send(help_out.at[0], helped.at[c - 2], 10, 2 * z, d)

    with jax.named_scope("w_copy"):
        w_copy.wait()

    def remap(count):
        out = [jnp.zeros((8, 128), F32)] * 4
        for c in range(count):
            if c < 2:
                landed(slots_in.at[0, pl.ds(0, N_GRP - 1)], recv_sem.at[(3, 9)[c]], f"recv3_{c}")
                xs[c] = collected(slots_in.at[c])
            else:
                if c == 2:
                    landed(helped, recv_sem.at[10 + 2 * core], "recv3_3")
                xs[c] = helped[c - 2].astype(F32)
            for r in range(4):
                x = [xs[c, pl.ds(4 * k + r, 4, stride=8), :] for k in range(2)]
                x = jnp.concatenate(x, axis=1)
                x = jnp.concatenate([x, jnp.zeros(x.shape, F32)], axis=0).astype(BF16)
                w = jnp.concatenate([w_v[r, 2 * c + k] for k in range(2)], axis=1)
                out[r] += lax.dot_general(x, w, (((1,), (1,)), ((), ())), preferred_element_type=F32)
        for r in range(4):
            q[0, 2 * r : 2 * r + 2] = out[r][0:2]
            q[1, 2 * r : 2 * r + 2] = out[r][2:4]

    @pl.when(polar)
    def _():
        remap(4)

    @pl.when(inner)
    def _():
        remap(1)

    tile = 8 * g + o
    m2[tile, pl.ds(0, 4, stride=2), :] = mass[z, core]
    m2[tile, pl.ds(1, 4, stride=2), :] = mass[z, core]
    chip = 4 * g + z
    base[chip, core] = m2[tile] * u_in[z, core] + wind[z, core] + q[1]

    def spread(order):
        for i in order:
            if i % 2 == 0:
                send(base.at[chip, core], base.at[chip, core], 6, to_o[i % 8], to_g[i // 8])

    pl.when(polar)(lambda: spread(FAR_FIRST))
    pl.when(inner)(lambda: spread(FAR_ALL))
    for sends, _, copy in halos:
        pl.when(sends)(lambda copy=copy: copy.start())


    landed(u_r.at[:, pl.ds(0, 3)], recv_sem.at[4], "recv4")
    for c in range(2):

        @pl.when(core == c)
        def _(c=c):
            for part in mine[c]:
                send(part, part, 5, partner, g)

    landed(u_r, recv_sem.at[5], "recv5")

    def twice(i, _):
        at = pl.ds(8 * i, 8)
        u_pad[pl.ds(8 * i + 1, 8)] = u_r[i].reshape(8, 8, 128)
        for to, part in ((m2, m_r), (st2, st_r)):
            once = part[i].reshape(8, 4, 128)
            to[at, pl.ds(0, 4, stride=2), :] = once
            to[at, pl.ds(1, 4, stride=2), :] = once
        return 0

    lax.fori_loop(0, N_GRP, twice, 0)

    tiles = TILES
    shape = (tiles, 8, 128)
    lane = lax.broadcasted_iota(jnp.int32, shape, 2)
    sub = lax.broadcasted_iota(jnp.int32, shape, 1)

    def dot(a, b):
        return jnp.sum(a * b, axis=0)

    def mean(acc):
        return jnp.sum(jnp.sum(acc, axis=1, keepdims=True), axis=0, keepdims=True) / (2.0 * 65536.0)

    us = (u_pad, g0_pad, u_pad, u_pad)
    fs = (f_a, f_b, f_a, None)
    ds = (None, d1, d2, None)
    gram = {}

    def g_at(k, i):
        return g0_pad[pl.ds(tiles * i + 1, tiles)] if k == 0 else (None, g1, g2, g3)[k][pl.ds(tiles * i, tiles)]

    def force(i):
        return base[pl.ds(tiles // 2 * i, tiles // 2)].reshape(shape)

    def drag(src, i, u):
        at = pl.ds(tiles * i, tiles)
        before = src[pl.ds(tiles * i, tiles)]
        after = src[pl.ds(tiles * i + 2, tiles)]
        up = pltpu.roll(jnp.where(sub >= 6, before, u), 2, 1)
        down = pltpu.roll(jnp.where(sub < 2, after, u), 6, 1)
        left = pltpu.roll(jnp.where(lane == 127, up, u), 1, 2)
        right = pltpu.roll(jnp.where(lane == 0, down, u), 127, 2)
        strain = 0.5 * (right - left)
        square = strain * strain
        other = jnp.where((sub & 1) == 1, pltpu.roll(square, 1, 1), pltpu.roll(square, 7, 1))
        return (0.5 * st2[at]) * lax.rsqrt(square + other + 0.25), left + right

    def ahead(i, _):
        at = pl.ds(tiles * i, tiles)
        zeta, both = drag(u_pad, i, u_pad[pl.ds(tiles * i + 1, tiles)])
        share = 1.0 / (m2[at] + 1.0 + 2.0 * zeta)
        d1[at] = share
        d2[at] = zeta * both * share
        return 0

    with jax.named_scope("ahead"):
        lax.fori_loop(0, N_ALL // tiles, ahead, 0, unroll=8)
    landed(base.at[pl.ds(0, N_ALL // 2 - 1), 0], recv_sem.at[6], "recv6")
    send(base.at[:, core], base.at[:, core], 13, partner, g)
    landed(base.at[:, 0], recv_sem.at[13], "recv13")

    for step in range(ITERS):

        def picard(i, sums, step=step):
            at = pl.ds(tiles * i, tiles)
            src = us[step]
            u = src[pl.ds(tiles * i + 1, tiles)]
            if step == 0:
                new = force(i) * d1[at] + d2[at]
                g0_pad[pl.ds(tiles * i + 1, tiles)] = new
                fs[0][at] = new - u
                return sums
            zeta, both = drag(src, i, u)
            new = (force(i) + zeta * both) / (m2[at] + 1.0 + 2.0 * zeta)
            res = new - u
            (None, g1, g2, g3)[step][at] = new
            diff = res - fs[step - 1][at]
            if step < ITERS - 1:
                fs[step][at] = res
                ds[step][at] = diff
            diffs = [ds[j][at] for j in range(1, step)] + [diff]
            terms = [dot(d, diff) for d in diffs] + [dot(d, res) for d in diffs]
            return tuple(s + t for s, t in zip(sums, terms))

        zeros = tuple(jnp.zeros((8, 128), F32) for _ in range(2 * step))
        with jax.named_scope(f"picard{step}"):
            sums = lax.fori_loop(0, N_ALL // tiles, picard, zeros, unroll=UNROLL)
        if step == 0:
            continue
        means = [mean(s) for s in sums]
        for j in range(step):
            gram[(j, step - 1)] = means[j]
        norms = [jnp.sqrt(gram[(j, j)] + 1e-6) for j in range(step)]
        rows = [
            [
                gram[(min(a, b), max(a, b))] / (norms[a] * norms[b]) + (0.1 if a == b else 0.0)
                for b in range(step)
            ]
            + [means[step + a] / norms[a]]
            for a in range(step)
        ]
        for a in range(step):
            for b in range(a + 1, step):
                ratio = rows[b][a] / rows[a][a]
                rows[b] = [y - ratio * x for x, y in zip(rows[a], rows[b])]
        coef = [None] * step
        for a in reversed(range(step)):
            rest = rows[a][step]
            for b in range(a + 1, step):
                rest = rest - rows[a][b] * coef[b]
            coef[a] = rest / rows[a][a]
        scale = [jnp.broadcast_to(c / n, (8, 128))[None] for c, n in zip(coef, norms)]

        def combine(i, step=step, scale=scale):
            values = [g_at(j, i) for j in range(step + 1)]
            out = values[step]
            for j in range(step):
                out = out - scale[j] * (values[j + 1] - values[j])
            return out

        if step < ITERS - 1:

            def update(i, _, combine=combine):
                u_pad[pl.ds(tiles * i + 1, tiles)] = combine(i)
                return 0

            with jax.named_scope(f"update{step}"):
                lax.fori_loop(0, N_ALL // tiles, update, 0, unroll=UNROLL)
        else:
            for i in range(8 // tiles):
                ice[tiles * i : tiles * (i + 1)] = combine(8 // tiles * g + i)

    stress = ice[o] - q[1]
    for r in range(4):
        fx[r] = jnp.zeros((8, 128), F32)
        fx[r, 0:2] = stress[2 * r : 2 * r + 2]
        fx[r, 2:3] = 0.5 * (-0.05 * q[0, 2 * r + 1 : 2 * r + 2] - q[0, 2 * r : 2 * r + 1])

    lane1 = lax.broadcasted_iota(jnp.int32, (8, 128), 1)
    sub1 = lax.broadcasted_iota(jnp.int32, (8, 128), 0)

    def contribute(at, count, to):
        for r in range(4):
            x = fx[r].astype(BF16)
            w = jnp.concatenate([w_v[r, k] for k in range(2 * count)], axis=1)
            out = jnp.dot(x, w, preferred_element_type=F32)
            for k in range(2 * count):
                cbuf[k // 2, pl.ds((k % 2) * 4 + r, 3, stride=8), :] = out[0:3, 128 * k : 128 * (k + 1)]
        table = jnp.zeros((8, 128), F32)
        for c in range(count):
            values = cbuf[c].reshape(3, 8, 128)
            exponent = eighths(values)
            cq[1 + 3 * c : 4 + 3 * c] = counted(values, power(exponent))
            chunk = at + c
            own = lane1 == lax.rem(chunk, 16) * 8 + sub1
            for f in range(3):
                line = jnp.sum(jnp.where(own, exponent[f], 0.0), axis=0, keepdims=True)
                table += jnp.where(sub1 == 2 * f + chunk // 16, line, 0.0)
        cq[0] = table.astype(jnp.int32).astype(jnp.int16)
        planes = PLANES_1 if count == 1 else PLANES_4
        if planes > 1 + 3 * count:
            cq[planes - 1] = jnp.zeros((8, 128), jnp.int16)
        dst = crecv.at[pl.ds(to, planes)]
        over_grp(cq.at[pl.ds(0, planes)], dst, 7)
        crecv[pl.ds(to, planes)] = cq[0:planes]

    @pl.when(first)
    def _():
        contribute(0, 4, 0)

    @pl.when(last)
    def _():
        contribute(CHUNKS - 4, 4, PLANES - PLANES_4)

    @pl.when(inner)
    def _():
        contribute(3 + g, 1, PLANES_4 + PLANES_1 * (g - 1))

    with jax.named_scope("v_copy"):
        v_copy.wait()
    with jax.named_scope("halos"):
        for _, arrives, copy in halos:
            pl.when(arrives)(lambda copy=copy: copy.wait_recv())
    ys = lax.broadcasted_iota(jnp.int32, (L, 256), 0)
    cols = lax.broadcasted_iota(jnp.int32, (L, 256), 1)

    def stencil(t):
        def level(z, _):
            c = t_v[t, z]
            up = jnp.where(z > 0, t_v[t, jnp.maximum(z - 1, 0)], 0.0)
            down = jnp.where(z < L - 1, t_v[t, jnp.minimum(z + 1, L - 1)], 0.0)
            he = pltpu.roll(hx_r[0, t], 127 - z, 1)
            hw = pltpu.roll(hx_r[1, t], lax.rem(128 - z, 128), 1)
            east = jnp.where(cols == 255, jnp.concatenate([he, he], axis=1), pltpu.roll(c, 255, 1))
            west = jnp.where(cols == 0, jnp.concatenate([hw, hw], axis=1), pltpu.roll(c, 1, 1))
            north = jnp.where(ys == L - 1, hy_r[0, t, pl.ds(z, 1), :], pltpu.roll(c, L - 1, 0))
            south = jnp.where(ys == 0, hy_r[1, t, pl.ds(z, 1), :], pltpu.roll(c, 1, 0))
            pre[t, z] = (
                c
                + 0.2 * (east + west + north + south - 4.0 * c)
                - 0.25 * (v_v[0, z] * (east - west) + v_v[1, z] * (north - south))
                + 0.2 * (up + down - 2.0 * c)
            )
            return 0

        lax.fori_loop(0, L, level, 0)

    with jax.named_scope("stencil0"):
        stencil(0)

    @pl.when(polar)
    def _():
        landed(crecv.at[pl.ds(0, PLANES - PLANES_4)], recv_sem.at[7], "recv7")

    @pl.when(inner)
    def _():
        landed(crecv.at[pl.ds(0, PLANES - PLANES_1)], recv_sem.at[7], "recv7")

    starts = [0] + [PLANES_4 + PLANES_1 * i for i in range(N_GRP - 2)] + [PLANES - PLANES_4]
    table = jnp.zeros((8, 128), F32)
    for start in starts:
        table += crecv[start].astype(jnp.int32).astype(F32)
    table = power(table)
    for f in range(3):
        values = []
        for d, start in enumerate(starts):
            values += [crecv[start + 1 + 3 * c + f] for c in range(chunks_of(d))]
        values = [x.astype(jnp.int32).astype(F32) for x in values]
        values = jnp.concatenate(values + [jnp.zeros((8 * (PADDED - CHUNKS), 128), F32)], axis=0)
        values = halves(values)
        step = jnp.concatenate([table[2 * f : 2 * f + 1], table[2 * f + 1 : 2 * f + 2]], axis=1)
        out = jnp.dot(hits_t[...] * step.astype(BF16), values, preferred_element_type=F32)
        out = (out[:, 0:128] + out[:, 128:256]).reshape(4, 2, 64, 128)
        dense[0, :, f] = out[:, 0]
        dense[1, :, f] = out[:, 1]
    send(dense.at[1 - core], pair_in, 8, partner, g)
    landed(pair_in, recv_sem.at[8], "recv8")
    lane64 = lax.broadcasted_iota(jnp.int32, (64, 128), 1)
    row64 = lax.broadcasted_iota(jnp.int32, (64, 128), 0)
    for i in (1, 3, 2):
        to = lax.rem(z + i, 4)
        total = pair_in[to] + dense[core, to]
        step = power(eighths(total))
        pair_q[to] = counted(total, step)
        for f in range(3):
            line = jnp.sum(jnp.where(lane64 == row64, step[f], 0.0), axis=0, keepdims=True)
            pair_steps[to, f : f + 1] = line
        send(pair_q.at[to], dense_in.at[i - 1], 11, 2 * to + core, g)
        send(pair_steps.at[to], dense_steps.at[i - 1], 14, 2 * to + core, g)
    with jax.named_scope("stencil1"):
        stencil(1)
    landed(dense_in.at[pl.ds(0, 3)], recv_sem.at[11], "recv11")
    landed(dense_steps.at[pl.ds(0, 3)], recv_sem.at[14], "recv14")
    for f in range(3):
        out = pair_in[z, f] + dense[core, z, f]
        for i in range(3):
            step = jnp.where(lane64 == row64, dense_steps[i, f : f + 1], 0.0)
            step = jnp.sum(step, axis=1, keepdims=True)
            out += step * dense_in[i, f].astype(jnp.int32).astype(F32)
        flux[f, :, 0:128] = out[0:32]
        flux[f, :, 128:256] = out[32:64]

    for phase in (15, 16, 17, 18, 19, 20, 21):
        landed(surf.at[0], send_sem.at[phase])
    landed(base.at[pl.ds(0, N_ALL // 2 - 1), 0], send_sem.at[6])
    landed(base.at[:, 0], send_sem.at[13])
    landed(pair_in, send_sem.at[8])
    landed(dense_in.at[pl.ds(0, 3)], send_sem.at[11])
    landed(dense_steps.at[pl.ds(0, 3)], send_sem.at[14])

    landed(u_r.at[pl.ds(0, N_GRP - 1), 0], send_sem.at[2])
    landed(u_r.at[:, pl.ds(0, 3)], send_sem.at[4])
    landed(u_r, send_sem.at[5])

    @pl.when(polar)
    def _():
        landed(g1.at[pl.ds(0, 4 * (N_GRP - 1))], send_sem.at[1])
        landed(sel.at[pl.ds(0, 15)], send_sem.at[3])
        landed(sel.at[0], send_sem.at[9])
        landed(g1.at[pl.ds(0, 7 * (N_GRP - 1))], send_sem.at[7])

    @pl.when(inner)
    def _():
        landed(g1.at[pl.ds(0, N_GRP - 1)], send_sem.at[1])
        landed(sel.at[pl.ds(0, 15)], send_sem.at[3])
        landed(sel.at[pl.ds(0, 2)], send_sem.at[9])
        landed(crecv.at[pl.ds(0, 4 * (N_GRP - 1))], send_sem.at[7])

    helps = functools.reduce(jnp.logical_or, [g == d for d in HELPERS.values()])

    helps = jnp.logical_and(helps, core == 1)

    @pl.when(helps)
    def _():
        landed(sel.at[pl.ds(0, 3)], send_sem.at[23])
        landed(sel.at[0], send_sem.at[10])
        landed(sel.at[0], send_sem.at[12])

    @pl.when(jnp.logical_not(helps))
    def _():
        landed(sel.at[pl.ds(0, 4)], send_sem.at[22 + core])

    for sends, _, copy in halos:
        pl.when(sends)(lambda copy=copy: copy.wait_send())


def finish(pre, flux, ice, tracers_out, flux_out, ice_out, top, sem):
    copies = [
        pltpu.make_async_copy(pre.at[1], tracers_out.at[1], sem.at[0]),
        pltpu.make_async_copy(pre.at[0, pl.ds(1, L - 1)], tracers_out.at[0, pl.ds(1, L - 1)], sem.at[1]),
        pltpu.make_async_copy(flux, flux_out, sem.at[2]),
        pltpu.make_async_copy(ice, ice_out, sem.at[3]),
    ]
    for copy in copies:
        copy.start()
    top[...] = pre[0, 0] + 0.5 * flux[2]
    last = pltpu.make_async_copy(top, tracers_out.at[0, 0], sem.at[4])
    last.start()
    for copy in copies + [last]:
        copy.wait()


def on_device(
    tracers,
    velocity,
    remap_weights,
    remap_blocks,
    remap_count,
    ice_velocity,
    ice_mass_rate,
    ice_strength,
    wind_stress,
):
    def tiled(x):
        return x.reshape(2, 32, 128).transpose(1, 0, 2).reshape(4, 2, 8, 128)

    hbm = pl.BlockSpec(memory_space=pltpu.HBM)
    smem = pl.BlockSpec(memory_space=pltpu.SMEM)
    vmem = pl.BlockSpec(memory_space=pltpu.VMEM)
    scratch = [
        pltpu.SMEM((8, 32), jnp.int32),
        pltpu.SMEM((32,), jnp.int32),
        pltpu.VMEM((4, 2, 8, 128), F32),
        pltpu.VMEM((4, 2, 8, 128), F32),
        pltpu.VMEM((4, 2, 4, 128), F32),
        pltpu.VMEM((4, 2, 4, 128), F32),
        pltpu.VMEM((2, L, 32, 256), F32),
        pltpu.VMEM((2, L, 32, 256), F32),
        pltpu.VMEM((4, 8, 128, 128), BF16),
        pltpu.VMEM((4, 32, 256), F32),
        pltpu.VMEM((N_OCN, 64, 512), BF16),
        pltpu.VMEM((PADDED, 8, 128), jnp.int32),
        pltpu.VMEM((4, CHUNKS * 8, 128), BF16),
        pltpu.VMEM((512, 256), BF16),
        pltpu.VMEM((CHUNKS, 32, 128), BF16),
        pltpu.VMEM((2, N_GRP, 32, 128), BF16),
        pltpu.VMEM((2, N_GRP, 32, 128), BF16),
        pltpu.VMEM((2, 32, 128), BF16),
        pltpu.VMEM((2, 32, 128), BF16),
        pltpu.VMEM((4, 32, 128), F32),
        pltpu.VMEM((2, 8, 128), F32),
        pltpu.VMEM((2, 2, L, 128), F32),
        pltpu.VMEM((2, 2, L, 128), F32),
        pltpu.VMEM((2, 2, L, 256), F32),
        pltpu.VMEM((2, 2, L, 256), F32),
        pltpu.VMEM((N_GRP, 4, 2, 8, 128), F32),
        pltpu.VMEM((N_ALL + 2, 8, 128), F32),
        pltpu.VMEM((N_GRP, 4, 2, 4, 128), F32),
        pltpu.VMEM((N_GRP, 4, 2, 4, 128), F32),
        pltpu.VMEM((N_ALL, 8, 128), F32),
        pltpu.VMEM((N_ALL, 8, 128), F32),
        pltpu.VMEM((N_ALL // 2, 2, 8, 128), F32),
        pltpu.VMEM((N_ALL + 2, 8, 128), F32),
        *[pltpu.VMEM((N_ALL, 8, 128), F32)] * 7,
        pltpu.VMEM((4, 8, 128), F32),
        pltpu.VMEM((4, 24, 128), F32),
        pltpu.VMEM((PLANES_4, 8, 128), jnp.int16),
        pltpu.VMEM((PLANES, 8, 128), jnp.int16),
        pltpu.VMEM((2, 4, 3, 64, 128), F32),
        pltpu.VMEM((4, 3, 64, 128), F32),
        pltpu.VMEM((4, 3, 64, 128), jnp.int16),
        pltpu.VMEM((4, 3, 64, 128), jnp.int16),
        pltpu.VMEM((4, 8, 128), F32),
        pltpu.VMEM((4, 8, 128), F32),
        pltpu.SemaphoreType.DMA((16,)),
        pltpu.SemaphoreType.DMA((24,)),
        pltpu.SemaphoreType.DMA((24,)),
        pltpu.SemaphoreType.DMA((4,)),
        pltpu.SemaphoreType.DMA((4,)),
    ]
    pre, flux, ice = pl.pallas_call(
        kernel,
        out_shape=(
            jax.ShapeDtypeStruct((2, L, 32, 256), F32),
            jax.ShapeDtypeStruct((3, 32, 256), F32),
            jax.ShapeDtypeStruct((8, 8, 128), F32),
        ),
        in_specs=[hbm] * 9,
        out_specs=(vmem, vmem, vmem),
        scratch_shapes=scratch,
        compiler_params=pltpu.CompilerParams(
            collective_id=0, has_side_effects=True, vmem_limit_bytes=40 * 1024 * 1024
        ),
    )(
        *(
            pltpu.with_memory_space_constraint(x, pltpu.HBM)
            for x in (
                tracers,
                velocity,
                remap_weights,
                remap_blocks.T,
                remap_count,
                tiled(ice_velocity),
                tiled(wind_stress),
                ice_mass_rate.reshape(4, 2, 4, 128),
                ice_strength.reshape(4, 2, 4, 128),
            )
        )
    )
    tracers_next, flux, ice = pl.pallas_call(
        finish,
        out_shape=(
            jax.ShapeDtypeStruct((2, L, 32, 256), F32),
            jax.ShapeDtypeStruct((3, 32, 256), F32),
            jax.ShapeDtypeStruct((8, 8, 128), F32),
        ),
        in_specs=[vmem] * 3,
        out_specs=(hbm, hbm, hbm),
        scratch_shapes=[pltpu.VMEM((32, 256), F32), pltpu.SemaphoreType.DMA((5,))],
        compiler_params=pltpu.CompilerParams(vmem_limit_bytes=8 * 1024 * 1024),
    )(pre, flux, ice)
    ice_final = ice.reshape(32, 2, 128).transpose(1, 0, 2).reshape(2, 4096)
    return tracers_next, flux, ice_final


def solution(mesh):
    placed = (
        P(None, None, "grp", "ocn"),
        P(None, None, "grp", "ocn"),
        P("grp", None, None, None),
        P("grp", None),
        P("grp"),
        P(None, "grp"),
        P("grp"),
        P("grp"),
        P(None, "grp"),
    )
    return jax.shard_map(
        on_device,
        mesh=mesh,
        in_specs=placed,
        out_specs=(P(None, None, "grp", "ocn"), P(None, "grp", "ocn"), P(None, "grp")),
        check_vma=False,
    )
```

```python
import functools

import jax
import jax.numpy as jnp
from jax import lax
from jax.experimental import pallas as pl
from jax.experimental.pallas import tpu as pltpu
from jax.sharding import PartitionSpec as P

MESH = pl.DeviceIdType.MESH
F32 = jnp.float32
BF16 = jnp.bfloat16
N_OCN = 8
N_GRP = 16
N_ALL = N_OCN * N_GRP
LAST = N_GRP - 1
L = 32
CHUNKS = 22
PADDED = 32
PLANES_1, PLANES_4 = 4, 14
PLANES = 2 * PLANES_4 + (N_GRP - 2) * PLANES_1
ITERS = 4
TILES = 4
UNROLL = 32


def hops(*shifts):
    return sum(min(i, 4 - i) for i in shifts)


FAR_GRP = sorted(range(1, N_GRP), key=lambda i: -hops(i // 4, i % 4))
FAR_ALL = sorted(range(1, N_ALL), key=lambda i: (-hops(i // 32, i // 8 % 4, i // 2 % 4) // 2, (i * 37) % 128))
HELPERS = {(0, 2): 1, (0, 3): 4, (LAST, 2): LAST - 1, (LAST, 3): LAST - 4}
FAR_FIRST = sorted(range(1, N_ALL), key=lambda i: -hops(i // 32, i // 8 % 4, i // 2 % 4))


def chunk_of(g):
    return 0 if g == 0 else (CHUNKS - 4 if g == LAST else 3 + g)


def chunks_of(g):
    return 4 if g in (0, LAST) else 1


def power(x):
    return jnp.exp2(0.125 * x).astype(BF16).astype(F32)


def eighths(x):
    top = jnp.max(jnp.abs(x), axis=-1, keepdims=True)
    return jnp.ceil(8.0 * jnp.log2(jnp.maximum(top * (1.0 / 32000.0), 1e-37)))


def counted(x, step):
    return jnp.floor(x * (1.0 / step) + 0.5).astype(jnp.int32).astype(jnp.int16)


def halves(x):
    high = x.astype(BF16)
    return jnp.concatenate([high, (x - high.astype(F32)).astype(BF16)], axis=-1)


def landed(ref, sem, name="left"):
    with jax.named_scope(name):
        pltpu.make_async_copy(ref, ref, sem).wait()


def kernel(
    tracers,
    velocity,
    weights,
    blocks_hbm,
    counts_hbm,
    u_hbm,
    wind_hbm,
    mass_hbm,
    strength_hbm,
    pre,
    flux,
    ice,
    blocks,
    counts,
    u_in,
    wind,
    mass,
    strength,
    t_v,
    v_v,
    w_v,
    level0,
    surf,
    codes,
    hits,
    hits_t,
    sel,
    slots_in,
    help_in,
    help_out,
    helped,
    xs,
    q,
    hx_s,
    hx_r,
    hy_s,
    hy_r,
    u_r,
    u_pad,
    m_r,
    st_r,
    m2,
    st2,
    base,
    g0_pad,
    g1,
    g2,
    g3,
    f_a,
    f_b,
    d1,
    d2,
    fx,
    cbuf,
    cq,
    crecv,
    dense,
    pair_in,
    pair_q,
    dense_in,
    pair_steps,
    dense_steps,
    local_sem,
    send_sem,
    recv_sem,
    halo_send,
    halo_recv,
):
    o = lax.axis_index("ocn")
    g = lax.axis_index("grp")
    z, core = o // 2, lax.rem(o, 2)
    partner = o + 1 - 2 * core
    first, last = g == 0, g == LAST
    polar = jnp.logical_or(first, last)
    inner = jnp.logical_and(g > 0, g < LAST)

    def send(src, dst, phase, ocn, grp):
        pltpu.make_async_remote_copy(
            src_ref=src,
            dst_ref=dst,
            send_sem=send_sem.at[phase],
            recv_sem=recv_sem.at[phase],
            device_id={"ocn": ocn, "grp": grp},
            device_id_type=MESH,
        ).start()

    gx, gy = g // 4, lax.rem(g, 4)
    to_x = [lax.rem(gx + i, 4) for i in range(4)]
    to_y = [lax.rem(gy + i, 4) for i in range(4)]
    to_o = [2 * lax.rem(z + i, 4) + (core if c == 0 else 1 - core) for i in range(4) for c in range(2)]
    to_g = [4 * to_x[i] + to_y[j] for i in range(4) for j in range(4)]

    def over_grp(src, dst, phase):
        for i in FAR_GRP:
            send(src, dst, phase, o, to_g[i])

    barrier = pltpu.get_barrier_semaphore()
    for i in range(1, N_GRP):
        pl.semaphore_signal(
            barrier, inc=1, device_id={"ocn": o, "grp": lax.rem(g + i, N_GRP)}, device_id_type=MESH
        )
    for i in range(1, N_OCN):
        pl.semaphore_signal(
            barrier, inc=1, device_id={"ocn": lax.rem(o + i, N_OCN), "grp": g}, device_id_type=MESH
        )

    small = [
        pltpu.make_async_copy(tracers.at[0, 0], level0.at[0], local_sem.at[0]),
        pltpu.make_async_copy(tracers.at[1, 0], level0.at[1], local_sem.at[1]),
        pltpu.make_async_copy(velocity.at[0, 0], level0.at[2], local_sem.at[2]),
        pltpu.make_async_copy(velocity.at[1, 0], level0.at[3], local_sem.at[3]),
    ]
    for copy in small:
        copy.start()
    index_copies = [
        pltpu.make_async_copy(blocks_hbm, blocks, local_sem.at[7]),
        pltpu.make_async_copy(counts_hbm, counts, local_sem.at[8]),
    ]
    ice_copies = [
        pltpu.make_async_copy(u_hbm, u_in, local_sem.at[9]),
        pltpu.make_async_copy(wind_hbm, wind, local_sem.at[10]),
        pltpu.make_async_copy(mass_hbm, mass, local_sem.at[11]),
        pltpu.make_async_copy(strength_hbm, strength, local_sem.at[12]),
    ]
    for copy in index_copies + ice_copies:
        copy.start()
    t_copy = pltpu.make_async_copy(tracers, t_v, local_sem.at[4])
    v_copy = pltpu.make_async_copy(velocity, v_v, local_sem.at[5])
    w_copy = pltpu.make_async_copy(weights.at[pl.ds(4 * o, 4)], w_v, local_sem.at[6])
    t_copy.start()
    w_copy.start()
    v_copy.start()

    def fill_codes(at, count):
        for k in range(2 * count):
            for r in range(4):
                block = blocks[k, 4 * o + r]
                code = jnp.where(k < counts[4 * o + r], block, -1)
                codes[at + k // 2, pl.ds((k % 2) * 4 + r, 1), :] = jnp.full((1, 128), code, jnp.int32)

    for copy in index_copies:
        copy.wait()

    @pl.when(first)
    def _():
        fill_codes(0, 4)

    @pl.when(last)
    def _():
        fill_codes(CHUNKS - 4, 4)

    @pl.when(inner)
    def _():
        fill_codes(3 + g, 1)

    codes[pl.ds(CHUNKS, PADDED - CHUNKS)] = jnp.full((PADDED - CHUNKS, 8, 128), -1, jnp.int32)
    u_pad[0] = jnp.zeros((8, 128), F32)
    u_pad[N_ALL + 1] = jnp.zeros((8, 128), F32)
    for copy in ice_copies:
        copy.wait()
    g0_pad[0] = jnp.zeros((8, 128), F32)
    g0_pad[N_ALL + 1] = jnp.zeros((8, 128), F32)

    @pl.when(core == 0)
    def _():
        u_r[g, z] = u_in[z]

    @pl.when(core == 1)
    def _():
        m_r[g, z] = mass[z]
        st_r[g, z] = strength[z]


    @pl.when(o == N_OCN - 1)
    def _():
        hx_r[0] = jnp.zeros((2, L, 128), F32)

    @pl.when(o == 0)
    def _():
        hx_r[1] = jnp.zeros((2, L, 128), F32)

    @pl.when(last)
    def _():
        hy_r[0] = jnp.zeros((2, L, 256), F32)

    @pl.when(first)
    def _():
        hy_r[1] = jnp.zeros((2, L, 256), F32)

    for copy in small:
        copy.wait()
    for f in range(4):
        field = level0[f]
        surf[o, 0:32, f * 128 : (f + 1) * 128] = field[:, 0:128].astype(BF16)
        surf[o, 32:64, f * 128 : (f + 1) * 128] = field[:, 128:256].astype(BF16)
    with jax.named_scope("barrier"):
        pl.semaphore_wait(barrier, N_GRP - 1 + N_OCN - 1)

    for i in (2, 1, 3):
        send(surf.at[o], surf.at[o], 14 + i, 2 * lax.rem(z + i, 4) + core, g)
    send(surf.at[o], surf.at[o], 18, partner, g)

    @pl.when(first)
    def _():
        part = codes.at[pl.ds(0, 4)]
        over_grp(part, part, 1)

    @pl.when(last)
    def _():
        part = codes.at[pl.ds(CHUNKS - 4, 4)]
        over_grp(part, part, 1)

    @pl.when(inner)
    def _():
        part = codes.at[pl.ds(3 + g, 1)]
        over_grp(part, part, 1)

    @pl.when(core == 0)
    def _():
        over_grp(u_in.at[z], u_r.at[g, z], 2)

    @pl.when(core == 1)
    def _():
        over_grp(mass.at[z], m_r.at[g, z], 2)
        over_grp(strength.at[z], st_r.at[g, z], 2)

    def pass_on(i):
        part = surf.at[2 * lax.rem(z + 4 - i, 4) + core]
        landed(part, recv_sem.at[14 + i], f"recv0_{i}")
        send(part, part, 18 + i, partner, g)

    pass_on(1)
    pass_on(3)
    pass_on(2)

    @pl.when(polar)
    def _():
        landed(codes.at[pl.ds(0, CHUNKS - 4)], recv_sem.at[1], "recv1")

    @pl.when(inner)
    def _():
        landed(codes.at[pl.ds(0, CHUNKS - 1)], recv_sem.at[1], "recv1")

    code = codes[...].reshape(PADDED * 8, 128)
    here = jnp.logical_and(code >= 0, ((code >> 6) & (N_GRP - 1)) == g)
    row = ((code >> 10) << 6) + ((code & 1) << 5) + ((code & 63) >> 1)
    row = jnp.where(here, row, -1)
    lane8 = lax.broadcasted_iota(jnp.int32, (CHUNKS * 8, 128), 1)
    for part in range(4):
        hit = row[: CHUNKS * 8] == lane8 + 128 * part
        hits[part] = jnp.where(hit, 1.0, 0.0).astype(BF16)
    row_f = row.astype(F32)
    row_t = jnp.concatenate([row_f[0:128].T[0:1], row_f[128:256].T[0:1]], axis=1)
    for part in range(8):
        ids = lax.broadcasted_iota(jnp.int32, (64, 256), 0).astype(F32) + 64.0 * part
        hits_t[part * 64 : (part + 1) * 64] = jnp.where(ids == row_t, 1.0, 0.0).astype(BF16)

    mine = ((u_r,), (m_r, st_r))
    landed(u_r.at[pl.ds(0, N_GRP - 1), 0], recv_sem.at[2], "recv2")
    for c in range(2):

        @pl.when(core == c)
        def _(c=c):
            for i in (1, 3, 2):
                for part in mine[c]:
                    send(part.at[:, z], part.at[:, z], 4, 2 * lax.rem(z + i, 4) + core, g)

    def select(i):
        part = lax.rem(z + 4 - i, 4)
        landed(surf.at[0], recv_sem.at[18 + i], f"recv18_{i}")
        rows = surf[pl.ds(2 * part, 2)].reshape(128, 512)
        return jnp.dot(hits[part], rows, preferred_element_type=F32)

    chosen = select(0)
    chosen += select(1)
    chosen += select(3)
    chosen += select(2)
    sel[...] = jnp.concatenate(
        [chosen[:, f * 128 : (f + 1) * 128].reshape(CHUNKS, 8, 128) for f in range(4)], axis=1
    ).astype(BF16)
    def give(at, dst, own, phase, d):
        @pl.when(g != d)
        def _():
            send(sel.at[at], dst.at[g], phase, o, d)

        @pl.when(g == d)
        def _():
            own[d] = sel[at]

    for (d, c), helper in HELPERS.items():
        at = chunk_of(d) + c
        alone = jnp.logical_and(g == helper, core == 1)

        @pl.when(jnp.logical_not(alone))
        def _(at=at, helper=helper):
            send(sel.at[at], help_in.at[core, g], 22 + core, 2 * z + 1, helper)

        @pl.when(alone)
        def _(at=at, helper=helper):
            help_in[1, helper] = sel[at]

    for c in range(2):
        for d in (0, LAST):
            give(chunk_of(d) + c, slots_in.at[c], slots_in.at[c], (3, 9)[c], d)
    for d in range(1, LAST):
        give(chunk_of(d), slots_in.at[0], slots_in.at[0], 3, d)

    with jax.named_scope("t_copy"):
        t_copy.wait()
    lanes = lax.broadcasted_iota(jnp.int32, (L, 128), 1)
    for t in range(2):
        hy_s[0, t] = t_v[t, :, 0, :]
        hy_s[1, t] = t_v[t, :, 31, :]

        def gather(z, carry, t=t):
            west, east = carry
            tile = t_v[t, z]
            west = jnp.where(lanes == z, pltpu.roll(tile[:, 0:128], z, 1), west)
            east = jnp.where(lanes == z, pltpu.roll(tile[:, 128:256], z + 1, 1), east)
            return west, east

        zero = jnp.zeros((L, 128), F32)
        west, east = lax.fori_loop(0, L, gather, (zero, zero), unroll=8)
        hx_s[0, t] = west
        hx_s[1, t] = east

    def halo(src, dst, which, ocn, grp):
        return pltpu.make_async_remote_copy(
            src_ref=src,
            dst_ref=dst,
            send_sem=halo_send.at[which],
            recv_sem=halo_recv.at[which],
            device_id={"ocn": ocn, "grp": grp},
            device_id_type=MESH,
        )

    halos = (
        (o > 0, o < N_OCN - 1, halo(hx_s.at[0], hx_r.at[0], 0, jnp.maximum(o - 1, 0), g)),
        (o < N_OCN - 1, o > 0, halo(hx_s.at[1], hx_r.at[1], 1, jnp.minimum(o + 1, N_OCN - 1), g)),
        (g > 0, g < LAST, halo(hy_s.at[0], hy_r.at[0], 2, o, jnp.maximum(g - 1, 0))),
        (g < LAST, g > 0, halo(hy_s.at[1], hy_r.at[1], 3, o, jnp.minimum(g + 1, LAST))),
    )
    def collected(part):
        total = jnp.zeros((32, 128), F32)
        for s in range(N_GRP):
            total += part[s].astype(F32)
        return total

    for (d, c), helper in HELPERS.items():

        @pl.when(jnp.logical_and(g == helper, core == 1))
        def _(d=d, c=c):
            landed(help_in.at[1, pl.ds(0, N_GRP - 1)], recv_sem.at[23], "recv23")
            help_out[1] = collected(help_in.at[1]).astype(BF16)
            send(help_out.at[1], helped.at[c - 2], 12, 2 * z + 1, d)
            landed(help_in.at[0], recv_sem.at[22], "recv22")
            help_out[0] = collected(help_in.at[0]).astype(BF16)
            send(help_out.at[0], helped.at[c - 2], 10, 2 * z, d)

    with jax.named_scope("w_copy"):
        w_copy.wait()

    def remap(count):
        out = [jnp.zeros((8, 128), F32)] * 4
        for c in range(count):
            if c < 2:
                landed(slots_in.at[0, pl.ds(0, N_GRP - 1)], recv_sem.at[(3, 9)[c]], f"recv3_{c}")
                xs[c] = collected(slots_in.at[c])
            else:
                if c == 2:
                    landed(helped, recv_sem.at[10 + 2 * core], "recv3_3")
                xs[c] = helped[c - 2].astype(F32)
            for r in range(4):
                x = [xs[c, pl.ds(4 * k + r, 4, stride=8), :] for k in range(2)]
                x = jnp.concatenate(x, axis=1)
                x = jnp.concatenate([x, jnp.zeros(x.shape, F32)], axis=0).astype(BF16)
                w = jnp.concatenate([w_v[r, 2 * c + k] for k in range(2)], axis=1)
                out[r] += lax.dot_general(x, w, (((1,), (1,)), ((), ())), preferred_element_type=F32)
        for r in range(4):
            q[0, 2 * r : 2 * r + 2] = out[r][0:2]
            q[1, 2 * r : 2 * r + 2] = out[r][2:4]

    @pl.when(polar)
    def _():
        remap(4)

    @pl.when(inner)
    def _():
        remap(1)

    tile = 8 * g + o
    m2[tile, pl.ds(0, 4, stride=2), :] = mass[z, core]
    m2[tile, pl.ds(1, 4, stride=2), :] = mass[z, core]
    chip = 4 * g + z
    base[chip, core] = m2[tile] * u_in[z, core] + wind[z, core] + q[1]

    def spread(order):
        for i in order:
            if i % 2 == 0:
                send(base.at[chip, core], base.at[chip, core], 6, to_o[i % 8], to_g[i // 8])

    pl.when(polar)(lambda: spread(FAR_FIRST))
    pl.when(inner)(lambda: spread(FAR_ALL))
    for sends, _, copy in halos:
        pl.when(sends)(lambda copy=copy: copy.start())


    landed(u_r.at[:, pl.ds(0, 3)], recv_sem.at[4], "recv4")
    for c in range(2):

        @pl.when(core == c)
        def _(c=c):
            for part in mine[c]:
                send(part, part, 5, partner, g)

    landed(u_r, recv_sem.at[5], "recv5")

    def twice(i, _):
        at = pl.ds(8 * i, 8)
        u_pad[pl.ds(8 * i + 1, 8)] = u_r[i].reshape(8, 8, 128)
        for to, part in ((m2, m_r), (st2, st_r)):
            once = part[i].reshape(8, 4, 128)
            to[at, pl.ds(0, 4, stride=2), :] = once
            to[at, pl.ds(1, 4, stride=2), :] = once
        return 0

    lax.fori_loop(0, N_GRP, twice, 0)

    tiles = TILES
    shape = (tiles, 8, 128)
    lane = lax.broadcasted_iota(jnp.int32, shape, 2)
    sub = lax.broadcasted_iota(jnp.int32, shape, 1)

    def dot(a, b):
        return jnp.sum(a * b, axis=0)

    def mean(acc):
        return jnp.sum(jnp.sum(acc, axis=1, keepdims=True), axis=0, keepdims=True) / (2.0 * 65536.0)

    us = (u_pad, g0_pad, u_pad, u_pad)
    fs = (f_a, f_b, f_a, None)
    ds = (None, d1, d2, None)
    gram = {}

    def g_at(k, i):
        return g0_pad[pl.ds(tiles * i + 1, tiles)] if k == 0 else (None, g1, g2, g3)[k][pl.ds(tiles * i, tiles)]

    def force(i):
        return base[pl.ds(tiles // 2 * i, tiles // 2)].reshape(shape)

    def drag(src, i, u):
        at = pl.ds(tiles * i, tiles)
        before = src[pl.ds(tiles * i, tiles)]
        after = src[pl.ds(tiles * i + 2, tiles)]
        up = pltpu.roll(jnp.where(sub >= 6, before, u), 2, 1)
        down = pltpu.roll(jnp.where(sub < 2, after, u), 6, 1)
        left = pltpu.roll(jnp.where(lane == 127, up, u), 1, 2)
        right = pltpu.roll(jnp.where(lane == 0, down, u), 127, 2)
        strain = 0.5 * (right - left)
        square = strain * strain
        other = jnp.where((sub & 1) == 1, pltpu.roll(square, 1, 1), pltpu.roll(square, 7, 1))
        return (0.5 * st2[at]) * lax.rsqrt(square + other + 0.25), left + right

    def ahead(i, _):
        at = pl.ds(tiles * i, tiles)
        zeta, both = drag(u_pad, i, u_pad[pl.ds(tiles * i + 1, tiles)])
        share = 1.0 / (m2[at] + 1.0 + 2.0 * zeta)
        d1[at] = share
        d2[at] = zeta * both * share
        return 0

    with jax.named_scope("ahead"):
        lax.fori_loop(0, N_ALL // tiles, ahead, 0, unroll=8)
    landed(base.at[pl.ds(0, N_ALL // 2 - 1), 0], recv_sem.at[6], "recv6")
    send(base.at[:, core], base.at[:, core], 13, partner, g)
    landed(base.at[:, 0], recv_sem.at[13], "recv13")

    for step in range(ITERS):

        def picard(i, sums, step=step):
            at = pl.ds(tiles * i, tiles)
            src = us[step]
            u = src[pl.ds(tiles * i + 1, tiles)]
            if step == 0:
                new = force(i) * d1[at] + d2[at]
                g0_pad[pl.ds(tiles * i + 1, tiles)] = new
                fs[0][at] = new - u
                return sums
            zeta, both = drag(src, i, u)
            new = (force(i) + zeta * both) / (m2[at] + 1.0 + 2.0 * zeta)
            res = new - u
            (None, g1, g2, g3)[step][at] = new
            diff = res - fs[step - 1][at]
            if step < ITERS - 1:
                fs[step][at] = res
                ds[step][at] = diff
            diffs = [ds[j][at] for j in range(1, step)] + [diff]
            terms = [dot(d, diff) for d in diffs] + [dot(d, res) for d in diffs]
            return tuple(s + t for s, t in zip(sums, terms))

        zeros = tuple(jnp.zeros((8, 128), F32) for _ in range(2 * step))
        with jax.named_scope(f"picard{step}"):
            sums = lax.fori_loop(0, N_ALL // tiles, picard, zeros, unroll=UNROLL)
        if step == 0:
            continue
        means = [mean(s) for s in sums]
        for j in range(step):
            gram[(j, step - 1)] = means[j]
        norms = [jnp.sqrt(gram[(j, j)] + 1e-6) for j in range(step)]
        rows = [
            [
                gram[(min(a, b), max(a, b))] / (norms[a] * norms[b]) + (0.1 if a == b else 0.0)
                for b in range(step)
            ]
            + [means[step + a] / norms[a]]
            for a in range(step)
        ]
        for a in range(step):
            for b in range(a + 1, step):
                ratio = rows[b][a] / rows[a][a]
                rows[b] = [y - ratio * x for x, y in zip(rows[a], rows[b])]
        coef = [None] * step
        for a in reversed(range(step)):
            rest = rows[a][step]
            for b in range(a + 1, step):
                rest = rest - rows[a][b] * coef[b]
            coef[a] = rest / rows[a][a]
        scale = [jnp.broadcast_to(c / n, (8, 128))[None] for c, n in zip(coef, norms)]

        def combine(i, step=step, scale=scale):
            values = [g_at(j, i) for j in range(step + 1)]
            out = values[step]
            for j in range(step):
                out = out - scale[j] * (values[j + 1] - values[j])
            return out

        if step < ITERS - 1:

            def update(i, _, combine=combine):
                u_pad[pl.ds(tiles * i + 1, tiles)] = combine(i)
                return 0

            with jax.named_scope(f"update{step}"):
                lax.fori_loop(0, N_ALL // tiles, update, 0, unroll=UNROLL)
        else:
            for i in range(8 // tiles):
                ice[tiles * i : tiles * (i + 1)] = combine(8 // tiles * g + i)

    stress = ice[o] - q[1]
    for r in range(4):
        fx[r] = jnp.zeros((8, 128), F32)
        fx[r, 0:2] = stress[2 * r : 2 * r + 2]
        fx[r, 2:3] = 0.5 * (-0.05 * q[0, 2 * r + 1 : 2 * r + 2] - q[0, 2 * r : 2 * r + 1])

    lane1 = lax.broadcasted_iota(jnp.int32, (8, 128), 1)
    sub1 = lax.broadcasted_iota(jnp.int32, (8, 128), 0)

    def contribute(at, count, to):
        for r in range(4):
            x = fx[r].astype(BF16)
            w = jnp.concatenate([w_v[r, k] for k in range(2 * count)], axis=1)
            out = jnp.dot(x, w, preferred_element_type=F32)
            for k in range(2 * count):
                cbuf[k // 2, pl.ds((k % 2) * 4 + r, 3, stride=8), :] = out[0:3, 128 * k : 128 * (k + 1)]
        table = jnp.zeros((8, 128), F32)
        for c in range(count):
            values = cbuf[c].reshape(3, 8, 128)
            exponent = eighths(values)
            cq[1 + 3 * c : 4 + 3 * c] = counted(values, power(exponent))
            chunk = at + c
            own = lane1 == lax.rem(chunk, 16) * 8 + sub1
            for f in range(3):
                line = jnp.sum(jnp.where(own, exponent[f], 0.0), axis=0, keepdims=True)
                table += jnp.where(sub1 == 2 * f + chunk // 16, line, 0.0)
        cq[0] = table.astype(jnp.int32).astype(jnp.int16)
        planes = PLANES_1 if count == 1 else PLANES_4
        if planes > 1 + 3 * count:
            cq[planes - 1] = jnp.zeros((8, 128), jnp.int16)
        dst = crecv.at[pl.ds(to, planes)]
        over_grp(cq.at[pl.ds(0, planes)], dst, 7)
        crecv[pl.ds(to, planes)] = cq[0:planes]

    @pl.when(first)
    def _():
        contribute(0, 4, 0)

    @pl.when(last)
    def _():
        contribute(CHUNKS - 4, 4, PLANES - PLANES_4)

    @pl.when(inner)
    def _():
        contribute(3 + g, 1, PLANES_4 + PLANES_1 * (g - 1))

    with jax.named_scope("v_copy"):
        v_copy.wait()
    with jax.named_scope("halos"):
        for _, arrives, copy in halos:
            pl.when(arrives)(lambda copy=copy: copy.wait_recv())
    ys = lax.broadcasted_iota(jnp.int32, (L, 256), 0)
    cols = lax.broadcasted_iota(jnp.int32, (L, 256), 1)

    def stencil(t):
        def level(z, _):
            c = t_v[t, z]
            up = jnp.where(z > 0, t_v[t, jnp.maximum(z - 1, 0)], 0.0)
            down = jnp.where(z < L - 1, t_v[t, jnp.minimum(z + 1, L - 1)], 0.0)
            he = pltpu.roll(hx_r[0, t], 127 - z, 1)
            hw = pltpu.roll(hx_r[1, t], lax.rem(128 - z, 128), 1)
            east = jnp.where(cols == 255, jnp.concatenate([he, he], axis=1), pltpu.roll(c, 255, 1))
            west = jnp.where(cols == 0, jnp.concatenate([hw, hw], axis=1), pltpu.roll(c, 1, 1))
            north = jnp.where(ys == L - 1, hy_r[0, t, pl.ds(z, 1), :], pltpu.roll(c, L - 1, 0))
            south = jnp.where(ys == 0, hy_r[1, t, pl.ds(z, 1), :], pltpu.roll(c, 1, 0))
            pre[t, z] = (
                c
                + 0.2 * (east + west + north + south - 4.0 * c)
                - 0.25 * (v_v[0, z] * (east - west) + v_v[1, z] * (north - south))
                + 0.2 * (up + down - 2.0 * c)
            )
            return 0

        lax.fori_loop(0, L, level, 0)

    with jax.named_scope("stencil0"):
        stencil(0)

    @pl.when(polar)
    def _():
        landed(crecv.at[pl.ds(0, PLANES - PLANES_4)], recv_sem.at[7], "recv7")

    @pl.when(inner)
    def _():
        landed(crecv.at[pl.ds(0, PLANES - PLANES_1)], recv_sem.at[7], "recv7")

    starts = [0] + [PLANES_4 + PLANES_1 * i for i in range(N_GRP - 2)] + [PLANES - PLANES_4]
    table = jnp.zeros((8, 128), F32)
    for start in starts:
        table += crecv[start].astype(jnp.int32).astype(F32)
    table = power(table)
    for f in range(3):
        values = []
        for d, start in enumerate(starts):
            values += [crecv[start + 1 + 3 * c + f] for c in range(chunks_of(d))]
        values = [x.astype(jnp.int32).astype(F32) for x in values]
        values = jnp.concatenate(values + [jnp.zeros((8 * (PADDED - CHUNKS), 128), F32)], axis=0)
        values = halves(values)
        step = jnp.concatenate([table[2 * f : 2 * f + 1], table[2 * f + 1 : 2 * f + 2]], axis=1)
        out = jnp.dot(hits_t[...] * step.astype(BF16), values, preferred_element_type=F32)
        out = (out[:, 0:128] + out[:, 128:256]).reshape(4, 2, 64, 128)
        dense[0, :, f] = out[:, 0]
        dense[1, :, f] = out[:, 1]
    pair_phase = {2: 8, 1: 0, 3: 24, 0: 25}
    for i, phase in pair_phase.items():
        to = lax.rem(z + i, 4)
        send(dense.at[1 - core, to], pair_in.at[to], phase, partner, g)
    lane64 = lax.broadcasted_iota(jnp.int32, (64, 128), 1)
    row64 = lax.broadcasted_iota(jnp.int32, (64, 128), 0)
    for i in (2, 1, 3):
        to = lax.rem(z + i, 4)
        landed(pair_in.at[to], recv_sem.at[pair_phase[i]], "recv8")
        total = pair_in[to] + dense[core, to]
        step = power(eighths(total))
        pair_q[to] = counted(total, step)
        for f in range(3):
            line = jnp.sum(jnp.where(lane64 == row64, step[f], 0.0), axis=0, keepdims=True)
            pair_steps[to, f : f + 1] = line
        send(pair_q.at[to], dense_in.at[i - 1], 11, 2 * to + core, g)
        send(pair_steps.at[to], dense_steps.at[i - 1], 14, 2 * to + core, g)
    with jax.named_scope("stencil1"):
        stencil(1)
    landed(pair_in.at[z], recv_sem.at[25], "recv25")
    landed(dense_in.at[pl.ds(0, 3)], recv_sem.at[11], "recv11")
    landed(dense_steps.at[pl.ds(0, 3)], recv_sem.at[14], "recv14")
    for f in range(3):
        out = pair_in[z, f] + dense[core, z, f]
        for i in range(3):
            step = jnp.where(lane64 == row64, dense_steps[i, f : f + 1], 0.0)
            step = jnp.sum(step, axis=1, keepdims=True)
            out += step * dense_in[i, f].astype(jnp.int32).astype(F32)
        flux[f, :, 0:128] = out[0:32]
        flux[f, :, 128:256] = out[32:64]

    for phase in (15, 16, 17, 18, 19, 20, 21):
        landed(surf.at[0], send_sem.at[phase])
    landed(base.at[pl.ds(0, N_ALL // 2 - 1), 0], send_sem.at[6])
    landed(base.at[:, 0], send_sem.at[13])
    for phase in pair_phase.values():
        landed(pair_in.at[0], send_sem.at[phase])
    landed(dense_in.at[pl.ds(0, 3)], send_sem.at[11])
    landed(dense_steps.at[pl.ds(0, 3)], send_sem.at[14])

    landed(u_r.at[pl.ds(0, N_GRP - 1), 0], send_sem.at[2])
    landed(u_r.at[:, pl.ds(0, 3)], send_sem.at[4])
    landed(u_r, send_sem.at[5])

    @pl.when(polar)
    def _():
        landed(g1.at[pl.ds(0, 4 * (N_GRP - 1))], send_sem.at[1])
        landed(sel.at[pl.ds(0, 15)], send_sem.at[3])
        landed(sel.at[0], send_sem.at[9])
        landed(g1.at[pl.ds(0, 7 * (N_GRP - 1))], send_sem.at[7])

    @pl.when(inner)
    def _():
        landed(g1.at[pl.ds(0, N_GRP - 1)], send_sem.at[1])
        landed(sel.at[pl.ds(0, 15)], send_sem.at[3])
        landed(sel.at[pl.ds(0, 2)], send_sem.at[9])
        landed(crecv.at[pl.ds(0, 4 * (N_GRP - 1))], send_sem.at[7])

    helps = functools.reduce(jnp.logical_or, [g == d for d in HELPERS.values()])

    helps = jnp.logical_and(helps, core == 1)

    @pl.when(helps)
    def _():
        landed(sel.at[pl.ds(0, 3)], send_sem.at[23])
        landed(sel.at[0], send_sem.at[10])
        landed(sel.at[0], send_sem.at[12])

    @pl.when(jnp.logical_not(helps))
    def _():
        landed(sel.at[pl.ds(0, 4)], send_sem.at[22 + core])

    for sends, _, copy in halos:
        pl.when(sends)(lambda copy=copy: copy.wait_send())


def finish(pre, flux, ice, tracers_out, flux_out, ice_out, top, sem):
    copies = [
        pltpu.make_async_copy(pre.at[1], tracers_out.at[1], sem.at[0]),
        pltpu.make_async_copy(pre.at[0, pl.ds(1, L - 1)], tracers_out.at[0, pl.ds(1, L - 1)], sem.at[1]),
        pltpu.make_async_copy(flux, flux_out, sem.at[2]),
        pltpu.make_async_copy(ice, ice_out, sem.at[3]),
    ]
    for copy in copies:
        copy.start()
    top[...] = pre[0, 0] + 0.5 * flux[2]
    last = pltpu.make_async_copy(top, tracers_out.at[0, 0], sem.at[4])
    last.start()
    for copy in copies + [last]:
        copy.wait()


def on_device(
    tracers,
    velocity,
    remap_weights,
    remap_blocks,
    remap_count,
    ice_velocity,
    ice_mass_rate,
    ice_strength,
    wind_stress,
):
    def tiled(x):
        return x.reshape(2, 32, 128).transpose(1, 0, 2).reshape(4, 2, 8, 128)

    hbm = pl.BlockSpec(memory_space=pltpu.HBM)
    smem = pl.BlockSpec(memory_space=pltpu.SMEM)
    vmem = pl.BlockSpec(memory_space=pltpu.VMEM)
    scratch = [
        pltpu.SMEM((8, 32), jnp.int32),
        pltpu.SMEM((32,), jnp.int32),
        pltpu.VMEM((4, 2, 8, 128), F32),
        pltpu.VMEM((4, 2, 8, 128), F32),
        pltpu.VMEM((4, 2, 4, 128), F32),
        pltpu.VMEM((4, 2, 4, 128), F32),
        pltpu.VMEM((2, L, 32, 256), F32),
        pltpu.VMEM((2, L, 32, 256), F32),
        pltpu.VMEM((4, 8, 128, 128), BF16),
        pltpu.VMEM((4, 32, 256), F32),
        pltpu.VMEM((N_OCN, 64, 512), BF16),
        pltpu.VMEM((PADDED, 8, 128), jnp.int32),
        pltpu.VMEM((4, CHUNKS * 8, 128), BF16),
        pltpu.VMEM((512, 256), BF16),
        pltpu.VMEM((CHUNKS, 32, 128), BF16),
        pltpu.VMEM((2, N_GRP, 32, 128), BF16),
        pltpu.VMEM((2, N_GRP, 32, 128), BF16),
        pltpu.VMEM((2, 32, 128), BF16),
        pltpu.VMEM((2, 32, 128), BF16),
        pltpu.VMEM((4, 32, 128), F32),
        pltpu.VMEM((2, 8, 128), F32),
        pltpu.VMEM((2, 2, L, 128), F32),
        pltpu.VMEM((2, 2, L, 128), F32),
        pltpu.VMEM((2, 2, L, 256), F32),
        pltpu.VMEM((2, 2, L, 256), F32),
        pltpu.VMEM((N_GRP, 4, 2, 8, 128), F32),
        pltpu.VMEM((N_ALL + 2, 8, 128), F32),
        pltpu.VMEM((N_GRP, 4, 2, 4, 128), F32),
        pltpu.VMEM((N_GRP, 4, 2, 4, 128), F32),
        pltpu.VMEM((N_ALL, 8, 128), F32),
        pltpu.VMEM((N_ALL, 8, 128), F32),
        pltpu.VMEM((N_ALL // 2, 2, 8, 128), F32),
        pltpu.VMEM((N_ALL + 2, 8, 128), F32),
        *[pltpu.VMEM((N_ALL, 8, 128), F32)] * 7,
        pltpu.VMEM((4, 8, 128), F32),
        pltpu.VMEM((4, 24, 128), F32),
        pltpu.VMEM((PLANES_4, 8, 128), jnp.int16),
        pltpu.VMEM((PLANES, 8, 128), jnp.int16),
        pltpu.VMEM((2, 4, 3, 64, 128), F32),
        pltpu.VMEM((4, 3, 64, 128), F32),
        pltpu.VMEM((4, 3, 64, 128), jnp.int16),
        pltpu.VMEM((4, 3, 64, 128), jnp.int16),
        pltpu.VMEM((4, 8, 128), F32),
        pltpu.VMEM((4, 8, 128), F32),
        pltpu.SemaphoreType.DMA((16,)),
        pltpu.SemaphoreType.DMA((26,)),
        pltpu.SemaphoreType.DMA((26,)),
        pltpu.SemaphoreType.DMA((4,)),
        pltpu.SemaphoreType.DMA((4,)),
    ]
    pre, flux, ice = pl.pallas_call(
        kernel,
        out_shape=(
            jax.ShapeDtypeStruct((2, L, 32, 256), F32),
            jax.ShapeDtypeStruct((3, 32, 256), F32),
            jax.ShapeDtypeStruct((8, 8, 128), F32),
        ),
        in_specs=[hbm] * 9,
        out_specs=(vmem, vmem, vmem),
        scratch_shapes=scratch,
        compiler_params=pltpu.CompilerParams(
            collective_id=0, has_side_effects=True, vmem_limit_bytes=40 * 1024 * 1024
        ),
    )(
        *(
            pltpu.with_memory_space_constraint(x, pltpu.HBM)
            for x in (
                tracers,
                velocity,
                remap_weights,
                remap_blocks.T,
                remap_count,
                tiled(ice_velocity),
                tiled(wind_stress),
                ice_mass_rate.reshape(4, 2, 4, 128),
                ice_strength.reshape(4, 2, 4, 128),
            )
        )
    )
    tracers_next, flux, ice = pl.pallas_call(
        finish,
        out_shape=(
            jax.ShapeDtypeStruct((2, L, 32, 256), F32),
            jax.ShapeDtypeStruct((3, 32, 256), F32),
            jax.ShapeDtypeStruct((8, 8, 128), F32),
        ),
        in_specs=[vmem] * 3,
        out_specs=(hbm, hbm, hbm),
        scratch_shapes=[pltpu.VMEM((32, 256), F32), pltpu.SemaphoreType.DMA((5,))],
        compiler_params=pltpu.CompilerParams(vmem_limit_bytes=8 * 1024 * 1024),
    )(pre, flux, ice)
    ice_final = ice.reshape(32, 2, 128).transpose(1, 0, 2).reshape(2, 4096)
    return tracers_next, flux, ice_final


def solution(mesh):
    placed = (
        P(None, None, "grp", "ocn"),
        P(None, None, "grp", "ocn"),
        P("grp", None, None, None),
        P("grp", None),
        P("grp"),
        P(None, "grp"),
        P("grp"),
        P("grp"),
        P(None, "grp"),
    )
    return jax.shard_map(
        on_device,
        mesh=mesh,
        in_specs=placed,
        out_specs=(P(None, None, "grp", "ocn"), P(None, "grp", "ocn"), P(None, "grp")),
        check_vma=False,
    )
```
